128 devices in a mesh: head: 8 (over y, core), row: 16 (over x, z).
Axes of the slice: x: 4, y: 4, z: 4, core: 2. Of those that a mesh axis runs over, the one named last changes fastest.
Arguments:
- hidden_in: bfloat16 [512, 2048], replicated, may hold values from -6 to 6
- w_query: bfloat16 [2048, 16, 128], P(None, 'head', 'row'), may hold values from -0.125 to 0.125
- w_key: bfloat16 [2048, 16, 128], P(None, 'head', 'row'), may hold values from -0.125 to 0.125
- w_value: bfloat16 [2048, 32, 128], P(None, 'head'), may hold values from -0.125 to 0.125
- w_zgate: bfloat16 [2048, 32, 128], P(None, 'head'), may hold values from -0.125 to 0.125
- w_decay: bfloat16 [2048, 32], P(None, 'head'), may hold values from -0.125 to 0.125
- w_beta: bfloat16 [2048, 32], P(None, 'head'), may hold values from -0.125 to 0.125
- decay_log: float32 [32], P('head'), may hold values from -1.5 to 1.5
- dt_bias: float32 [32], P('head'), may hold values from -2 to 2
- norm_gain: float32 [128], replicated, may hold values from 0.1 to 1.9
- w_out: bfloat16 [32, 128, 2048], P('head'), may hold values from -0.09375 to 0.09375
- state: float32 [512, 32, 128, 128], P(None, 'head', 'row'), may hold values from -6 to 6
Outputs:
- layer_out: bfloat16 [512, 2048], P('row', 'head')
- new_state: float32 [512, 32, 128, 128], P(None, 'head', 'row')
The draws below stay inside these ranges and needn't reach their ends.
All inputs are finite; a program needn't handle non-finite values.
Results may differ from the reference program's by a relative error of at most 0.005.
Values sent between devices are 32-bit elements; how exact they have to be, the bound alone decides.
A program may use at most 128 MiB of HBM per device.

```python
import jax
import jax.numpy as jnp
from jax import lax

D = 2048
H = 32
HK = 16
K = 128
V = 128
SEQS = 512


def block_levels(rng, extent, shards, least, top_value):
    loudness = 1.0
    for dim, parts in shards:
        draws = jax.random.uniform(jax.random.fold_in(jax.random.fold_in(rng, 6), dim), (parts,), jnp.float32, least / len(shards), top_value / len(shards))
        loudness = loudness * jnp.repeat(jnp.exp(draws), extent[dim] // parts).reshape((-1,) + (1,) * (len(extent) - 1 - dim))
    return loudness


def noise(key, extent, width, reach, split=(), held_as=jnp.bfloat16):
    result = width * jax.random.normal(key, extent, jnp.float32)
    if split:
        result = result * block_levels(key, extent, split, -0.22, 0.18)
    return jnp.clip(result, -reach, reach).astype(held_as)


def setup_inputs(seed: int = 0) -> dict:
    arg_keys = jax.random.split(jax.random.key(seed), 13)
    hidden_in = noise(arg_keys[0], (SEQS, D), 1.0, 6.0)
    w_query = noise(arg_keys[1], (D, HK, K), D ** -0.5, 0.125, ((1, 8), (2, 16)))
    w_key = noise(arg_keys[2], (D, HK, K), D ** -0.5, 0.125, ((1, 8), (2, 16)))
    w_value = noise(arg_keys[3], (D, H, V), D ** -0.5, 0.125, ((1, 8),))
    w_zgate = noise(arg_keys[4], (D, H, V), D ** -0.5, 0.125, ((1, 8),))
    w_decay = noise(arg_keys[5], (D, H), D ** -0.5, 0.125, ((1, 8),))
    w_beta = noise(arg_keys[6], (D, H), D ** -0.5, 0.125, ((1, 8),))
    decay_log = jnp.clip(jax.random.uniform(arg_keys[7], (H,), jnp.float32, -1.5, 1.5) * block_levels(arg_keys[7], (H,), ((0, 8),), -0.4, 0.0), -1.5, 1.5)
    dt_bias = jnp.clip(jax.random.uniform(arg_keys[8], (H,), jnp.float32, -2.0, 2.0) * block_levels(arg_keys[8], (H,), ((0, 8),), -0.4, 0.0), -2.0, 2.0)
    norm_gain = jnp.clip(1.0 + 0.18 * jax.random.normal(arg_keys[9], (V,), jnp.float32), 0.1, 1.9)
    w_out = noise(arg_keys[10], (H, V, D), (H * V) ** -0.5, 0.09375, ((0, 8),))
    state = noise(arg_keys[11], (SEQS, H, K, V), 1.0, 6.0, ((1, 8), (2, 16)), jnp.float32)
    return {"hidden_in": hidden_in, "w_query": w_query, "w_key": w_key, "w_value": w_value, "w_zgate": w_zgate, "w_decay": w_decay, "w_beta": w_beta, "decay_log": decay_log, "dt_bias": dt_bias, "norm_gain": norm_gain, "w_out": w_out, "state": state}


def reference(hidden_in, w_query, w_key, w_value, w_zgate, w_decay, w_beta, decay_log, dt_bias, norm_gain, w_out, state):
    xf = hidden_in.astype(jnp.float32)
    query = jnp.einsum('bd,dhk->bhk', xf, w_query.astype(jnp.float32))
    keys = jnp.einsum('bd,dhk->bhk', xf, w_key.astype(jnp.float32))
    values = jnp.einsum('bd,dhv->bhv', xf, w_value.astype(jnp.float32))
    zgate = jnp.einsum('bd,dhv->bhv', xf, w_zgate.astype(jnp.float32))
    decay_in = jnp.dot(hidden_in, w_decay, preferred_element_type=jnp.float32) + dt_bias
    decay = jnp.exp(-jnp.exp(decay_log) * jax.nn.softplus(decay_in))
    beta = jax.nn.sigmoid(jnp.dot(hidden_in, w_beta, preferred_element_type=jnp.float32))
    group = state.shape[1] // keys.shape[1]
    query_unit = query * lax.rsqrt(1.0 + lax.optimization_barrier(jnp.sum(query * query, axis=-1, keepdims=True)))
    key_unit = keys * lax.rsqrt(1.0 + lax.optimization_barrier(jnp.sum(keys * keys, axis=-1, keepdims=True)))
    query_wide = jnp.repeat(query_unit, group, axis=1)
    key_wide = jnp.repeat(key_unit, group, axis=1)
    readk = jnp.einsum('bhkv,bhk->bhv', state, key_wide, precision=lax.Precision.HIGHEST)
    delta = beta[..., None] * (values - decay[..., None] * readk)
    new_state = decay[..., None, None] * state + key_wide[..., None] * delta[:, :, None, :]
    readq = jnp.einsum('bhkv,bhk->bhv', new_state, query_wide, precision=lax.Precision.HIGHEST)
    meansq = lax.optimization_barrier(jnp.mean(readq * readq, axis=-1, keepdims=True))
    normed = (readq * lax.rsqrt(meansq + 0.5) * norm_gain * jax.nn.silu(zgate)).astype(jnp.bfloat16)
    layer_out = jnp.einsum('bhv,hvd->bd', normed.astype(jnp.float32), w_out.astype(jnp.float32))
    return (layer_out.astype(jnp.bfloat16), new_state)
```

```python
import functools

import jax
import jax.numpy as jnp
from jax import lax
from jax.experimental import pallas as pl
from jax.experimental.pallas import tpu as pltpu
from jax.sharding import PartitionSpec as P

F32 = jnp.float32
BF16 = jnp.bfloat16
NT = (((1,), (1,)), ((), ()))
SIDE = 4
COLS = 40
HEADS = 8


def softplus(x):
    return jnp.maximum(x, 0.0) + jnp.log1p(jnp.exp(-jnp.abs(x)))


class Copies:
    def __init__(self, send, recv):
        self.send, self.recv, self.made = send, recv, []

    def start(self, src, dst, peer):
        n = len(self.made)
        copy = pltpu.make_async_remote_copy(
            src_ref=src,
            dst_ref=dst,
            send_sem=self.send.at[n],
            recv_sem=self.recv.at[n],
            device_id=peer,
            device_id_type=pl.DeviceIdType.MESH,
        )
        copy.start()
        self.made.append(copy)
        return copy


class Ring:
    def __init__(self, me, row_of):
        self.me = me
        self.right = lax.rem(me + 1, SIDE)
        self.far = lax.rem(me + 2, SIDE)
        self.left = lax.rem(me + 3, SIDE)
        self.to_right = {"row": row_of(self.right)}
        self.to_far = {"row": row_of(self.far)}
        self.to_left = {"row": row_of(self.left)}


class Scatter:
    def __init__(self, copies, ring, part, land):
        self.copies, self.ring, self.part, self.land = copies, ring, part, land

    def send_far(self):
        r = self.ring
        self.relay = [
            self.copies.start(self.part(0, r.far), self.land.at[0, 0], r.to_left),
            self.copies.start(self.part(1, r.far), self.land.at[1, 0], r.to_right),
        ]

    def send_near(self):
        r = self.ring
        self.direct = [
            self.copies.start(self.part(0, r.right), self.land.at[0, 1], r.to_right),
            self.copies.start(self.part(1, r.left), self.land.at[1, 1], r.to_left),
        ]

    def forward(self):
        r = self.ring
        self.joint = []
        for half, to, peer in ((0, r.left, r.to_left), (1, r.right, r.to_right)):
            self.relay[half].wait_recv()
            piece = self.part(half, to)
            piece[...] = piece[...] + self.land[half, 0]
            self.joint.append(self.copies.start(piece, self.land.at[half, 2], peer))

    def finish(self):
        for half in (0, 1):
            self.direct[half].wait_recv()
            self.joint[half].wait_recv()
            piece = self.part(half, self.ring.me)
            piece[...] = piece[...] + self.land[half, 1] + self.land[half, 2]


class Gather:
    def __init__(self, copies, ring, part, both):
        self.copies, self.ring, self.part, self.both = copies, ring, part, both

    def send(self):
        r = self.ring
        mine = self.both(r.me)
        self.near = [
            self.copies.start(mine, mine, r.to_right),
            self.copies.start(mine, mine, r.to_left),
        ]

    def forward(self):
        r = self.ring
        self.far = []
        for n, (half, at, peer) in enumerate(((0, r.left, r.to_right), (1, r.right, r.to_left))):
            self.near[n].wait_recv()
            piece = self.part(half, at)
            self.far.append(self.copies.start(piece, piece, peer))

    def finish(self):
        for copy in self.far:
            copy.wait_recv()


def exchange_kernel(
    hid,
    wq,
    wk,
    wd,
    wb,
    values,
    zgate,
    decay_log,
    dt_bias,
    gain,
    w_out,
    state,
    delta_all,
    proj,
    layer_out,
    held,
    spread,
    part,
    land1,
    land2,
    small,
    small_land1,
    small_land2,
    scales,
    normed,
    outs,
    outs_land,
    load_sem,
    send_sem,
    recv_sem,
):
    row = lax.axis_index("row")
    head = lax.axis_index("head")
    x, z = row // SIDE, lax.rem(row, SIDE)
    blk = held.shape[0] // (SIDE * SIDE)

    barrier = pltpu.get_barrier_semaphore()
    peers = []
    for d in (1, 2, 3):
        peers.append({"row": lax.rem(x + d, SIDE) * SIDE + z})
        peers.append({"row": x * SIDE + lax.rem(z + d, SIDE)})
    for d in range(1, HEADS):
        peers.append({"head": lax.rem(head + d, HEADS)})
    for peer in peers:
        pl.semaphore_signal(barrier, inc=1, device_id=peer, device_id_type=pl.DeviceIdType.MESH)

    def row_at(o, first, second):
        return first * SIDE + second if o == 0 else second * SIDE + first

    rings1 = [
        Ring(x, lambda a: row_at(0, a, z)),
        Ring(z, lambda a: row_at(1, a, x)),
    ]
    rings2 = [
        Ring(z, lambda b: row_at(0, x, b)),
        Ring(x, lambda b: row_at(1, z, b)),
    ]
    order = [[r.far, r.right, r.left, r.me] for r in rings1]

    loads = {}
    for j in range(SIDE):
        for o in (0, 1):
            for b in range(SIDE):
                n = (j * 2 + o) * SIDE + b
                at = row_at(o, order[o][j], b) * blk
                loads[j, o, b] = pltpu.make_async_copy(
                    state.at[pl.ds(at, blk), pl.ds(2 * o, 2)],
                    held.at[pl.ds(at, blk), pl.ds(2 * o, 2)],
                    load_sem.at[n],
                )
                loads[j, o, b].start()

    w = jnp.concatenate(
        [wq[0].astype(F32), wq[1].astype(F32), wk[0].astype(F32), wk[1].astype(F32), wd[...].astype(F32), wb[...].astype(F32)],
        axis=0,
    ).astype(BF16)
    proj[...] = lax.dot_general(hid[...], w, NT, preferred_element_type=F32)

    col = lax.broadcasted_iota(jnp.int32, (COLS, 512), 0)
    lane = lax.broadcasted_iota(jnp.int32, (COLS, 512), 1)
    for hk in (0, 1):
        base = jnp.where(lane < 256, 16, 0) + 8 * hk
        spread[hk] = (col == base + lane % 8).astype(F32).astype(BF16)

    q, k = proj[:, 0:16], proj[:, 16:32]
    seg = (
        lax.broadcasted_iota(jnp.int32, (8, 16), 1) // 8 == lax.broadcasted_iota(jnp.int32, (8, 16), 0)
    ).astype(F32)
    seg_k = (
        lax.broadcasted_iota(jnp.int32, (8, 16), 1) // 8 + 2 == lax.broadcasted_iota(jnp.int32, (8, 16), 0)
    ).astype(F32)
    seg_qk = (
        lax.broadcasted_iota(jnp.int32, (8, 16), 1) // 8 + 4 == lax.broadcasted_iota(jnp.int32, (8, 16), 0)
    ).astype(F32)
    sums = (
        lax.dot_general(seg, q * q, NT, precision=lax.Precision.HIGHEST, preferred_element_type=F32)
        + lax.dot_general(seg_k, k * k, NT, precision=lax.Precision.HIGHEST, preferred_element_type=F32)
        + lax.dot_general(seg_qk, q * k, NT, precision=lax.Precision.HIGHEST, preferred_element_type=F32)
    )
    for a in range(SIDE):
        small[a] = sums[:, a * 128 : (a + 1) * 128]

    pl.semaphore_wait(barrier, len(peers))
    copies = Copies(send_sem, recv_sem)

    small1 = []
    for d in (1, 2, 3):
        to = lax.rem(x + d, SIDE)
        small1.append(copies.start(small.at[to], small_land1.at[d - 1], {"row": to * SIDE + z}))

    own_lane = lax.broadcasted_iota(jnp.int32, (2 * blk, 8 * blk), 1) // 8
    own_row = lax.rem(lax.broadcasted_iota(jnp.int32, (2 * blk, 8 * blk), 0), blk)
    own = own_lane == own_row

    def read_block(o, first, second):
        at = pl.multiple_of(row_at(o, first, second) * blk, blk)
        vec = proj[pl.ds(at, blk), :].astype(BF16)
        wide = jnp.dot(vec, spread[o], preferred_element_type=F32)
        wide = jnp.concatenate([wide[:, : 8 * blk], wide[:, 8 * blk :]], axis=0)
        wide = jnp.where(own, wide, 0.0).astype(BF16)
        block = jnp.concatenate(
            [held[pl.ds(at, blk), 2 * o + c].reshape(8 * blk, 128).astype(BF16) for c in (0, 1)], axis=1
        )
        read = jnp.dot(wide, block, preferred_element_type=F32)
        for c in (0, 1):
            for t in (0, 1):
                part[o, c, t, first, second] = read[t * blk : (t + 1) * blk, c * 128 : (c + 1) * 128]

    def scatter1(o, t):
        return Scatter(copies, rings1[o], lambda c, a: part.at[o, c, t, a], land1.at[o, t])

    def scatter2(o, t):
        return Scatter(copies, rings2[o], lambda c, b: part.at[o, c, t, rings1[o].me, b], land2.at[o, t])

    k1 = [scatter1(o, 0) for o in (0, 1)]
    q1 = [scatter1(o, 1) for o in (0, 1)]
    k2 = [scatter2(o, 0) for o in (0, 1)]
    q2 = [scatter2(o, 1) for o in (0, 1)]

    for j in range(SIDE):
        for o in (0, 1):
            for b in range(SIDE):
                loads[j, o, b].wait()
                read_block(o, order[o][j], b)
            if j == 0:
                k1[o].send_far()
            if j == 2:
                k1[o].send_near()

    for s in q1:
        s.send_far()

    for copy in small1:
        copy.wait_recv()
    small[x] = small[x] + small_land1[0] + small_land1[1] + small_land1[2]
    small2 = []
    for d in (1, 2, 3):
        to = lax.rem(z + d, SIDE)
        small2.append(copies.start(small.at[x], small_land2.at[d - 1], {"row": x * SIDE + to}))

    for s in k1:
        s.forward()
    for s in q1:
        s.send_near()
    for s in q1:
        s.forward()
    for s in k1:
        s.finish()
    for s in k2:
        s.send_far()
        s.send_near()

    for copy in small2:
        copy.wait_recv()
    total = small[x] + small_land2[0] + small_land2[1] + small_land2[2]
    scales[...] = jnp.concatenate([total, jnp.zeros((120, 128), F32)], axis=0).T
    mine = pl.ds(pl.multiple_of(row * blk, blk), blk)
    raw = scales[pl.ds(pl.multiple_of(z * blk, blk), blk), :]
    own_proj = proj[mine, :]
    q_scale = lax.rsqrt(1.0 + raw[:, 0:2])
    k_scale = lax.rsqrt(1.0 + raw[:, 2:4])
    unit_dot = raw[:, 4:6] * q_scale * k_scale
    decay = jnp.exp(-jnp.exp(decay_log[...]) * softplus(own_proj[:, 32:36] + dt_bias[...]))
    beta = 1.0 / (1.0 + jnp.exp(-own_proj[:, 36:40]))

    for s in k2:
        s.forward()
    for s in k2:
        s.finish()

    deltas = []
    for h in range(4):
        o, c = h // 2, h % 2
        r1, r2 = rings1[o], rings2[o]
        readk = part[o, c, 0, r1.me, r2.me] * k_scale[:, o : o + 1]
        delta = beta[:, h : h + 1] * (values[:, h * 128 : (h + 1) * 128] - decay[:, h : h + 1] * readk)
        delta_all[o, c, r1.me, r2.me] = delta * k_scale[:, o : o + 1]
        deltas.append(delta)

    g2 = [
        Gather(
            copies,
            rings2[o],
            lambda c, b, o=o: delta_all.at[o, c, rings1[o].me, b],
            lambda b, o=o: delta_all.at[o, :, rings1[o].me, b],
        )
        for o in (0, 1)
    ]
    g1 = [
        Gather(
            copies,
            rings1[o],
            lambda c, a, o=o: delta_all.at[o, c, a],
            lambda a, o=o: delta_all.at[o, :, a],
        )
        for o in (0, 1)
    ]
    for g in g2:
        g.send()
    for s in q1:
        s.finish()
    for s in q2:
        s.send_far()
        s.send_near()
    for g in g2:
        g.forward()
    for s in q2:
        s.forward()
    for g in g2:
        g.finish()
    for g in g1:
        g.send()
    for s in q2:
        s.finish()

    for h in range(4):
        o, c = h // 2, h % 2
        r1, r2 = rings1[o], rings2[o]
        old = part[o, c, 1, r1.me, r2.me] * q_scale[:, o : o + 1]
        readq = decay[:, h : h + 1] * old + unit_dot[:, o : o + 1] * deltas[h]
        meansq = jnp.mean(readq * readq, axis=-1, keepdims=True)
        gate = zgate[:, h * 128 : (h + 1) * 128]
        gate = gate / (1.0 + jnp.exp(-gate))
        normed[:, h * 128 : (h + 1) * 128] = (readq * lax.rsqrt(meansq + 0.5) * gain[...] * gate).astype(BF16)

    width = outs.shape[-1]
    for n in range(HEADS):
        outs[n] = jnp.dot(normed[...], w_out[:, n * width : (n + 1) * width], preferred_element_type=F32)
    out_copies = []
    for d in range(1, HEADS):
        to = lax.rem(head + d, HEADS)
        out_copies.append(copies.start(outs.at[to], outs_land.at[head], {"head": to}))
    outs_land[head] = outs[head]

    for g in g1:
        g.forward()
    for copy in out_copies:
        copy.wait_recv()
    total_out = outs_land[0]
    for n in range(1, HEADS):
        total_out = total_out + outs_land[n]
    layer_out[...] = total_out.astype(BF16)
    for g in g1:
        g.finish()
    for copy in copies.made:
        copy.wait_send()


def update_kernel(decay_log, dt_bias, proj, delta_all, state, new_state):
    r = pl.program_id(0)
    a, b = r // SIDE, lax.rem(r, SIDE)
    blk = state.shape[0]
    vec = proj[...]
    decay = jnp.exp(-jnp.exp(decay_log[...]) * softplus(vec[:, 32:36] + dt_bias[...]))
    hi = vec.astype(BF16)
    lo = (vec - hi.astype(F32)).astype(BF16)
    three = jnp.concatenate([hi.astype(F32), hi.astype(F32), lo.astype(F32)], axis=0).astype(BF16)
    own = (
        lax.broadcasted_iota(jnp.int32, (8 * blk, 3 * blk), 0) // 8
        == lax.rem(lax.broadcasted_iota(jnp.int32, (8 * blk, 3 * blk), 1), blk)
    )
    for o in (0, 1):
        pick = (
            lax.broadcasted_iota(jnp.int32, (8 * blk, COLS), 1)
            == 16 + 8 * o + lax.rem(lax.broadcasted_iota(jnp.int32, (8 * blk, COLS), 0), 8)
        ).astype(F32).astype(BF16)
        wide = lax.dot_general(pick, three, NT, preferred_element_type=F32)
        wide = jnp.where(own, wide, 0.0).astype(BF16)
        first, second = (a, b) if o == 0 else (b, a)
        step = jnp.concatenate([delta_all[o, c, first, second] for c in (0, 1)], axis=1)
        step_hi = step.astype(BF16)
        step_lo = (step - step_hi.astype(F32)).astype(BF16)
        steps = jnp.concatenate([step_hi, step_lo, step_hi], axis=0)
        add = jnp.dot(wide, steps, preferred_element_type=F32)
        for c in (0, 1):
            h = 2 * o + c
            keep = jnp.broadcast_to(decay[:, h : h + 1], (blk, 128))
            new_state[:, h] = keep[:, None, :] * state[:, h] + add[:, c * 128 : (c + 1) * 128].reshape(blk, 8, 128)


def local(
    hidden_in,
    w_query,
    w_key,
    w_value,
    w_zgate,
    w_decay,
    w_beta,
    decay_log,
    dt_bias,
    norm_gain,
    w_out,
    state,
):
    seqs, width = hidden_in.shape
    rows = SIDE * SIDE
    blk = seqs // rows
    first_row = lax.axis_index("row") * blk
    own_hidden = lax.dynamic_slice_in_dim(hidden_in, first_row, blk, 0)
    values = jnp.einsum("bd,dhv->bhv", own_hidden, w_value, preferred_element_type=F32).reshape(blk, 512)
    zgate = jnp.einsum("bd,dhv->bhv", own_hidden, w_zgate, preferred_element_type=F32).reshape(blk, 512)
    vmem = pl.BlockSpec(memory_space=pltpu.VMEM)
    n_copies = 3 + 3 + 2 * 2 * 6 * 2 + 2 * 2 * 4 + HEADS - 1
    delta_all, proj, layer_out = pl.pallas_call(
        exchange_kernel,
        out_shape=(
            jax.ShapeDtypeStruct((2, 2, SIDE, SIDE, blk, 128), F32),
            jax.ShapeDtypeStruct((seqs, COLS), F32),
            jax.ShapeDtypeStruct((blk, 256), BF16),
        ),
        in_specs=[vmem] * 11 + [pl.BlockSpec(memory_space=pl.ANY)],
        out_specs=(vmem, vmem, vmem),
        scratch_shapes=[
            pltpu.VMEM((seqs, 4, 8, 128), F32),
            pltpu.VMEM((2, COLS, 512), BF16),
            pltpu.VMEM((2, 2, 2, SIDE, SIDE, blk, 128), F32),
            pltpu.VMEM((2, 2, 2, 3, SIDE, blk, 128), F32),
            pltpu.VMEM((2, 2, 2, 3, blk, 128), F32),
            pltpu.VMEM((SIDE, 8, 128), F32),
            pltpu.VMEM((3, 8, 128), F32),
            pltpu.VMEM((3, 8, 128), F32),
            pltpu.VMEM((128, 128), F32),
            pltpu.VMEM((blk, 512), BF16),
            pltpu.VMEM((HEADS, blk, 256), F32),
            pltpu.VMEM((HEADS, blk, 256), F32),
            pltpu.SemaphoreType.DMA((32,)),
            pltpu.SemaphoreType.DMA((n_copies,)),
            pltpu.SemaphoreType.DMA((n_copies,)),
        ],
        compiler_params=pltpu.CompilerParams(
            collective_id=0, has_side_effects=True, vmem_limit_bytes=48 * 1024 * 1024
        ),
        name="exchange",
    )(
        hidden_in,
        jnp.transpose(w_query, (1, 2, 0)),
        jnp.transpose(w_key, (1, 2, 0)),
        jnp.transpose(w_decay, (1, 0)),
        jnp.transpose(w_beta, (1, 0)),
        values,
        zgate,
        decay_log.reshape(1, 4),
        dt_bias.reshape(1, 4),
        norm_gain.reshape(1, 128),
        w_out.reshape(512, width),
        state,
    )
    new_state = pl.pallas_call(
        update_kernel,
        grid=(rows,),
        out_shape=jax.ShapeDtypeStruct(state.shape, F32),
        in_specs=[
            pl.BlockSpec((1, 4), lambda r: (0, 0)),
            pl.BlockSpec((1, 4), lambda r: (0, 0)),
            pl.BlockSpec((blk, COLS), lambda r: (r, 0)),
            pl.BlockSpec((2, 2, SIDE, SIDE, blk, 128), lambda r: (0, 0, 0, 0, 0, 0)),
            pl.BlockSpec((blk, 4, 8, 128), lambda r: (r, 0, 0, 0)),
        ],
        out_specs=pl.BlockSpec((blk, 4, 8, 128), lambda r: (r, 0, 0, 0)),
        name="update",
    )(decay_log.reshape(1, 4), dt_bias.reshape(1, 4), proj, delta_all, state)
    return (layer_out, new_state)


def solution(mesh):
    in_specs = (
        P(),
        P(None, "head", "row"),
        P(None, "head", "row"),
        P(None, "head", None),
        P(None, "head", None),
        P(None, "head"),
        P(None, "head"),
        P("head"),
        P("head"),
        P(),
        P("head", None, None),
        P(None, "head", "row", None),
    )
    out_specs = (P("row", "head"), P(None, "head", "row", None))
    return jax.shard_map(local, mesh=mesh, in_specs=in_specs, out_specs=out_specs, check_vma=False)
```

```python
import functools

import jax
import jax.numpy as jnp
from jax import lax
from jax.experimental import pallas as pl
from jax.experimental.pallas import tpu as pltpu
from jax.sharding import PartitionSpec as P

F32 = jnp.float32
BF16 = jnp.bfloat16
NT = (((1,), (1,)), ((), ()))
SIDE = 4
COLS = 40
HEADS = 8


def softplus(x):
    return jnp.maximum(x, 0.0) + jnp.log1p(jnp.exp(-jnp.abs(x)))


class Copies:
    def __init__(self, send, recv):
        self.send, self.recv, self.made = send, recv, []

    def start(self, src, dst, peer):
        n = len(self.made)
        copy = pltpu.make_async_remote_copy(
            src_ref=src,
            dst_ref=dst,
            send_sem=self.send.at[n],
            recv_sem=self.recv.at[n],
            device_id=peer,
            device_id_type=pl.DeviceIdType.MESH,
        )
        copy.start()
        self.made.append(copy)
        return copy


class Ring:
    def __init__(self, me, row_of):
        self.me = me
        self.right = lax.rem(me + 1, SIDE)
        self.far = lax.rem(me + 2, SIDE)
        self.left = lax.rem(me + 3, SIDE)
        self.to_right = {"row": row_of(self.right)}
        self.to_far = {"row": row_of(self.far)}
        self.to_left = {"row": row_of(self.left)}


class Scatter:
    def __init__(self, copies, ring, part, land):
        self.copies, self.ring, self.part, self.land = copies, ring, part, land

    def send_far(self):
        r = self.ring
        self.relay = [
            self.copies.start(self.part(0, r.far), self.land.at[0, 0], r.to_left),
            self.copies.start(self.part(1, r.far), self.land.at[1, 0], r.to_right),
        ]

    def send_near(self):
        r = self.ring
        self.direct = [
            self.copies.start(self.part(0, r.right), self.land.at[0, 1], r.to_right),
            self.copies.start(self.part(1, r.left), self.land.at[1, 1], r.to_left),
        ]

    def forward(self):
        r = self.ring
        self.joint = []
        for half, to, peer in ((0, r.left, r.to_left), (1, r.right, r.to_right)):
            self.relay[half].wait_recv()
            piece = self.part(half, to)
            piece[...] = piece[...] + self.land[half, 0]
            self.joint.append(self.copies.start(piece, self.land.at[half, 2], peer))

    def finish(self):
        for half in (0, 1):
            self.direct[half].wait_recv()
            self.joint[half].wait_recv()
            piece = self.part(half, self.ring.me)
            piece[...] = piece[...] + self.land[half, 1] + self.land[half, 2]


class Direct:
    def __init__(self, copies, ring):
        self.copies, self.ring, self.sent = copies, ring, []

    def send(self, src, dst):
        r = self.ring
        for d, (at, peer) in enumerate(((r.right, r.to_right), (r.left, r.to_left), (r.far, r.to_far))):
            self.sent.append(self.copies.start(src(at), dst(d), peer))

    def wait(self):
        for copy in self.sent:
            copy.wait_recv()


class Gather:
    def __init__(self, copies, ring, part, both):
        self.copies, self.ring, self.part, self.both = copies, ring, part, both

    def send(self):
        r = self.ring
        mine = self.both(r.me)
        self.near = [
            self.copies.start(mine, mine, r.to_right),
            self.copies.start(mine, mine, r.to_left),
        ]

    def forward(self):
        r = self.ring
        self.far = []
        for n, (half, at, peer) in enumerate(((0, r.left, r.to_right), (1, r.right, r.to_left))):
            self.near[n].wait_recv()
            piece = self.part(half, at)
            self.far.append(self.copies.start(piece, piece, peer))

    def finish(self):
        for copy in self.far:
            copy.wait_recv()


def split(x):
    hi = x.astype(BF16)
    return hi, (x - hi.astype(F32)).astype(BF16)


def exchange_kernel(
    wq,
    wk,
    wd,
    wb,
    decay_log,
    dt_bias,
    gain,
    hid_hbm,
    wv_hbm,
    wz_hbm,
    w_out_hbm,
    state,
    layer_out,
    held,
    hid,
    wv,
    wz,
    w_out,
    proj,
    decay_all,
    spread,
    part,
    land1,
    land2,
    delta_all,
    lift,
    small,
    small_land1,
    small_land2,
    scales,
    normed,
    outs,
    outs_land,
    load_sem,
    weight_sem,
    send_sem,
    recv_sem,
):
    row = lax.axis_index("row")
    head = lax.axis_index("head")
    x, z = row // SIDE, lax.rem(row, SIDE)
    rows = SIDE * SIDE
    blk = held.shape[0] // rows

    barrier = pltpu.get_barrier_semaphore()
    peers = []
    for d in (1, 2, 3):
        peers.append({"row": lax.rem(x + d, SIDE) * SIDE + z})
        peers.append({"row": x * SIDE + lax.rem(z + d, SIDE)})
    for d in range(1, HEADS):
        peers.append({"head": lax.rem(head + d, HEADS)})
    for peer in peers:
        pl.semaphore_signal(barrier, inc=1, device_id=peer, device_id_type=pl.DeviceIdType.MESH)

    def row_at(o, first, second):
        return first * SIDE + second if o == 0 else second * SIDE + first

    rings1 = [
        Ring(x, lambda a: row_at(0, a, z)),
        Ring(z, lambda a: row_at(1, a, x)),
    ]
    rings2 = [
        Ring(z, lambda b: row_at(0, x, b)),
        Ring(x, lambda b: row_at(1, z, b)),
    ]
    order = [[r.far, r.right, r.left, r.me] for r in rings1]

    load_hid = pltpu.make_async_copy(hid_hbm, hid, weight_sem.at[0])
    load_hid.start()
    loads = {}
    for j in range(SIDE):
        for o in (0, 1):
            for b in range(SIDE):
                n = (j * 2 + o) * SIDE + b
                at = row_at(o, order[o][j], b) * blk
                loads[j, o, b] = pltpu.make_async_copy(
                    state.at[pl.ds(at, blk), pl.ds(2 * o, 2)],
                    held.at[pl.ds(at, blk), pl.ds(2 * o, 2)],
                    load_sem.at[n],
                )
                loads[j, o, b].start()
    load_weights = []
    for n, (src, dst) in enumerate(((wv_hbm, wv), (wz_hbm, wz), (w_out_hbm, w_out))):
        load_weights.append(pltpu.make_async_copy(src, dst, weight_sem.at[n + 1]))
        load_weights[-1].start()

    w = jnp.concatenate(
        [
            wq[0].astype(F32),
            wq[1].astype(F32),
            wk[0].astype(F32),
            wk[1].astype(F32),
            wd[...].astype(F32),
            wb[...].astype(F32),
        ],
        axis=0,
    ).astype(BF16)
    col = lax.broadcasted_iota(jnp.int32, (COLS, 512), 0)
    lane = lax.broadcasted_iota(jnp.int32, (COLS, 512), 1)
    for hk in (0, 1):
        base = jnp.where(lane < 256, 16, 0) + 8 * hk
        spread[hk] = (col == base + lane % 8).astype(F32).astype(BF16)
    load_hid.wait()
    proj[...] = lax.dot_general(hid[...], w, NT, preferred_element_type=F32)

    q, k = proj[:, 0:16], proj[:, 16:32]
    sums = 0.0
    for n, product in enumerate((q * q, k * k, q * k)):
        seg = (
            lax.broadcasted_iota(jnp.int32, (8, 16), 1) // 8 + 2 * n == lax.broadcasted_iota(jnp.int32, (8, 16), 0)
        ).astype(F32)
        sums = sums + lax.dot_general(
            seg, product, NT, precision=lax.Precision.HIGHEST, preferred_element_type=F32
        )
    for a in range(SIDE):
        small[a] = sums[:, a * 128 : (a + 1) * 128]

    copies = Copies(send_sem, recv_sem)
    own_lane = lax.broadcasted_iota(jnp.int32, (4 * blk, 8 * blk), 1) // 8
    own_row = lax.rem(lax.broadcasted_iota(jnp.int32, (4 * blk, 8 * blk), 0), blk)
    own = own_lane == own_row

    def read_block(o, first, second):
        at = pl.multiple_of(row_at(o, first, second) * blk, blk)
        vec = jnp.concatenate(split(proj[pl.ds(at, blk), :]), axis=0)
        wide = jnp.dot(vec, spread[o], preferred_element_type=F32)
        wide = jnp.concatenate(
            [wide[:blk, : 8 * blk], wide[:blk, 8 * blk :], wide[blk:, : 8 * blk], wide[blk:, 8 * blk :]], axis=0
        )
        wide = jnp.where(own, wide, 0.0).astype(BF16)
        hi, lo = split(
            jnp.concatenate([held[pl.ds(at, blk), 2 * o + c].reshape(8 * blk, 128) for c in (0, 1)], axis=1)
        )
        main = jnp.dot(wide, hi, preferred_element_type=F32)
        rest = jnp.dot(wide[: 2 * blk], lo, preferred_element_type=F32)
        read = main[: 2 * blk] + (main[2 * blk :] + rest)
        for c in (0, 1):
            for t in (0, 1):
                part[o, c, t, first, second] = read[t * blk : (t + 1) * blk, c * 128 : (c + 1) * 128]

    def scatter1(o, t):
        return Scatter(copies, rings1[o], lambda c, a: part.at[o, c, t, a], land1.at[o, t])

    def own_piece(o, c, t):
        return part.at[o, c, t, rings1[o].me, rings2[o].me]

    def send2(o, t):
        s = Direct(copies, rings2[o])
        s.send(lambda b: part.at[o, :, t, rings1[o].me, b], lambda d: land2.at[o, t, d])
        return s

    def finish2(o, t, s):
        s.wait()
        for c in (0, 1):
            piece = own_piece(o, c, t)
            piece[...] = piece[...] + land2[o, t, 0, c] + land2[o, t, 1, c] + land2[o, t, 2, c]

    k1 = [scatter1(o, 0) for o in (0, 1)]
    q1 = [scatter1(o, 1) for o in (0, 1)]

    for j in range(SIDE):
        for o in (0, 1):
            for b in range(SIDE):
                loads[j, o, b].wait()
                read_block(o, order[o][j], b)
            if j == 0 and o == 0:
                pl.semaphore_wait(barrier, len(peers))
            if j == 0:
                k1[o].send_far()
            if j == 2:
                k1[o].send_near()
        if j == 0:
            small1 = Direct(copies, rings1[0])
            small1.send(lambda a: small.at[a], lambda d: small_land1.at[d])

    for s in q1:
        s.send_far()
    small1.wait()
    small[x] = small[x] + small_land1[0] + small_land1[1] + small_land1[2]
    small2 = Direct(copies, rings2[0])
    small2.send(lambda b: small.at[x], lambda d: small_land2.at[d])
    for s in k1:
        s.forward()
    for s in q1:
        s.send_near()

    mine = pl.ds(pl.multiple_of(row * blk, blk), blk)
    own_hid = hid[mine, :]
    chunks = own_hid.shape[1] // 256
    tall = jnp.concatenate([own_hid[:, n * 256 : (n + 1) * 256] for n in range(chunks)], axis=0)
    repeat = (
        lax.broadcasted_iota(jnp.int32, (256, 1024), 1) // 4 == lax.broadcasted_iota(jnp.int32, (256, 1024), 0)
    ).astype(F32).astype(BF16)
    tall = jnp.dot(tall, repeat, preferred_element_type=F32)
    at_head = lax.broadcasted_iota(jnp.int32, (blk, 1024), 1) % 4
    load_weights[0].wait()
    load_weights[1].wait()
    both = jnp.zeros((4 * blk, 256), F32)
    for n in range(chunks):
        piece = tall[n * blk : (n + 1) * blk]
        piece = jnp.concatenate([jnp.where(at_head == h, piece, 0.0).astype(BF16) for h in range(4)], axis=0)
        at = slice(n * 1024, (n + 1) * 1024)
        weights = jnp.concatenate([wv[at, :], wz[at, :]], axis=1)
        both = both + jnp.dot(piece, weights, preferred_element_type=F32)

    for s in q1:
        s.forward()
    for s in k1:
        s.finish()
    k2 = [send2(o, 0) for o in (0, 1)]

    decay_all[...] = jnp.exp(-jnp.exp(decay_log[...]) * softplus(proj[:, 32:36] + dt_bias[...]))
    own_t = lax.broadcasted_iota(jnp.int32, (8 * blk, 3 * blk), 0) // 8 == lax.rem(
        lax.broadcasted_iota(jnp.int32, (8 * blk, 3 * blk), 1), blk
    )
    picks = [
        (
            lax.broadcasted_iota(jnp.int32, (8 * blk, COLS), 1)
            == 16 + 8 * o + lax.broadcasted_iota(jnp.int32, (8 * blk, COLS), 0) % 8
        )
        .astype(F32)
        .astype(BF16)
        for o in (0, 1)
    ]

    def prepare(r, carry):
        at = pl.ds(pl.multiple_of(r * blk, blk), blk)
        hi, lo = split(proj[at, :])
        three = jnp.concatenate([hi.astype(F32), hi.astype(F32), lo.astype(F32)], axis=0).astype(BF16)
        decay = decay_all[at, :]
        for o in (0, 1):
            wide = lax.dot_general(picks[o], three, NT, preferred_element_type=F32)
            lift[r, o] = jnp.where(own_t, wide, 0.0).astype(BF16)
            for c in (0, 1):
                h = 2 * o + c
                keep = jnp.broadcast_to(decay[:, h : h + 1], (blk, 128))
                held[at, h] = keep[:, None, :] * held[at, h]
        return carry

    lax.fori_loop(0, rows // 2, prepare, 0)

    for s in q1:
        s.finish()
    q2 = [send2(o, 1) for o in (0, 1)]

    small2.wait()
    total = small[x] + small_land2[0] + small_land2[1] + small_land2[2]
    scales[...] = jnp.concatenate([total, jnp.zeros((120, 128), F32)], axis=0).T
    raw = scales[pl.ds(pl.multiple_of(z * blk, blk), blk), :]
    q_scale = lax.rsqrt(1.0 + raw[:, 0:2])
    k_scale = lax.rsqrt(1.0 + raw[:, 2:4])
    unit_dot = raw[:, 4:6] * q_scale * k_scale
    decay = decay_all[mine, :]
    beta = 1.0 / (1.0 + jnp.exp(-proj[mine, 36:40]))

    g1 = [
        Gather(
            copies,
            rings1[o],
            lambda c, a, o=o: delta_all.at[o, c, a],
            lambda a, o=o: delta_all.at[o, :, a],
        )
        for o in (0, 1)
    ]
    g2 = []
    deltas = []
    for o in (0, 1):
        finish2(o, 0, k2[o])
        for c in (0, 1):
            h = 2 * o + c
            readk = own_piece(o, c, 0)[...] * k_scale[:, o : o + 1]
            value = both[h * blk : (h + 1) * blk, :128]
            delta = beta[:, h : h + 1] * (value - decay[:, h : h + 1] * readk)
            delta_all[o, c, rings1[o].me, rings2[o].me] = delta * k_scale[:, o : o + 1]
            deltas.append(delta)
        g2.append(Direct(copies, rings2[o]))
        here = delta_all.at[o, :, rings1[o].me, rings2[o].me]
        g2[o].send(lambda b: here, lambda d: here)

    lax.fori_loop(rows // 2, rows, prepare, 0)

    for o in (0, 1):
        finish2(o, 1, q2[o])
        for c in (0, 1):
            h = 2 * o + c
            old = own_piece(o, c, 1)[...] * q_scale[:, o : o + 1]
            readq = decay[:, h : h + 1] * old + unit_dot[:, o : o + 1] * deltas[h]
            meansq = jnp.mean(readq * readq, axis=-1, keepdims=True)
            gate = both[h * blk : (h + 1) * blk, 128:]
            gate = gate / (1.0 + jnp.exp(-gate))
            normed[:, h * 128 : (h + 1) * 128] = (readq * lax.rsqrt(meansq + 0.5) * gain[...] * gate).astype(BF16)

    load_weights[2].wait()
    width = outs.shape[-1]
    for n in range(HEADS):
        outs[n] = jnp.dot(normed[...], w_out[:, n * width : (n + 1) * width], preferred_element_type=F32)
    out_copies = []
    for d in range(1, HEADS):
        to = lax.rem(head + d, HEADS)
        out_copies.append(copies.start(outs.at[to], outs_land.at[head], {"head": to}))
    outs_land[head] = outs[head]

    for o in (0, 1):
        g2[o].wait()
        g1[o].send()

    def update(o, first, second):
        r = row_at(o, first, second)
        at = pl.ds(pl.multiple_of(r * blk, blk), blk)
        hi, lo = split(jnp.concatenate([delta_all[o, c, first, second] for c in (0, 1)], axis=1))
        add = jnp.dot(lift[r, o], jnp.concatenate([hi, lo, hi], axis=0), preferred_element_type=F32)
        for c in (0, 1):
            h = 2 * o + c
            held[at, h] = held[at, h] + add[:, c * 128 : (c + 1) * 128].reshape(blk, 8, 128)

    def update_rows(o, first):
        def body(b, carry):
            update(o, first, b)
            return carry

        lax.fori_loop(0, SIDE, body, 0)

    for o in (0, 1):
        update_rows(o, rings1[o].me)
    for o in (0, 1):
        g1[o].forward()
    for o in (0, 1):
        update_rows(o, rings1[o].left)
        update_rows(o, rings1[o].right)
    for copy in out_copies:
        copy.wait_recv()
    total_out = outs_land[0]
    for n in range(1, HEADS):
        total_out = total_out + outs_land[n]
    layer_out[...] = total_out.astype(BF16)
    for o in (0, 1):
        g1[o].finish()
        update_rows(o, rings1[o].far)
    for copy in copies.made:
        copy.wait_send()


def local(
    hidden_in,
    w_query,
    w_key,
    w_value,
    w_zgate,
    w_decay,
    w_beta,
    decay_log,
    dt_bias,
    norm_gain,
    w_out,
    state,
):
    seqs, width = hidden_in.shape
    rows = SIDE * SIDE
    blk = seqs // rows
    vmem = pl.BlockSpec(memory_space=pltpu.VMEM)
    anywhere = pl.BlockSpec(memory_space=pltpu.HBM)
    n_copies = 2 * 3 + 4 * 6 + 4 * 3 + 2 * 3 + 2 * 4 + HEADS - 1
    return pl.pallas_call(
        exchange_kernel,
        out_shape=(
            jax.ShapeDtypeStruct((blk, 256), BF16),
            pltpu.VMEM(state.shape, F32),
        ),
        in_specs=[vmem] * 7 + [anywhere] * 5,
        out_specs=(vmem, vmem),
        scratch_shapes=[
            pltpu.VMEM((seqs, width), BF16),
            pltpu.VMEM((4 * width, 128), BF16),
            pltpu.VMEM((4 * width, 128), BF16),
            pltpu.VMEM((512, width), BF16),
            pltpu.VMEM((seqs, COLS), F32),
            pltpu.VMEM((seqs, 4), F32),
            pltpu.VMEM((2, COLS, 512), BF16),
            pltpu.VMEM((2, 2, 2, SIDE, SIDE, blk, 128), F32),
            pltpu.VMEM((2, 2, 2, 3, SIDE, blk, 128), F32),
            pltpu.VMEM((2, 2, 3, 2, blk, 128), F32),
            pltpu.VMEM((2, 2, SIDE, SIDE, blk, 128), F32),
            pltpu.VMEM((rows, 2, 8 * blk, 3 * blk), BF16),
            pltpu.VMEM((SIDE, 8, 128), F32),
            pltpu.VMEM((3, 8, 128), F32),
            pltpu.VMEM((3, 8, 128), F32),
            pltpu.VMEM((128, 128), F32),
            pltpu.VMEM((blk, 512), BF16),
            pltpu.VMEM((HEADS, blk, 256), F32),
            pltpu.VMEM((HEADS, blk, 256), F32),
            pltpu.SemaphoreType.DMA((32,)),
            pltpu.SemaphoreType.DMA((4,)),
            pltpu.SemaphoreType.DMA((n_copies,)),
            pltpu.SemaphoreType.DMA((n_copies,)),
        ],
        compiler_params=pltpu.CompilerParams(
            collective_id=0, has_side_effects=True, vmem_limit_bytes=36 * 1024 * 1024
        ),
        name="exchange",
    )(
        *(
            pltpu.with_memory_space_constraint(operand, pltpu.HBM)
            for operand in (
                jnp.transpose(w_query, (1, 2, 0)),
                jnp.transpose(w_key, (1, 2, 0)),
                jnp.transpose(w_decay, (1, 0)),
                jnp.transpose(w_beta, (1, 0)),
                decay_log.reshape(1, 4),
                dt_bias.reshape(1, 4),
                norm_gain.reshape(1, 128),
                hidden_in,
                w_value.reshape(4 * width, 128),
                w_zgate.reshape(4 * width, 128),
                w_out.reshape(512, width),
                state,
            )
        )
    )


def solution(mesh):
    in_specs = (
        P(),
        P(None, "head", "row"),
        P(None, "head", "row"),
        P(None, "head", None),
        P(None, "head", None),
        P(None, "head"),
        P(None, "head"),
        P("head"),
        P("head"),
        P(),
        P("head", None, None),
        P(None, "head", "row", None),
    )
    out_specs = (P("row", "head"), P(None, "head", "row", None))
    return jax.shard_map(local, mesh=mesh, in_specs=in_specs, out_specs=out_specs, check_vma=False)
```

```python
import functools

import jax
import jax.numpy as jnp
from jax import lax
from jax.experimental import pallas as pl
from jax.experimental.pallas import tpu as pltpu
from jax.sharding import PartitionSpec as P

F32 = jnp.float32
BF16 = jnp.bfloat16
NT = (((1,), (1,)), ((), ()))
SIDE = 4
COLS = 40
HEADS = 8


def softplus(x):
    return jnp.maximum(x, 0.0) + jnp.log1p(jnp.exp(-jnp.abs(x)))


class Copies:
    def __init__(self, send, recv):
        self.send, self.recv, self.made = send, recv, []

    def start(self, src, dst, peer):
        n = len(self.made)
        copy = pltpu.make_async_remote_copy(
            src_ref=src,
            dst_ref=dst,
            send_sem=self.send.at[n],
            recv_sem=self.recv.at[n],
            device_id=peer,
            device_id_type=pl.DeviceIdType.MESH,
        )
        copy.start()
        self.made.append(copy)
        return copy


class Ring:
    def __init__(self, me, row_of):
        self.me = me
        self.right = lax.rem(me + 1, SIDE)
        self.far = lax.rem(me + 2, SIDE)
        self.left = lax.rem(me + 3, SIDE)
        self.to_right = {"row": row_of(self.right)}
        self.to_far = {"row": row_of(self.far)}
        self.to_left = {"row": row_of(self.left)}


class Scatter:
    def __init__(self, copies, ring, part, land):
        self.copies, self.ring, self.part, self.land = copies, ring, part, land

    def send_far(self):
        r = self.ring
        self.relay = [
            self.copies.start(self.part(0, r.far), self.land.at[0, 0], r.to_left),
            self.copies.start(self.part(1, r.far), self.land.at[1, 0], r.to_right),
        ]

    def send_near(self):
        r = self.ring
        self.direct = [
            self.copies.start(self.part(0, r.right), self.land.at[0, 1], r.to_right),
            self.copies.start(self.part(1, r.left), self.land.at[1, 1], r.to_left),
        ]

    def forward(self):
        r = self.ring
        self.joint = []
        for half, to, peer in ((0, r.left, r.to_left), (1, r.right, r.to_right)):
            self.relay[half].wait_recv()
            piece = self.part(half, to)
            piece[...] = piece[...] + self.land[half, 0]
            self.joint.append(self.copies.start(piece, self.land.at[half, 2], peer))

    def finish(self):
        for half in (0, 1):
            self.direct[half].wait_recv()
            self.joint[half].wait_recv()
            piece = self.part(half, self.ring.me)
            piece[...] = piece[...] + self.land[half, 1] + self.land[half, 2]


class Direct:
    def __init__(self, copies, ring):
        self.copies, self.ring, self.sent = copies, ring, []

    def send(self, src, dst):
        r = self.ring
        for d, (at, peer) in enumerate(((r.far, r.to_far), (r.right, r.to_right), (r.left, r.to_left))):
            self.sent.append(self.copies.start(src(at), dst(d), peer))

    def wait(self):
        for copy in self.sent:
            copy.wait_recv()


class Gather:
    def __init__(self, copies, ring, part, both):
        self.copies, self.ring, self.part, self.both = copies, ring, part, both

    def send(self):
        r = self.ring
        mine = self.both(r.me)
        self.near = [
            self.copies.start(mine, mine, r.to_right),
            self.copies.start(mine, mine, r.to_left),
        ]

    def forward(self):
        r = self.ring
        self.far = []
        for n, (half, at, peer) in enumerate(((0, r.left, r.to_right), (1, r.right, r.to_left))):
            self.near[n].wait_recv()
            piece = self.part(half, at)
            self.far.append(self.copies.start(piece, piece, peer))

    def finish(self):
        for copy in self.far:
            copy.wait_recv()


def split(x):
    hi = x.astype(BF16)
    return hi, (x - hi.astype(F32)).astype(BF16)


def exchange_kernel(
    wq_hbm,
    wk_hbm,
    wd_hbm,
    wb_hbm,
    decay_log,
    dt_bias,
    gain,
    hid_hbm,
    wv_hbm,
    wz_hbm,
    w_out_hbm,
    state,
    layer_out,
    held,
    wq,
    wk,
    wd,
    wb,
    hid,
    wv,
    wz,
    w_out,
    proj,
    decay_all,
    spread,
    part,
    land1,
    land2,
    delta_all,
    lift,
    small,
    small_land1,
    small_land2,
    scales,
    normed,
    outs,
    outs_land,
    load_sem,
    weight_sem,
    send_sem,
    recv_sem,
):
    row = lax.axis_index("row")
    head = lax.axis_index("head")
    x, z = row // SIDE, lax.rem(row, SIDE)
    rows = SIDE * SIDE
    blk = held.shape[0] // rows

    barrier = pltpu.get_barrier_semaphore()
    peers = []
    for d in (1, 2, 3):
        peers.append({"row": lax.rem(x + d, SIDE) * SIDE + z})
        peers.append({"row": x * SIDE + lax.rem(z + d, SIDE)})
    for d in range(1, HEADS):
        peers.append({"head": lax.rem(head + d, HEADS)})
    for peer in peers:
        pl.semaphore_signal(barrier, inc=1, device_id=peer, device_id_type=pl.DeviceIdType.MESH)

    def row_at(o, first, second):
        return first * SIDE + second if o == 0 else second * SIDE + first

    rings1 = [
        Ring(x, lambda a: row_at(0, a, z)),
        Ring(z, lambda a: row_at(1, a, x)),
    ]
    rings2 = [
        Ring(z, lambda b: row_at(0, x, b)),
        Ring(x, lambda b: row_at(1, z, b)),
    ]
    order = [[r.far, r.right, r.left, r.me] for r in rings1]

    first = []
    small_weights = ((wq_hbm, wq), (wk_hbm, wk), (wd_hbm, wd), (wb_hbm, wb))
    quarter = hid.shape[0] // 4
    pieces = tuple((hid_hbm.at[pl.ds(n * quarter, quarter)], hid.at[pl.ds(n * quarter, quarter)]) for n in range(4))
    for n, (src, dst) in enumerate(small_weights + pieces):
        first.append(pltpu.make_async_copy(src, dst, weight_sem.at[n]))
        first[-1].start()
    loads = {}
    for j in range(SIDE):
        for o in (0, 1):
            for b in range(SIDE):
                n = (j * 2 + o) * SIDE + b
                at = row_at(o, order[o][j], b) * blk
                loads[j, o, b] = pltpu.make_async_copy(
                    state.at[pl.ds(at, blk), pl.ds(2 * o, 2)],
                    held.at[pl.ds(at, blk), pl.ds(2 * o, 2)],
                    load_sem.at[n],
                )
                if j == 0:
                    loads[j, o, b].start()

    col = lax.broadcasted_iota(jnp.int32, (COLS, 512), 0)
    lane = lax.broadcasted_iota(jnp.int32, (COLS, 512), 1)
    for hk in (0, 1):
        base = jnp.where(lane < 256, 16, 0) + 8 * hk
        spread[hk] = (col == base + lane % 8).astype(F32).astype(BF16)
    for copy in first:
        copy.wait()
    for j in (1, 2, 3):
        for o in (0, 1):
            for b in range(SIDE):
                loads[j, o, b].start()
    w = jnp.concatenate(
        [
            wq[0].astype(F32),
            wq[1].astype(F32),
            wk[0].astype(F32),
            wk[1].astype(F32),
            wd[...].astype(F32),
            wb[...].astype(F32),
        ],
        axis=0,
    ).astype(BF16)
    proj[...] = lax.dot_general(hid[...], w, NT, preferred_element_type=F32)

    copies = Copies(send_sem, recv_sem)
    own_lane = lax.broadcasted_iota(jnp.int32, (4 * blk, 8 * blk), 1) // 8
    own_row = lax.rem(lax.broadcasted_iota(jnp.int32, (4 * blk, 8 * blk), 0), blk)
    own = own_lane == own_row

    def read_block(o, first, second):
        at = pl.multiple_of(row_at(o, first, second) * blk, blk)
        vec = jnp.concatenate(split(proj[pl.ds(at, blk), :]), axis=0)
        wide = jnp.dot(vec, spread[o], preferred_element_type=F32)
        wide = jnp.concatenate(
            [wide[:blk, : 8 * blk], wide[:blk, 8 * blk :], wide[blk:, : 8 * blk], wide[blk:, 8 * blk :]], axis=0
        )
        wide = jnp.where(own, wide, 0.0).astype(BF16)
        hi, lo = split(
            jnp.concatenate([held[pl.ds(at, blk), 2 * o + c].reshape(8 * blk, 128) for c in (0, 1)], axis=1)
        )
        main = jnp.dot(wide, hi, preferred_element_type=F32)
        rest = jnp.dot(wide[: 2 * blk], lo, preferred_element_type=F32)
        read = main[: 2 * blk] + (main[2 * blk :] + rest)
        for c in (0, 1):
            for t in (0, 1):
                part[o, c, t, first, second] = read[t * blk : (t + 1) * blk, c * 128 : (c + 1) * 128]

    def scatter1(o, t):
        return Scatter(copies, rings1[o], lambda c, a: part.at[o, c, t, a], land1.at[o, t])

    def own_piece(o, c, t):
        return part.at[o, c, t, rings1[o].me, rings2[o].me]

    def send2(o, t):
        s = Direct(copies, rings2[o])
        s.send(lambda b: part.at[o, :, t, rings1[o].me, b], lambda d: land2.at[o, t, d])
        return s

    def finish2(o, t, s):
        s.wait()
        for c in (0, 1):
            piece = own_piece(o, c, t)
            piece[...] = piece[...] + land2[o, t, 0, c] + land2[o, t, 1, c] + land2[o, t, 2, c]

    k1 = [scatter1(o, 0) for o in (0, 1)]
    q1 = [scatter1(o, 1) for o in (0, 1)]

    for j in range(SIDE):
        for o in (0, 1):
            for b in range(SIDE):
                loads[j, o, b].wait()
            if j == 0:
                for b in range(SIDE):
                    read_block(o, order[o][j], b)
                if o == 0:
                    pl.semaphore_wait(barrier, len(peers))
                k1[o].send_far()
        if j > 0:
            for o in (0, 1):
                for b in range(SIDE):
                    read_block(o, order[o][j], b)
        if j == 2:
            for o in (0, 1):
                k1[o].send_near()
    for s in q1:
        s.send_far()
    load_weights = []
    for n, (src, dst) in enumerate(((wv_hbm, wv), (wz_hbm, wz), (w_out_hbm, w_out))):
        load_weights.append(pltpu.make_async_copy(src, dst, weight_sem.at[n + 8]))
        load_weights[-1].start()

    q, k = proj[:, 0:16], proj[:, 16:32]
    sums = 0.0
    for n, product in enumerate((q * q, k * k, q * k)):
        seg = (
            lax.broadcasted_iota(jnp.int32, (8, 16), 1) // 8 + 2 * n == lax.broadcasted_iota(jnp.int32, (8, 16), 0)
        ).astype(F32)
        sums = sums + lax.dot_general(
            seg, product, NT, precision=lax.Precision.HIGHEST, preferred_element_type=F32
        )
    for a in range(SIDE):
        small[a] = sums[:, a * 128 : (a + 1) * 128]

    small1 = Direct(copies, rings1[0])
    small1.send(lambda a: small.at[a], lambda d: small_land1.at[d])
    for s in k1:
        s.forward()
    for s in q1:
        s.send_near()

    mine = pl.ds(pl.multiple_of(row * blk, blk), blk)
    own_hid = hid[mine, :]
    chunks = own_hid.shape[1] // 256
    tall = jnp.concatenate([own_hid[:, n * 256 : (n + 1) * 256] for n in range(chunks)], axis=0)
    repeat = (
        lax.broadcasted_iota(jnp.int32, (256, 1024), 1) // 4 == lax.broadcasted_iota(jnp.int32, (256, 1024), 0)
    ).astype(F32).astype(BF16)
    tall = jnp.dot(tall, repeat, preferred_element_type=F32)
    at_head = lax.broadcasted_iota(jnp.int32, (blk, 1024), 1) % 4
    load_weights[0].wait()
    load_weights[1].wait()
    both = jnp.zeros((4 * blk, 256), F32)
    for n in range(chunks):
        piece = tall[n * blk : (n + 1) * blk]
        piece = jnp.concatenate([jnp.where(at_head == h, piece, 0.0).astype(BF16) for h in range(4)], axis=0)
        at = slice(n * 1024, (n + 1) * 1024)
        weights = jnp.concatenate([wv[at, :], wz[at, :]], axis=1)
        both = both + jnp.dot(piece, weights, preferred_element_type=F32)

    small1.wait()
    small[x] = small[x] + small_land1[0] + small_land1[1] + small_land1[2]
    small2 = Direct(copies, rings2[0])
    small2.send(lambda b: small.at[x], lambda d: small_land2.at[d])
    for s in q1:
        s.forward()
    for s in k1:
        s.finish()
    k2 = [send2(o, 0) for o in (0, 1)]

    decay_all[...] = jnp.exp(-jnp.exp(decay_log[...]) * softplus(proj[:, 32:36] + dt_bias[...]))
    own_t = lax.broadcasted_iota(jnp.int32, (8 * blk, 3 * blk), 0) // 8 == lax.rem(
        lax.broadcasted_iota(jnp.int32, (8 * blk, 3 * blk), 1), blk
    )
    picks = [
        (
            lax.broadcasted_iota(jnp.int32, (8 * blk, COLS), 1)
            == 16 + 8 * o + lax.broadcasted_iota(jnp.int32, (8 * blk, COLS), 0) % 8
        )
        .astype(F32)
        .astype(BF16)
        for o in (0, 1)
    ]

    def prepare(r, carry):
        at = pl.ds(pl.multiple_of(r * blk, blk), blk)
        hi, lo = split(proj[at, :])
        three = jnp.concatenate([hi.astype(F32), hi.astype(F32), lo.astype(F32)], axis=0).astype(BF16)
        decay = decay_all[at, :]
        for o in (0, 1):
            wide = lax.dot_general(picks[o], three, NT, preferred_element_type=F32)
            lift[r, o] = jnp.where(own_t, wide, 0.0).astype(BF16)
            for c in (0, 1):
                h = 2 * o + c
                keep = jnp.broadcast_to(decay[:, h : h + 1], (blk, 128))
                held[at, h] = keep[:, None, :] * held[at, h]
        return carry

    lax.fori_loop(0, rows // 2, prepare, 0)

    for s in q1:
        s.finish()
    q2 = [send2(o, 1) for o in (0, 1)]

    small2.wait()
    total = small[x] + small_land2[0] + small_land2[1] + small_land2[2]
    scales[...] = jnp.concatenate([total, jnp.zeros((120, 128), F32)], axis=0).T
    raw = scales[pl.ds(pl.multiple_of(z * blk, blk), blk), :]
    q_scale = lax.rsqrt(1.0 + raw[:, 0:2])
    k_scale = lax.rsqrt(1.0 + raw[:, 2:4])
    unit_dot = raw[:, 4:6] * q_scale * k_scale
    decay = decay_all[mine, :]
    beta = 1.0 / (1.0 + jnp.exp(-proj[mine, 36:40]))

    def gather1(o, b):
        return Gather(
            copies,
            rings1[o],
            lambda c, a: delta_all.at[o, c, a, b],
            lambda a: delta_all.at[o, :, a, b],
        )

    g1 = {}
    for o in (0, 1):
        r = rings2[o]
        for name, b in (("me", r.me), ("far", r.far), ("left", r.left), ("right", r.right)):
            g1[o, name] = gather1(o, b)
    g2 = []
    deltas = []
    for o in (0, 1):
        finish2(o, 0, k2[o])
        for c in (0, 1):
            h = 2 * o + c
            readk = own_piece(o, c, 0)[...] * k_scale[:, o : o + 1]
            value = both[h * blk : (h + 1) * blk, :128]
            delta = beta[:, h : h + 1] * (value - decay[:, h : h + 1] * readk)
            delta_all[o, c, rings1[o].me, rings2[o].me] = delta * k_scale[:, o : o + 1]
            deltas.append(delta)
        g2.append(Direct(copies, rings2[o]))
        here = delta_all.at[o, :, rings1[o].me, rings2[o].me]
        g2[o].send(lambda b: here, lambda d: here)
        g1[o, "me"].send()

    lax.fori_loop(rows // 2, rows, prepare, 0)
    for o in (0, 1):
        for n, name in ((1, "left"), (2, "right")):
            g2[o].sent[n].wait_recv()
            g1[o, name].send()
    for o in (0, 1):
        g1[o, "me"].forward()
        g2[o].sent[0].wait_recv()
        g1[o, "far"].send()

    for o in (0, 1):
        finish2(o, 1, q2[o])
        for c in (0, 1):
            h = 2 * o + c
            old = own_piece(o, c, 1)[...] * q_scale[:, o : o + 1]
            readq = decay[:, h : h + 1] * old + unit_dot[:, o : o + 1] * deltas[h]
            meansq = jnp.mean(readq * readq, axis=-1, keepdims=True)
            gate = both[h * blk : (h + 1) * blk, 128:]
            gate = gate / (1.0 + jnp.exp(-gate))
            normed[:, h * 128 : (h + 1) * 128] = (readq * lax.rsqrt(meansq + 0.5) * gain[...] * gate).astype(BF16)

    load_weights[2].wait()
    width = outs.shape[-1]
    for n in range(HEADS):
        outs[n] = jnp.dot(normed[...], w_out[:, n * width : (n + 1) * width], preferred_element_type=F32)
    out_copies = []
    for d in range(1, HEADS):
        to = lax.rem(head + d, HEADS)
        out_copies.append(copies.start(outs.at[to], outs_land.at[head], {"head": to}))
    outs_land[head] = outs[head]

    for o in (0, 1):
        for name in ("left", "right"):
            g1[o, name].forward()

    def update(o, first, second):
        r = row_at(o, first, second)
        at = pl.ds(pl.multiple_of(r * blk, blk), blk)
        hi, lo = split(jnp.concatenate([delta_all[o, c, first, second] for c in (0, 1)], axis=1))
        add = jnp.dot(lift[r, o], jnp.concatenate([hi, lo, hi], axis=0), preferred_element_type=F32)
        for c in (0, 1):
            h = 2 * o + c
            held[at, h] = held[at, h] + add[:, c * 128 : (c + 1) * 128].reshape(blk, 8, 128)

    def update_rows(o, first):
        for b in range(SIDE):
            update(o, first, b)

    for o in (0, 1):
        update_rows(o, rings1[o].me)
    for o in (0, 1):
        g1[o, "far"].forward()
    for o in (0, 1):
        update_rows(o, rings1[o].left)
        update_rows(o, rings1[o].right)
    for copy in out_copies:
        copy.wait_recv()
    total_out = outs_land[0]
    for n in range(1, HEADS):
        total_out = total_out + outs_land[n]
    layer_out[...] = total_out.astype(BF16)
    for g in g1.values():
        g.finish()
    for o in (0, 1):
        update_rows(o, rings1[o].far)
    for copy in copies.made:
        copy.wait_send()


def local(
    hidden_in,
    w_query,
    w_key,
    w_value,
    w_zgate,
    w_decay,
    w_beta,
    decay_log,
    dt_bias,
    norm_gain,
    w_out,
    state,
):
    seqs, width = hidden_in.shape
    rows = SIDE * SIDE
    blk = seqs // rows
    vmem = pl.BlockSpec(memory_space=pltpu.VMEM)
    anywhere = pl.BlockSpec(memory_space=pltpu.HBM)
    n_copies = 2 * 3 + 4 * 6 + 4 * 3 + 2 * 3 + 2 * 4 * 4 + HEADS - 1
    return pl.pallas_call(
        exchange_kernel,
        out_shape=(
            jax.ShapeDtypeStruct((blk, 256), BF16),
            pltpu.VMEM(state.shape, F32),
        ),
        in_specs=[anywhere] * 4 + [vmem] * 3 + [anywhere] * 5,
        out_specs=(vmem, vmem),
        scratch_shapes=[
            pltpu.VMEM((2, 8, width), BF16),
            pltpu.VMEM((2, 8, width), BF16),
            pltpu.VMEM((4, width), BF16),
            pltpu.VMEM((4, width), BF16),
            pltpu.VMEM((seqs, width), BF16),
            pltpu.VMEM((4 * width, 128), BF16),
            pltpu.VMEM((4 * width, 128), BF16),
            pltpu.VMEM((512, width), BF16),
            pltpu.VMEM((seqs, COLS), F32),
            pltpu.VMEM((seqs, 4), F32),
            pltpu.VMEM((2, COLS, 512), BF16),
            pltpu.VMEM((2, 2, 2, SIDE, SIDE, blk, 128), F32),
            pltpu.VMEM((2, 2, 2, 3, SIDE, blk, 128), F32),
            pltpu.VMEM((2, 2, 3, 2, blk, 128), F32),
            pltpu.VMEM((2, 2, SIDE, SIDE, blk, 128), F32),
            pltpu.VMEM((rows, 2, 8 * blk, 3 * blk), BF16),
            pltpu.VMEM((SIDE, 8, 128), F32),
            pltpu.VMEM((3, 8, 128), F32),
            pltpu.VMEM((3, 8, 128), F32),
            pltpu.VMEM((128, 128), F32),
            pltpu.VMEM((blk, 512), BF16),
            pltpu.VMEM((HEADS, blk, 256), F32),
            pltpu.VMEM((HEADS, blk, 256), F32),
            pltpu.SemaphoreType.DMA((32,)),
            pltpu.SemaphoreType.DMA((11,)),
            pltpu.SemaphoreType.DMA((n_copies,)),
            pltpu.SemaphoreType.DMA((n_copies,)),
        ],
        compiler_params=pltpu.CompilerParams(
            collective_id=0, has_side_effects=True, vmem_limit_bytes=36 * 1024 * 1024
        ),
        name="exchange",
    )(
        *(
            pltpu.with_memory_space_constraint(operand, pltpu.HBM)
            for operand in (
                jnp.transpose(w_query, (1, 2, 0)),
                jnp.transpose(w_key, (1, 2, 0)),
                jnp.transpose(w_decay, (1, 0)),
                jnp.transpose(w_beta, (1, 0)),
                decay_log.reshape(1, 4),
                dt_bias.reshape(1, 4),
                norm_gain.reshape(1, 128),
                hidden_in,
                w_value.reshape(4 * width, 128),
                w_zgate.reshape(4 * width, 128),
                w_out.reshape(512, width),
                state,
            )
        )
    )


def solution(mesh):
    in_specs = (
        P(),
        P(None, "head", "row"),
        P(None, "head", "row"),
        P(None, "head", None),
        P(None, "head", None),
        P(None, "head"),
        P(None, "head"),
        P("head"),
        P("head"),
        P(),
        P("head", None, None),
        P(None, "head", "row", None),
    )
    out_specs = (P("row", "head"), P(None, "head", "row", None))
    return jax.shard_map(local, mesh=mesh, in_specs=in_specs, out_specs=out_specs, check_vma=False)
```

```python
import functools

import jax
import jax.numpy as jnp
from jax import lax
from jax.experimental import pallas as pl
from jax.experimental.pallas import tpu as pltpu
from jax.sharding import PartitionSpec as P

F32 = jnp.float32
BF16 = jnp.bfloat16
NT = (((1,), (1,)), ((), ()))
SIDE = 4
COLS = 40
HEADS = 8


def softplus(x):
    return jnp.maximum(x, 0.0) + jnp.log1p(jnp.exp(-jnp.abs(x)))


class Copies:
    def __init__(self, send, recv):
        self.send, self.recv, self.made = send, recv, []

    def start(self, src, dst, peer):
        n = len(self.made)
        copy = pltpu.make_async_remote_copy(
            src_ref=src,
            dst_ref=dst,
            send_sem=self.send.at[n],
            recv_sem=self.recv.at[n],
            device_id=peer,
            device_id_type=pl.DeviceIdType.MESH,
        )
        copy.start()
        self.made.append(copy)
        return copy


class Ring:
    def __init__(self, me, row_of):
        self.me = me
        self.right = lax.rem(me + 1, SIDE)
        self.far = lax.rem(me + 2, SIDE)
        self.left = lax.rem(me + 3, SIDE)
        self.to_right = {"row": row_of(self.right)}
        self.to_far = {"row": row_of(self.far)}
        self.to_left = {"row": row_of(self.left)}


class Scatter:
    def __init__(self, copies, ring, part, land):
        self.copies, self.ring, self.part, self.land = copies, ring, part, land

    def send_far(self):
        r = self.ring
        self.relay = [
            self.copies.start(self.part(0, r.far), self.land.at[0, 0], r.to_left),
            self.copies.start(self.part(1, r.far), self.land.at[1, 0], r.to_right),
        ]

    def send_right(self):
        r = self.ring
        self.direct = [self.copies.start(self.part(0, r.right), self.land.at[0, 1], r.to_right)]

    def send_left(self):
        r = self.ring
        self.direct.append(self.copies.start(self.part(1, r.left), self.land.at[1, 1], r.to_left))

    def forward(self):
        r = self.ring
        self.joint = []
        for half, to, peer in ((0, r.left, r.to_left), (1, r.right, r.to_right)):
            self.relay[half].wait_recv()
            piece = self.part(half, to)
            piece[...] = piece[...] + self.land[half, 0]
            self.joint.append(self.copies.start(piece, self.land.at[half, 2], peer))

    def finish(self):
        for half in (0, 1):
            self.direct[half].wait_recv()
            self.joint[half].wait_recv()
            piece = self.part(half, self.ring.me)
            piece[...] = piece[...] + self.land[half, 1] + self.land[half, 2]


class Direct:
    def __init__(self, copies, ring):
        self.copies, self.ring, self.sent = copies, ring, []

    def send(self, src, dst):
        r = self.ring
        for d, (at, peer) in enumerate(((r.far, r.to_far), (r.right, r.to_right), (r.left, r.to_left))):
            self.sent.append(self.copies.start(src(at), dst(d), peer))

    def wait(self):
        for copy in self.sent:
            copy.wait_recv()


class Gather:
    def __init__(self, copies, ring, part, both):
        self.copies, self.ring, self.part, self.both = copies, ring, part, both

    def send(self):
        r = self.ring
        mine = self.both(r.me)
        self.near = [
            self.copies.start(mine, mine, r.to_right),
            self.copies.start(mine, mine, r.to_left),
        ]

    def forward(self):
        r = self.ring
        self.far = []
        for n, (half, at, peer) in enumerate(((0, r.left, r.to_right), (1, r.right, r.to_left))):
            self.near[n].wait_recv()
            piece = self.part(half, at)
            self.far.append(self.copies.start(piece, piece, peer))

    def finish(self):
        for copy in self.far:
            copy.wait_recv()


def split(x):
    hi = x.astype(BF16)
    return hi, (x - hi.astype(F32)).astype(BF16)


def growth(delta_all, lift, o, first, second, r):
    hi, lo = split(jnp.concatenate([delta_all[o, c, first, second] for c in (0, 1)], axis=1))
    add = jnp.dot(lift[r, o], jnp.concatenate([hi, lo, hi], axis=0), preferred_element_type=F32)
    return [add[:, c * 128 : (c + 1) * 128].reshape(hi.shape[0], 8, 128) for c in (0, 1)]


def exchange_kernel(
    wq_hbm,
    wk_hbm,
    wd_hbm,
    wb_hbm,
    decay_log,
    dt_bias,
    gain,
    hid_hbm,
    wv_hbm,
    wz_hbm,
    w_out_hbm,
    state,
    held,
    delta_all,
    lift,
    outs_land,
    wq,
    wk,
    wd,
    wb,
    hid,
    wv,
    wz,
    w_out,
    proj,
    decay_all,
    spread,
    part,
    land1,
    land2,
    small,
    small_land1,
    small_land2,
    scales,
    normed,
    outs,
    load_sem,
    weight_sem,
    send_sem,
    recv_sem,
):
    row = lax.axis_index("row")
    head = lax.axis_index("head")
    x, z = row // SIDE, lax.rem(row, SIDE)
    rows = SIDE * SIDE
    blk = held.shape[0] // rows

    barrier = pltpu.get_barrier_semaphore()
    peers = []
    for d in (1, 2, 3):
        peers.append({"row": lax.rem(x + d, SIDE) * SIDE + z})
        peers.append({"row": x * SIDE + lax.rem(z + d, SIDE)})
    for d in range(1, HEADS):
        peers.append({"head": lax.rem(head + d, HEADS)})
    for peer in peers:
        pl.semaphore_signal(barrier, inc=1, device_id=peer, device_id_type=pl.DeviceIdType.MESH)

    def row_at(o, first, second):
        return first * SIDE + second if o == 0 else second * SIDE + first

    rings1 = [
        Ring(x, lambda a: row_at(0, a, z)),
        Ring(z, lambda a: row_at(1, a, x)),
    ]
    rings2 = [
        Ring(z, lambda b: row_at(0, x, b)),
        Ring(x, lambda b: row_at(1, z, b)),
    ]
    order = [[r.far, r.right, r.left, r.me] for r in rings1]

    first = []
    small_weights = ((wq_hbm, wq), (wk_hbm, wk), (wd_hbm, wd), (wb_hbm, wb))
    quarter = hid.shape[0] // 4
    pieces = tuple((hid_hbm.at[pl.ds(n * quarter, quarter)], hid.at[pl.ds(n * quarter, quarter)]) for n in range(4))
    for n, (src, dst) in enumerate(small_weights + pieces):
        first.append(pltpu.make_async_copy(src, dst, weight_sem.at[n]))
        first[-1].start()
    loads = {}
    for j in range(SIDE):
        for o in (0, 1):
            for b in range(SIDE):
                n = (j * 2 + o) * SIDE + b
                at = row_at(o, order[o][j], b) * blk
                loads[j, o, b] = pltpu.make_async_copy(
                    state.at[pl.ds(at, blk), pl.ds(2 * o, 2)],
                    held.at[pl.ds(at, blk), pl.ds(2 * o, 2)],
                    load_sem.at[n],
                )

    col = lax.broadcasted_iota(jnp.int32, (COLS, 512), 0)
    lane = lax.broadcasted_iota(jnp.int32, (COLS, 512), 1)
    for hk in (0, 1):
        base = jnp.where(lane < 256, 16, 0) + 8 * hk
        spread[hk] = (col == base + lane % 8).astype(F32).astype(BF16)
    for copy in first[:5]:
        copy.wait()
    for o in (0, 1):
        for b in range(SIDE):
            loads[0, o, b].start()
    w = jnp.concatenate(
        [
            wq[0].astype(F32),
            wq[1].astype(F32),
            wk[0].astype(F32),
            wk[1].astype(F32),
            wd[...].astype(F32),
            wb[...].astype(F32),
        ],
        axis=0,
    ).astype(BF16)
    for n in range(4):
        if n > 0:
            first[4 + n].wait()
        if n == 2:
            for o in (0, 1):
                for b in range(SIDE):
                    loads[1, o, b].start()
        at = pl.ds(n * quarter, quarter)
        proj[at, :] = lax.dot_general(hid[at, :], w, NT, preferred_element_type=F32)
    for j in (2, 3):
        for o in (0, 1):
            for b in range(SIDE):
                loads[j, o, b].start()

    copies = Copies(send_sem, recv_sem)
    own_lane = lax.broadcasted_iota(jnp.int32, (4 * blk, 8 * blk), 1) // 8
    own_row = lax.rem(lax.broadcasted_iota(jnp.int32, (4 * blk, 8 * blk), 0), blk)
    own = own_lane == own_row

    def read_block(o, first, second):
        at = pl.multiple_of(row_at(o, first, second) * blk, blk)
        vec = jnp.concatenate(split(proj[pl.ds(at, blk), :]), axis=0)
        wide = jnp.dot(vec, spread[o], preferred_element_type=F32)
        wide = jnp.concatenate(
            [wide[:blk, : 8 * blk], wide[:blk, 8 * blk :], wide[blk:, : 8 * blk], wide[blk:, 8 * blk :]], axis=0
        )
        wide = jnp.where(own, wide, 0.0).astype(BF16)
        hi, lo = split(
            jnp.concatenate([held[pl.ds(at, blk), 2 * o + c].reshape(8 * blk, 128) for c in (0, 1)], axis=1)
        )
        main = jnp.dot(wide, hi, preferred_element_type=F32)
        rest = jnp.dot(wide[: 2 * blk], lo, preferred_element_type=F32)
        read = main[: 2 * blk] + (main[2 * blk :] + rest)
        for c in (0, 1):
            for t in (0, 1):
                part[o, c, t, first, second] = read[t * blk : (t + 1) * blk, c * 128 : (c + 1) * 128]

    def scatter1(o, t):
        return Scatter(copies, rings1[o], lambda c, a: part.at[o, c, t, a], land1.at[o, t])

    def own_piece(o, c, t):
        return part.at[o, c, t, rings1[o].me, rings2[o].me]

    def send2(o, t):
        s = Direct(copies, rings2[o])
        s.send(lambda b: part.at[o, :, t, rings1[o].me, b], lambda d: land2.at[o, t, d])
        return s

    def finish2(o, t, s):
        s.wait()
        for c in (0, 1):
            piece = own_piece(o, c, t)
            piece[...] = piece[...] + land2[o, t, 0, c] + land2[o, t, 1, c] + land2[o, t, 2, c]

    k1 = [scatter1(o, 0) for o in (0, 1)]
    q1 = [scatter1(o, 1) for o in (0, 1)]

    for j in range(SIDE):
        for o in (0, 1):
            for b in range(SIDE):
                loads[j, o, b].wait()
            if j == 0:
                for b in range(SIDE):
                    read_block(o, order[o][j], b)
                if o == 0:
                    pl.semaphore_wait(barrier, len(peers))
                k1[o].send_far()
        if j == 0:
            for o in (0, 1):
                q1[o].send_far()
        else:
            for o in (0, 1):
                for b in range(SIDE):
                    read_block(o, order[o][j], b)
        if j == 1:
            for o in (0, 1):
                k1[o].send_right()
        if j == 2:
            for o in (0, 1):
                k1[o].send_left()
    for s in k1:
        s.forward()
    for s in q1:
        s.send_right()
        s.send_left()
    load_weights = []
    for n, (src, dst) in enumerate(((wv_hbm, wv), (wz_hbm, wz), (w_out_hbm, w_out))):
        load_weights.append(pltpu.make_async_copy(src, dst, weight_sem.at[n + 8]))
        load_weights[-1].start()

    q, k = proj[:, 0:16], proj[:, 16:32]
    sums = 0.0
    for n, product in enumerate((q * q, k * k, q * k)):
        seg = (
            lax.broadcasted_iota(jnp.int32, (8, 16), 1) // 8 + 2 * n == lax.broadcasted_iota(jnp.int32, (8, 16), 0)
        ).astype(F32)
        sums = sums + lax.dot_general(
            seg, product, NT, precision=lax.Precision.HIGHEST, preferred_element_type=F32
        )
    for a in range(SIDE):
        small[a] = sums[:, a * 128 : (a + 1) * 128]

    small1 = Direct(copies, rings1[0])
    small1.send(lambda a: small.at[a], lambda d: small_land1.at[d])
    for s in q1:
        s.forward()

    mine = pl.ds(pl.multiple_of(row * blk, blk), blk)
    own_hid = hid[mine, :]
    chunks = own_hid.shape[1] // 256
    tall = jnp.concatenate([own_hid[:, n * 256 : (n + 1) * 256] for n in range(chunks)], axis=0)
    repeat = (
        lax.broadcasted_iota(jnp.int32, (256, 1024), 1) // 4 == lax.broadcasted_iota(jnp.int32, (256, 1024), 0)
    ).astype(F32).astype(BF16)
    tall = jnp.dot(tall, repeat, preferred_element_type=F32)
    at_head = lax.broadcasted_iota(jnp.int32, (blk, 1024), 1) % 4
    load_weights[0].wait()
    load_weights[1].wait()
    both = jnp.zeros((4 * blk, 256), F32)
    for n in range(chunks):
        piece = tall[n * blk : (n + 1) * blk]
        piece = jnp.concatenate([jnp.where(at_head == h, piece, 0.0).astype(BF16) for h in range(4)], axis=0)
        at = slice(n * 1024, (n + 1) * 1024)
        weights = jnp.concatenate([wv[at, :], wz[at, :]], axis=1)
        both = both + jnp.dot(piece, weights, preferred_element_type=F32)

    small1.wait()
    small[x] = small[x] + small_land1[0] + small_land1[1] + small_land1[2]
    small2 = Direct(copies, rings2[0])
    small2.send(lambda b: small.at[x], lambda d: small_land2.at[d])
    for s in k1:
        s.finish()
    k2 = [send2(o, 0) for o in (0, 1)]

    decay_all[...] = jnp.exp(-jnp.exp(decay_log[...]) * softplus(proj[:, 32:36] + dt_bias[...]))
    own_t = lax.broadcasted_iota(jnp.int32, (8 * blk, 3 * blk), 0) // 8 == lax.rem(
        lax.broadcasted_iota(jnp.int32, (8 * blk, 3 * blk), 1), blk
    )
    picks = [
        (
            lax.broadcasted_iota(jnp.int32, (8 * blk, COLS), 1)
            == 16 + 8 * o + lax.broadcasted_iota(jnp.int32, (8 * blk, COLS), 0) % 8
        )
        .astype(F32)
        .astype(BF16)
        for o in (0, 1)
    ]

    def prepare(r, carry):
        at = pl.ds(pl.multiple_of(r * blk, blk), blk)
        hi, lo = split(proj[at, :])
        three = jnp.concatenate([hi.astype(F32), hi.astype(F32), lo.astype(F32)], axis=0).astype(BF16)
        decay = decay_all[at, :]
        for o in (0, 1):
            wide = lax.dot_general(picks[o], three, NT, preferred_element_type=F32)
            lift[r, o] = jnp.where(own_t, wide, 0.0).astype(BF16)
            for c in (0, 1):
                h = 2 * o + c
                keep = jnp.broadcast_to(decay[:, h : h + 1], (blk, 128))
                held[at, h] = keep[:, None, :] * held[at, h]
        return carry

    lax.fori_loop(0, rows // 2, prepare, 0)

    for s in q1:
        s.finish()
    q2 = [send2(o, 1) for o in (0, 1)]

    small2.wait()
    total = small[x] + small_land2[0] + small_land2[1] + small_land2[2]
    scales[...] = jnp.concatenate([total, jnp.zeros((120, 128), F32)], axis=0).T
    raw = scales[pl.ds(pl.multiple_of(z * blk, blk), blk), :]
    q_scale = lax.rsqrt(1.0 + raw[:, 0:2])
    k_scale = lax.rsqrt(1.0 + raw[:, 2:4])
    unit_dot = raw[:, 4:6] * q_scale * k_scale
    decay = decay_all[mine, :]
    beta = 1.0 / (1.0 + jnp.exp(-proj[mine, 36:40]))

    def gather1(o, b):
        return Gather(
            copies,
            rings1[o],
            lambda c, a: delta_all.at[o, c, a, b],
            lambda a: delta_all.at[o, :, a, b],
        )

    g1 = {}
    for o in (0, 1):
        r = rings2[o]
        for name, b in (("me", r.me), ("far", r.far), ("left", r.left), ("right", r.right)):
            g1[o, name] = gather1(o, b)
    g2 = []
    deltas = []
    for o in (0, 1):
        finish2(o, 0, k2[o])
        for c in (0, 1):
            h = 2 * o + c
            readk = own_piece(o, c, 0)[...] * k_scale[:, o : o + 1]
            value = both[h * blk : (h + 1) * blk, :128]
            delta = beta[:, h : h + 1] * (value - decay[:, h : h + 1] * readk)
            delta_all[o, c, rings1[o].me, rings2[o].me] = delta * k_scale[:, o : o + 1]
            deltas.append(delta)
        g2.append(Direct(copies, rings2[o]))
        here = delta_all.at[o, :, rings1[o].me, rings2[o].me]
        g2[o].send(lambda b: here, lambda d: here)
        g1[o, "me"].send()

    lax.fori_loop(rows // 2, rows, prepare, 0)
    for o in (0, 1):
        finish2(o, 1, q2[o])
        for c in (0, 1):
            h = 2 * o + c
            old = own_piece(o, c, 1)[...] * q_scale[:, o : o + 1]
            readq = decay[:, h : h + 1] * old + unit_dot[:, o : o + 1] * deltas[h]
            meansq = jnp.mean(readq * readq, axis=-1, keepdims=True)
            gate = both[h * blk : (h + 1) * blk, 128:]
            gate = gate / (1.0 + jnp.exp(-gate))
            normed[:, h * 128 : (h + 1) * 128] = (readq * lax.rsqrt(meansq + 0.5) * gain[...] * gate).astype(BF16)

    load_weights[2].wait()
    width = outs.shape[-1]
    for n in range(HEADS):
        outs[n] = jnp.dot(normed[...], w_out[:, n * width : (n + 1) * width], preferred_element_type=F32)
    out_copies = []
    for d in range(1, HEADS):
        to = lax.rem(head + d, HEADS)
        out_copies.append(copies.start(outs.at[to], outs_land.at[head], {"head": to}))
    outs_land[head] = outs[head]

    for o in (0, 1):
        for n, name in ((1, "left"), (2, "right")):
            g2[o].sent[n].wait_recv()
            g1[o, name].send()
    for o in (0, 1):
        g1[o, "me"].forward()
        g2[o].sent[0].wait_recv()
        g1[o, "far"].send()

    for o in (0, 1):
        for name in ("left", "right"):
            g1[o, name].forward()

    def update_rows(o, first):
        for b in range(SIDE):
            r = row_at(o, first, b)
            at = pl.ds(pl.multiple_of(r * blk, blk), blk)
            add = growth(delta_all, lift, o, first, b, r)
            for c in (0, 1):
                h = 2 * o + c
                held[at, h] = held[at, h] + add[c]

    for o in (0, 1):
        update_rows(o, rings1[o].me)
    for o in (0, 1):
        g1[o, "far"].forward()
    for o in (0, 1):
        update_rows(o, rings1[o].left)
        update_rows(o, rings1[o].right)
    for copy in out_copies:
        copy.wait_recv()
    for g in g1.values():
        g.finish()
    for copy in copies.made:
        copy.wait_send()


def finish_kernel(held, delta_all, lift, outs_land, layer_out, new_state, last, sems):
    row = lax.axis_index("row")
    spots = (row // SIDE, lax.rem(row, SIDE))
    blk = held.shape[0] // (SIDE * SIDE)
    made = []

    def store(src, o, r, count=1):
        dst = new_state.at[pl.ds(pl.multiple_of(r * blk, blk), count * blk), pl.ds(2 * o, 2)]
        made.append(pltpu.make_async_copy(src, dst, sems.at[len(made)]))
        made[-1].start()

    for d in (0, 1, 3):
        first = lax.rem(spots[0] + d, SIDE)
        at = pl.ds(pl.multiple_of(first * SIDE * blk, blk), SIDE * blk)
        store(held.at[at, pl.ds(0, 2)], 0, first * SIDE, SIDE)
        for b in range(SIDE):
            r = b * SIDE + lax.rem(spots[1] + d, SIDE)
            store(held.at[pl.ds(pl.multiple_of(r * blk, blk), blk), pl.ds(2, 2)], 1, r)
    for o in (0, 1):
        first = lax.rem(spots[o] + 2, SIDE)
        for b in range(SIDE):
            r = first * SIDE + b if o == 0 else b * SIDE + first
            at = pl.ds(pl.multiple_of(r * blk, blk), blk)
            add = growth(delta_all, lift, o, first, b, r)
            for c in (0, 1):
                last[o * SIDE + b, :, c] = held[at, 2 * o + c] + add[c]
            store(last.at[o * SIDE + b], o, r)
    total = outs_land[0]
    for n in range(1, HEADS):
        total = total + outs_land[n]
    layer_out[...] = total.astype(BF16)
    for copy in made:
        copy.wait()


def local(
    hidden_in,
    w_query,
    w_key,
    w_value,
    w_zgate,
    w_decay,
    w_beta,
    decay_log,
    dt_bias,
    norm_gain,
    w_out,
    state,
):
    seqs, width = hidden_in.shape
    rows = SIDE * SIDE
    blk = seqs // rows
    vmem = pl.BlockSpec(memory_space=pltpu.VMEM)
    anywhere = pl.BlockSpec(memory_space=pltpu.HBM)
    n_copies = 2 * 3 + 4 * 6 + 4 * 3 + 2 * 3 + 2 * 4 * 4 + HEADS - 1
    held, delta_all, lift, outs_land = pl.pallas_call(
        exchange_kernel,
        out_shape=(
            pltpu.VMEM(state.shape, F32),
            pltpu.VMEM((2, 2, SIDE, SIDE, blk, 128), F32),
            pltpu.VMEM((rows, 2, 8 * blk, 3 * blk), BF16),
            pltpu.VMEM((HEADS, blk, 256), F32),
        ),
        in_specs=[anywhere] * 4 + [vmem] * 3 + [anywhere] * 5,
        out_specs=(vmem,) * 4,
        scratch_shapes=[
            pltpu.VMEM((2, 8, width), BF16),
            pltpu.VMEM((2, 8, width), BF16),
            pltpu.VMEM((4, width), BF16),
            pltpu.VMEM((4, width), BF16),
            pltpu.VMEM((seqs, width), BF16),
            pltpu.VMEM((4 * width, 128), BF16),
            pltpu.VMEM((4 * width, 128), BF16),
            pltpu.VMEM((512, width), BF16),
            pltpu.VMEM((seqs, COLS), F32),
            pltpu.VMEM((seqs, 4), F32),
            pltpu.VMEM((2, COLS, 512), BF16),
            pltpu.VMEM((2, 2, 2, SIDE, SIDE, blk, 128), F32),
            pltpu.VMEM((2, 2, 2, 3, SIDE, blk, 128), F32),
            pltpu.VMEM((2, 2, 3, 2, blk, 128), F32),
            pltpu.VMEM((SIDE, 8, 128), F32),
            pltpu.VMEM((3, 8, 128), F32),
            pltpu.VMEM((3, 8, 128), F32),
            pltpu.VMEM((128, 128), F32),
            pltpu.VMEM((blk, 512), BF16),
            pltpu.VMEM((HEADS, blk, 256), F32),
            pltpu.SemaphoreType.DMA((32,)),
            pltpu.SemaphoreType.DMA((11,)),
            pltpu.SemaphoreType.DMA((n_copies,)),
            pltpu.SemaphoreType.DMA((n_copies,)),
        ],
        compiler_params=pltpu.CompilerParams(
            collective_id=0, has_side_effects=True, vmem_limit_bytes=36 * 1024 * 1024
        ),
        name="exchange",
    )(
        *(
            pltpu.with_memory_space_constraint(operand, pltpu.HBM)
            for operand in (
                jnp.transpose(w_query, (1, 2, 0)),
                jnp.transpose(w_key, (1, 2, 0)),
                jnp.transpose(w_decay, (1, 0)),
                jnp.transpose(w_beta, (1, 0)),
                decay_log.reshape(1, 4),
                dt_bias.reshape(1, 4),
                norm_gain.reshape(1, 128),
                hidden_in,
                w_value.reshape(4 * width, 128),
                w_zgate.reshape(4 * width, 128),
                w_out.reshape(512, width),
                state,
            )
        )
    )
    layer_out, new_state = pl.pallas_call(
        finish_kernel,
        out_shape=(
            jax.ShapeDtypeStruct((blk, 256), BF16),
            jax.ShapeDtypeStruct(state.shape, F32),
        ),
        in_specs=[vmem] * 4,
        out_specs=(vmem, anywhere),
        scratch_shapes=[
            pltpu.VMEM((2 * SIDE, blk, 2, 8, 128), F32),
            pltpu.SemaphoreType.DMA((23,)),
        ],
        compiler_params=pltpu.CompilerParams(vmem_limit_bytes=16 * 1024 * 1024),
        name="finish",
    )(*(pltpu.with_memory_space_constraint(a, pltpu.VMEM) for a in (held, delta_all, lift, outs_land)))
    return layer_out, new_state


def solution(mesh):
    in_specs = (
        P(),
        P(None, "head", "row"),
        P(None, "head", "row"),
        P(None, "head", None),
        P(None, "head", None),
        P(None, "head"),
        P(None, "head"),
        P("head"),
        P("head"),
        P(),
        P("head", None, None),
        P(None, "head", "row", None),
    )
    out_specs = (P("row", "head"), P(None, "head", "row", None))
    return jax.shard_map(local, mesh=mesh, in_specs=in_specs, out_specs=out_specs, check_vma=False)
```

```python
import math

import jax
import jax.numpy as jnp
from jax import lax
from jax.experimental import pallas as pl
from jax.experimental.pallas import tpu as pltpu
from jax.sharding import PartitionSpec as P

F32 = jnp.float32
BF16 = jnp.bfloat16
NT = (((1,), (1,)), ((), ()))
SIDE = 4
COLS = 40
HEADS = 8


def softplus(x):
    return jnp.maximum(x, 0.0) + jnp.log1p(jnp.exp(-jnp.abs(x)))


def size(ref):
    return math.prod(ref.shape) * jnp.dtype(ref.dtype).itemsize


class Group:
    def __init__(self, copies, sem, like):
        self.copies, self.sem, self.like, self.bytes = copies, sem, like, 0

    def start(self, src, dst, peer):
        self.bytes += size(src)
        self.copies.sent[self.like is None].bytes += size(src)
        pltpu.make_async_remote_copy(
            src_ref=src,
            dst_ref=dst,
            send_sem=self.copies.sent[self.like is None].sem,
            recv_sem=self.sem,
            device_id=peer,
            device_id_type=pl.DeviceIdType.MESH,
        ).start()

    def wait(self):
        if self.like is None:
            rows = self.bytes // size(self.copies.held.at[0])
            ref = self.copies.held.at[pl.ds(0, rows)]
        else:
            ref = self.like.at[pl.ds(0, self.bytes // size(self.like.at[0]))]
        pltpu.make_async_copy(ref, ref, self.sem).wait()


class Copies:
    def __init__(self, held, little, send, recv):
        self.held, self.recv, self.used = held, recv, 0
        self.sent = {True: Group(self, send.at[0], None), False: Group(self, send.at[1], little)}

    def group(self, like=None):
        self.used += 1
        return Group(self, self.recv.at[self.used - 1], like)

    def drain(self):
        for group in self.sent.values():
            group.wait()


class Ring:
    def __init__(self, me, row_of):
        self.me = me
        self.right = lax.rem(me + 1, SIDE)
        self.far = lax.rem(me + 2, SIDE)
        self.left = lax.rem(me + 3, SIDE)
        self.to_right = {"row": row_of(self.right)}
        self.to_far = {"row": row_of(self.far)}
        self.to_left = {"row": row_of(self.left)}
        self.at = {"far": self.far, "right": self.right, "left": self.left}
        self.to = {"far": self.to_far, "right": self.to_right, "left": self.to_left}


class Scatter:
    def __init__(self, copies, ring, pieces, part, land, fine):
        self.ring, self.pieces, self.part, self.land = ring, pieces, part, land
        if fine:
            self.relay = [copies.group() for _ in pieces]
            self.joint = [copies.group() for _ in pieces]
        else:
            self.relay = [copies.group()] * len(pieces)
            self.joint = [copies.group()] * len(pieces)

    def send_far(self):
        r = self.ring
        for n, b in enumerate(self.pieces):
            for half, peer in ((0, r.to_left), (1, r.to_right)):
                self.relay[n].start(self.part(half, r.far).at[b], self.land.at[half, 0, b], peer)

    def send_right(self):
        r = self.ring
        self.joint[0].start(self.part(0, r.right), self.land.at[0, 1], r.to_right)

    def send_left(self):
        r = self.ring
        self.joint[0].start(self.part(1, r.left), self.land.at[1, 1], r.to_left)

    def forward(self):
        r = self.ring
        for n, b in enumerate(self.pieces):
            if self.relay[n] not in self.relay[:n]:
                self.relay[n].wait()
            for half, to, peer in ((0, r.left, r.to_left), (1, r.right, r.to_right)):
                piece = self.part(half, to).at[b]
                piece[...] = piece[...] + self.land[half, 0, b]
                self.joint[n].start(piece, self.land.at[half, 2, b], peer)

    def finish(self, n):
        b = self.pieces[n]
        if self.joint[n] not in self.joint[:n]:
            self.joint[n].wait()
        for half in (0, 1):
            piece = self.part(half, self.ring.me).at[b]
            piece[...] = piece[...] + self.land[half, 1, b] + self.land[half, 2, b]


WAYS = ("far", "right", "left")


def split(x):
    hi = x.astype(BF16)
    return hi, (x - hi.astype(F32)).astype(BF16)


def growth(delta_all, lift, o, first, second, r):
    hi, lo = split(jnp.concatenate([delta_all[o, c, first, second] for c in (0, 1)], axis=1))
    add = jnp.dot(lift[r, o], jnp.concatenate([hi, lo, hi], axis=0), preferred_element_type=F32)
    return [add[:, c * 128 : (c + 1) * 128].reshape(hi.shape[0], 8, 128) for c in (0, 1)]


def exchange_kernel(
    wq_hbm,
    wk_hbm,
    wd_hbm,
    wb_hbm,
    decay_log,
    dt_bias,
    gain,
    hid_hbm,
    wv_hbm,
    wz_hbm,
    w_out_hbm,
    state,
    held,
    delta_all,
    lift,
    outs_land,
    wq,
    wk,
    wd,
    wb,
    hid,
    wv,
    wz,
    w_out,
    proj,
    decay_all,
    part,
    land1,
    land2,
    small,
    small_land1,
    small_land2,
    scales,
    normed,
    outs,
    load_sem,
    weight_sem,
    send_sem,
    recv_sem,
):
    row = lax.axis_index("row")
    head = lax.axis_index("head")
    x, z = row // SIDE, lax.rem(row, SIDE)
    rows = SIDE * SIDE
    blk = held.shape[0] // rows

    barrier = pltpu.get_barrier_semaphore()
    peers = []
    for d in (1, 2, 3):
        peers.append({"row": lax.rem(x + d, SIDE) * SIDE + z})
        peers.append({"row": x * SIDE + lax.rem(z + d, SIDE)})
    for d in range(1, HEADS):
        peers.append({"head": lax.rem(head + d, HEADS)})
    for peer in peers:
        pl.semaphore_signal(barrier, inc=1, device_id=peer, device_id_type=pl.DeviceIdType.MESH)

    def row_at(o, first, second):
        return first * SIDE + second if o == 0 else second * SIDE + first

    rings1 = [
        Ring(x, lambda a: row_at(0, a, z)),
        Ring(z, lambda a: row_at(1, a, x)),
    ]
    rings2 = [
        Ring(z, lambda b: row_at(0, x, b)),
        Ring(x, lambda b: row_at(1, z, b)),
    ]
    order = [[r.far, r.right, r.left, r.me] for r in rings1]

    first = []
    small_weights = ((wq_hbm, wq), (wk_hbm, wk), (wd_hbm, wd), (wb_hbm, wb))
    quarter = hid.shape[0] // 4
    pieces = tuple((hid_hbm.at[pl.ds(n * quarter, quarter)], hid.at[pl.ds(n * quarter, quarter)]) for n in range(4))
    for n, (src, dst) in enumerate(small_weights):
        first.append(pltpu.make_async_copy(src, dst, weight_sem.at[n]))
        first[-1].start()
    for src, dst in pieces:
        pltpu.make_async_copy(src, dst, weight_sem.at[4]).start()
    all_hid = pltpu.make_async_copy(hid, hid, weight_sem.at[4])

    def load(j, o):
        for b in range(SIDE):
            at = row_at(o, order[o][j], b) * blk
            pltpu.make_async_copy(
                state.at[pl.ds(at, blk), pl.ds(2 * o, 2)],
                held.at[pl.ds(at, blk), pl.ds(2 * o, 2)],
                load_sem.at[j * 2 + o],
            ).start()

    def await_load(j, o):
        ref = held.at[pl.ds(0, SIDE * blk // 2)]
        pltpu.make_async_copy(ref, ref, load_sem.at[j * 2 + o]).wait()

    load(0, 0)

    proj[...] = jnp.zeros_like(proj)
    for copy in first:
        copy.wait()
    load(0, 1)
    w = jnp.concatenate(
        [
            wq[0].astype(F32),
            wq[1].astype(F32),
            wk[0].astype(F32),
            wk[1].astype(F32),
            wd[...].astype(F32),
            wb[...].astype(F32),
        ],
        axis=0,
    ).astype(BF16)
    all_hid.wait()
    for j in (1, 2, 3):
        for o in (0, 1):
            load(j, o)
    proj[:, :COLS] = lax.dot_general(hid[...], w, NT, preferred_element_type=F32)

    copies = Copies(held, small_land1, send_sem, recv_sem)
    lane = lax.broadcasted_iota(jnp.int32, (blk, 128), 1)
    own = [
        lane // 8 + n * 16 == lax.broadcasted_iota(jnp.int32, (blk, 128), 0) for n in range(8 * blk // 128)
    ]

    def spread(vec, base):
        wide = jnp.where(lane < 8, vec if base == 0 else pltpu.roll(vec, 128 - base, 1), 0.0)
        for shift in (8, 16, 32, 64):
            wide = wide + pltpu.roll(wide, shift, 1)
        return jnp.concatenate([jnp.where(m, wide, 0.0) for m in own], axis=1)

    def read_block(o, first, second):
        at = pl.multiple_of(row_at(o, first, second) * blk, blk)
        vec = proj[pl.ds(at, blk), :]
        wide = jnp.concatenate([spread(vec, 16 + 8 * o), spread(vec, 8 * o)], axis=0)
        wide = jnp.concatenate(split(wide), axis=0)
        hi, lo = split(
            jnp.concatenate([held[pl.ds(at, blk), 2 * o + c].reshape(8 * blk, 128) for c in (0, 1)], axis=1)
        )
        main = jnp.dot(wide, hi, preferred_element_type=F32)
        rest = jnp.dot(wide[: 2 * blk], lo, preferred_element_type=F32)
        read = main[: 2 * blk] + (main[2 * blk :] + rest)
        for c in (0, 1):
            for t in (0, 1):
                part[o, c, t, first, second] = read[t * blk : (t + 1) * blk, c * 128 : (c + 1) * 128]

    def send_sums():
        for a in range(SIDE):
            cols = proj[a * 128 : (a + 1) * 128, :].T
            terms = []
            for u, v in ((0, 0), (16, 16), (0, 16)):
                for hk in (0, 8):
                    product = cols[u + hk : u + hk + 8] * cols[v + hk : v + hk + 8]
                    terms.append(jnp.sum(product, axis=0, keepdims=True))
            terms.append(jnp.zeros((2, 128), F32))
            small[a] = jnp.concatenate(terms, axis=0)
        group = copies.group(small_land1)
        for n, name in enumerate(WAYS):
            group.start(small.at[rings1[0].at[name]], small_land1.at[n], rings1[0].to[name])
        return group

    def scatter1(o, t):
        r = rings2[o]
        pieces = (r.far, r.right, r.left, r.me)
        return Scatter(copies, rings1[o], pieces, lambda c, a: part.at[o, c, t, a], land1.at[o, t], t == 0)

    def own_piece(o, c, t):
        return part.at[o, c, t, rings1[o].me, rings2[o].me]

    def finish1(o, t, s):
        r = rings2[o]
        group = copies.group()
        for n, name in enumerate(WAYS):
            s.finish(n)
            group.start(part.at[o, :, t, rings1[o].me, r.at[name]], land2.at[o, t, n], r.to[name])
        return group

    def finish2(o, t, first, s):
        first.finish(3)
        s.wait()
        for c in (0, 1):
            piece = own_piece(o, c, t)
            piece[...] = piece[...] + land2[o, t, 0, c] + land2[o, t, 1, c] + land2[o, t, 2, c]

    k1 = [scatter1(o, 0) for o in (0, 1)]
    q1 = [scatter1(o, 1) for o in (0, 1)]

    for j in range(SIDE):
        for o in (0, 1):
            await_load(j, o)
            if j == 0:
                for b in range(SIDE):
                    read_block(o, order[o][j], b)
                if o == 0:
                    pl.semaphore_wait(barrier, len(peers))
                k1[o].send_far()
        if j == 0:
            small1 = send_sums()
            for o in (0, 1):
                q1[o].send_far()
        else:
            for o in (0, 1):
                for b in range(SIDE):
                    read_block(o, order[o][j], b)
        if j == 1:
            for o in (0, 1):
                k1[o].send_right()
            load_weights = []
            for n, (src, dst) in enumerate(((wv_hbm, wv), (wz_hbm, wz), (w_out_hbm, w_out))):
                load_weights.append(pltpu.make_async_copy(src, dst, weight_sem.at[n + 5]))
                load_weights[-1].start()
        if j == 2:
            for o in (0, 1):
                k1[o].send_left()
    for s in k1:
        s.forward()
    for s in q1:
        s.send_right()
        s.send_left()
    small1.wait()
    small[x] = small[x] + small_land1[0] + small_land1[1] + small_land1[2]
    small2 = copies.group(small_land2)
    for n, name in enumerate(WAYS):
        small2.start(small.at[x], small_land2.at[n], rings2[0].to[name])

    mine = pl.ds(pl.multiple_of(row * blk, blk), blk)
    own_hid = hid[mine, :]
    chunks = own_hid.shape[1] // 256
    tall = jnp.concatenate([own_hid[:, n * 256 : (n + 1) * 256] for n in range(chunks)], axis=0)
    repeat = (
        lax.broadcasted_iota(jnp.int32, (256, 1024), 1) // 4 == lax.broadcasted_iota(jnp.int32, (256, 1024), 0)
    ).astype(F32).astype(BF16)
    tall = jnp.dot(tall, repeat, preferred_element_type=F32)
    at_head = lax.broadcasted_iota(jnp.int32, (blk, 1024), 1) % 4
    load_weights[0].wait()
    load_weights[1].wait()
    both = jnp.zeros((4 * blk, 256), F32)
    for n in range(chunks):
        piece = tall[n * blk : (n + 1) * blk]
        piece = jnp.concatenate([jnp.where(at_head == h, piece, 0.0).astype(BF16) for h in range(4)], axis=0)
        at = slice(n * 1024, (n + 1) * 1024)
        weights = jnp.concatenate([wv[at, :], wz[at, :]], axis=1)
        both = both + jnp.dot(piece, weights, preferred_element_type=F32)

    for s in q1:
        s.forward()
    k2 = [finish1(o, 0, k1[o]) for o in (0, 1)]

    decay_all[...] = jnp.exp(-jnp.exp(decay_log[...]) * softplus(proj[:, 32:36] + dt_bias[...]))
    own_t = lax.broadcasted_iota(jnp.int32, (8 * blk, 3 * blk), 0) // 8 == lax.rem(
        lax.broadcasted_iota(jnp.int32, (8 * blk, 3 * blk), 1), blk
    )
    picks = [
        (
            lax.broadcasted_iota(jnp.int32, (8 * blk, COLS), 1)
            == 16 + 8 * o + lax.broadcasted_iota(jnp.int32, (8 * blk, COLS), 0) % 8
        )
        .astype(F32)
        .astype(BF16)
        for o in (0, 1)
    ]

    def prepare(r, carry):
        at = pl.ds(pl.multiple_of(r * blk, blk), blk)
        hi, lo = split(proj[at, :COLS])
        three = jnp.concatenate([hi.astype(F32), hi.astype(F32), lo.astype(F32)], axis=0).astype(BF16)
        decay = decay_all[at, :]
        for o in (0, 1):
            wide = lax.dot_general(picks[o], three, NT, preferred_element_type=F32)
            lift[r, o] = jnp.where(own_t, wide, 0.0).astype(BF16)
            for c in (0, 1):
                h = 2 * o + c
                keep = jnp.broadcast_to(decay[:, h : h + 1], (blk, 128))
                held[at, h] = keep[:, None, :] * held[at, h]
        return carry

    lax.fori_loop(0, rows // 2, prepare, 0)

    q2 = [finish1(o, 1, q1[o]) for o in (0, 1)]

    small2.wait()
    total = small[x] + small_land2[0] + small_land2[1] + small_land2[2]
    scales[...] = jnp.concatenate([total, jnp.zeros((120, 128), F32)], axis=0).T
    raw = scales[pl.ds(pl.multiple_of(z * blk, blk), blk), :]
    q_scale = lax.rsqrt(1.0 + raw[:, 0:2])
    k_scale = lax.rsqrt(1.0 + raw[:, 2:4])
    unit_dot = raw[:, 4:6] * q_scale * k_scale
    decay = decay_all[mine, :]
    beta = 1.0 / (1.0 + jnp.exp(-proj[mine, 36:40]))

    g2 = {(o, name): copies.group() for o in (0, 1) for name in WAYS}
    near = {(o, name): copies.group() for o in (0, 1) for name in ("me", "left", "right", "far")}
    onward = [copies.group() for _ in (0, 1)]
    straight = [copies.group() for _ in (0, 1)]

    def send_near(o, name):
        r = rings1[o]
        b = rings2[o].me if name == "me" else rings2[o].at[name]
        piece = delta_all.at[o, :, r.me, b]
        for way in ("right", "left"):
            near[o, name].start(piece, piece, r.to[way])
        if name == "far":
            straight[o].start(piece, piece, r.to_far)

    def send_on(o, name):
        r = rings1[o]
        b = rings2[o].me if name == "me" else rings2[o].at[name]
        near[o, name].wait()
        for half, at, peer in ((0, r.left, r.to_right), (1, r.right, r.to_left)):
            piece = delta_all.at[o, half, at, b]
            onward[o].start(piece, piece, peer)

    deltas = []
    for o in (0, 1):
        finish2(o, 0, k1[o], k2[o])
        for c in (0, 1):
            h = 2 * o + c
            readk = own_piece(o, c, 0)[...] * k_scale[:, o : o + 1]
            value = both[h * blk : (h + 1) * blk, :128]
            delta = beta[:, h : h + 1] * (value - decay[:, h : h + 1] * readk)
            delta_all[o, c, rings1[o].me, rings2[o].me] = delta * k_scale[:, o : o + 1]
            deltas.append(delta)
        here = delta_all.at[o, :, rings1[o].me, rings2[o].me]
        for name in ("right", "left", "far"):
            g2[o, name].start(here, here, rings2[o].to[name])
    for o in (0, 1):
        send_near(o, "me")

    lax.fori_loop(rows // 2, rows, prepare, 0)
    for o in (0, 1):
        for sent, name in (("right", "left"), ("left", "right")):
            g2[o, sent].wait()
            send_near(o, name)
    for o in (0, 1):
        finish2(o, 1, q1[o], q2[o])
        for c in (0, 1):
            h = 2 * o + c
            old = own_piece(o, c, 1)[...] * q_scale[:, o : o + 1]
            readq = decay[:, h : h + 1] * old + unit_dot[:, o : o + 1] * deltas[h]
            meansq = jnp.mean(readq * readq, axis=-1, keepdims=True)
            gate = both[h * blk : (h + 1) * blk, 128:]
            gate = gate / (1.0 + jnp.exp(-gate))
            normed[:, h * 128 : (h + 1) * 128] = (readq * lax.rsqrt(meansq + 0.5) * gain[...] * gate).astype(BF16)

    load_weights[2].wait()
    width = outs.shape[-1]
    for n in range(HEADS):
        outs[n] = jnp.dot(normed[...], w_out[:, n * width : (n + 1) * width], preferred_element_type=F32)
    out_group = copies.group()
    for d in range(1, HEADS):
        to = lax.rem(head + d, HEADS)
        out_group.start(outs.at[to], outs_land.at[head], {"head": to})
    outs_land[head] = outs[head]

    for o in (0, 1):
        send_on(o, "me")
        g2[o, "far"].wait()
        send_near(o, "far")
    for o in (0, 1):
        for name in ("left", "right"):
            send_on(o, name)

    def update_rows(o, first):
        for b in range(SIDE):
            r = row_at(o, first, b)
            at = pl.ds(pl.multiple_of(r * blk, blk), blk)
            add = growth(delta_all, lift, o, first, b, r)
            for c in (0, 1):
                h = 2 * o + c
                held[at, h] = held[at, h] + add[c]

    for o in (0, 1):
        update_rows(o, rings1[o].me)
    for o in (0, 1):
        near[o, "far"].wait()
    for o in (0, 1):
        update_rows(o, rings1[o].left)
        update_rows(o, rings1[o].right)
    out_group.wait()
    for o in (0, 1):
        onward[o].wait()
        straight[o].wait()
    copies.drain()


def finish_kernel(held, delta_all, lift, outs_land, layer_out, new_state, last, layer, sems):
    row = lax.axis_index("row")
    spots = (row // SIDE, lax.rem(row, SIDE))
    blk = held.shape[0] // (SIDE * SIDE)

    def store(src, o, r, count=1):
        dst = new_state.at[pl.ds(pl.multiple_of(r * blk, blk), count * blk), pl.ds(2 * o, 2)]
        pltpu.make_async_copy(src, dst, sems.at[0]).start()

    for d in (0, 1, 3):
        first = lax.rem(spots[0] + d, SIDE)
        at = pl.ds(pl.multiple_of(first * SIDE * blk, blk), SIDE * blk)
        store(held.at[at, pl.ds(0, 2)], 0, first * SIDE, SIDE)
        for b in range(SIDE):
            r = b * SIDE + lax.rem(spots[1] + d, SIDE)
            store(held.at[pl.ds(pl.multiple_of(r * blk, blk), blk), pl.ds(2, 2)], 1, r)
    total = outs_land[0]
    for n in range(1, HEADS):
        total = total + outs_land[n]
    layer[...] = total.astype(BF16)
    layer_copy = pltpu.make_async_copy(layer, layer_out, sems.at[1])
    layer_copy.start()
    for o in (0, 1):
        first = lax.rem(spots[o] + 2, SIDE)
        for b in range(SIDE):
            r = first * SIDE + b if o == 0 else b * SIDE + first
            at = pl.ds(pl.multiple_of(r * blk, blk), blk)
            add = growth(delta_all, lift, o, first, b, r)
            for c in (0, 1):
                last[o * SIDE + b, :, c] = held[at, 2 * o + c] + add[c]
            store(last.at[o * SIDE + b], o, r)
    layer_copy.wait()
    pltpu.make_async_copy(held, new_state, sems.at[0]).wait()


def local(
    hidden_in,
    w_query,
    w_key,
    w_value,
    w_zgate,
    w_decay,
    w_beta,
    decay_log,
    dt_bias,
    norm_gain,
    w_out,
    state,
):
    seqs, width = hidden_in.shape
    rows = SIDE * SIDE
    blk = seqs // rows
    vmem = pl.BlockSpec(memory_space=pltpu.VMEM)
    anywhere = pl.BlockSpec(memory_space=pltpu.HBM)
    held, delta_all, lift, outs_land = pl.pallas_call(
        exchange_kernel,
        out_shape=(
            pltpu.VMEM(state.shape, F32),
            pltpu.VMEM((2, 2, SIDE, SIDE, blk, 128), F32),
            pltpu.VMEM((rows, 2, 8 * blk, 3 * blk), BF16),
            pltpu.VMEM((HEADS, blk, 256), F32),
        ),
        in_specs=[anywhere] * 4 + [vmem] * 3 + [anywhere] * 5,
        out_specs=(vmem,) * 4,
        scratch_shapes=[
            pltpu.VMEM((2, 8, width), BF16),
            pltpu.VMEM((2, 8, width), BF16),
            pltpu.VMEM((4, width), BF16),
            pltpu.VMEM((4, width), BF16),
            pltpu.VMEM((seqs, width), BF16),
            pltpu.VMEM((4 * width, 128), BF16),
            pltpu.VMEM((4 * width, 128), BF16),
            pltpu.VMEM((512, width), BF16),
            pltpu.VMEM((seqs, 128), F32),
            pltpu.VMEM((seqs, 4), F32),
            pltpu.VMEM((2, 2, 2, SIDE, SIDE, blk, 128), F32),
            pltpu.VMEM((2, 2, 2, 3, SIDE, blk, 128), F32),
            pltpu.VMEM((2, 2, 3, 2, blk, 128), F32),
            pltpu.VMEM((SIDE, 8, 128), F32),
            pltpu.VMEM((6, 8, 128), F32),
            pltpu.VMEM((3, 8, 128), F32),
            pltpu.VMEM((128, 128), F32),
            pltpu.VMEM((blk, 512), BF16),
            pltpu.VMEM((HEADS, blk, 256), F32),
            pltpu.SemaphoreType.DMA((2 * SIDE,)),
            pltpu.SemaphoreType.DMA((8,)),
            pltpu.SemaphoreType.DMA((2,)),
            pltpu.SemaphoreType.DMA((45,)),
        ],
        compiler_params=pltpu.CompilerParams(
            collective_id=0, has_side_effects=True, vmem_limit_bytes=36 * 1024 * 1024
        ),
        name="exchange",
    )(
        *(
            pltpu.with_memory_space_constraint(operand, pltpu.HBM)
            for operand in (
                jnp.transpose(w_query, (1, 2, 0)),
                jnp.transpose(w_key, (1, 2, 0)),
                jnp.transpose(w_decay, (1, 0)),
                jnp.transpose(w_beta, (1, 0)),
                decay_log.reshape(1, 4),
                dt_bias.reshape(1, 4),
                norm_gain.reshape(1, 128),
                hidden_in,
                w_value.reshape(4 * width, 128),
                w_zgate.reshape(4 * width, 128),
                w_out.reshape(512, width),
                state,
            )
        )
    )
    layer_out, new_state = pl.pallas_call(
        finish_kernel,
        out_shape=(
            jax.ShapeDtypeStruct((blk, 256), BF16),
            jax.ShapeDtypeStruct(state.shape, F32),
        ),
        in_specs=[vmem] * 4,
        out_specs=(anywhere, anywhere),
        scratch_shapes=[
            pltpu.VMEM((2 * SIDE, blk, 2, 8, 128), F32),
            pltpu.VMEM((blk, 256), BF16),
            pltpu.SemaphoreType.DMA((2,)),
        ],
        compiler_params=pltpu.CompilerParams(vmem_limit_bytes=16 * 1024 * 1024),
        name="finish",
    )(*(pltpu.with_memory_space_constraint(a, pltpu.VMEM) for a in (held, delta_all, lift, outs_land)))
    return layer_out, new_state


def solution(mesh):
    in_specs = (
        P(),
        P(None, "head", "row"),
        P(None, "head", "row"),
        P(None, "head", None),
        P(None, "head", None),
        P(None, "head"),
        P(None, "head"),
        P("head"),
        P("head"),
        P(),
        P("head", None, None),
        P(None, "head", "row", None),
    )
    out_specs = (P("row", "head"), P(None, "head", "row", None))
    return jax.shard_map(local, mesh=mesh, in_specs=in_specs, out_specs=out_specs, check_vma=False)
```

```python
import math

import jax
import jax.numpy as jnp
from jax import lax
from jax.experimental import pallas as pl
from jax.experimental.pallas import tpu as pltpu
from jax.sharding import PartitionSpec as P

F32 = jnp.float32
BF16 = jnp.bfloat16
NT = (((1,), (1,)), ((), ()))
SIDE = 4
COLS = 40
HEADS = 8
PITCH = 40


def softplus(x):
    return jnp.maximum(x, 0.0) + jnp.log1p(jnp.exp(-jnp.abs(x)))


def size(ref):
    return math.prod(ref.shape) * jnp.dtype(ref.dtype).itemsize


class Group:
    def __init__(self, copies, sem, like):
        self.copies, self.sem, self.like, self.bytes = copies, sem, like, 0

    def start(self, src, dst, peer):
        self.bytes += size(src)
        self.copies.sent[self.like is None].bytes += size(src)
        pltpu.make_async_remote_copy(
            src_ref=src,
            dst_ref=dst,
            send_sem=self.copies.sent[self.like is None].sem,
            recv_sem=self.sem,
            device_id=peer,
            device_id_type=pl.DeviceIdType.MESH,
        ).start()

    def wait(self):
        if self.like is None:
            rows = self.bytes // size(self.copies.held.at[0, pl.ds(0, 4)])
            ref = self.copies.held.at[pl.ds(0, rows), pl.ds(0, 4)]
        else:
            ref = self.like.at[pl.ds(0, self.bytes // size(self.like.at[0]))]
        pltpu.make_async_copy(ref, ref, self.sem).wait()


class Copies:
    def __init__(self, held, little, send, recv):
        self.held, self.recv, self.used = held, recv, 0
        self.sent = {True: Group(self, send.at[0], None), False: Group(self, send.at[1], little)}

    def group(self, like=None):
        self.used += 1
        return Group(self, self.recv.at[self.used - 1], like)

    def drain(self):
        for group in self.sent.values():
            group.wait()


class Ring:
    def __init__(self, me, row_of):
        self.me = me
        self.right = lax.rem(me + 1, SIDE)
        self.far = lax.rem(me + 2, SIDE)
        self.left = lax.rem(me + 3, SIDE)
        self.to_right = {"row": row_of(self.right)}
        self.to_far = {"row": row_of(self.far)}
        self.to_left = {"row": row_of(self.left)}
        self.at = {"far": self.far, "right": self.right, "left": self.left}
        self.to = {"far": self.to_far, "right": self.to_right, "left": self.to_left}


class Scatter:
    def __init__(self, copies, ring, pieces, part, land, fine):
        self.ring, self.pieces, self.part, self.land = ring, pieces, part, land
        if fine:
            self.relay = [copies.group() for _ in pieces]
            self.joint = [copies.group() for _ in pieces]
        else:
            self.relay = [copies.group()] * len(pieces)
            self.joint = [copies.group()] * len(pieces)

    def send_far(self):
        r = self.ring
        for n, b in enumerate(self.pieces):
            for half, peer in ((0, r.to_left), (1, r.to_right)):
                self.relay[n].start(self.part(half, r.far).at[b], self.land.at[half, 0, b], peer)

    def send_right(self):
        r = self.ring
        self.joint[0].start(self.part(0, r.right), self.land.at[0, 1], r.to_right)

    def send_left(self):
        r = self.ring
        self.joint[0].start(self.part(1, r.left), self.land.at[1, 1], r.to_left)

    def forward(self):
        r = self.ring
        for n, b in enumerate(self.pieces):
            if self.relay[n] not in self.relay[:n]:
                self.relay[n].wait()
            for half, to, peer in ((0, r.left, r.to_left), (1, r.right, r.to_right)):
                piece = self.part(half, to).at[b]
                piece[...] = piece[...] + self.land[half, 0, b]
                self.joint[n].start(piece, self.land.at[half, 2, b], peer)

    def finish(self, n):
        b = self.pieces[n]
        if self.joint[n] not in self.joint[:n]:
            self.joint[n].wait()
        for half in (0, 1):
            piece = self.part(half, self.ring.me).at[b]
            piece[...] = piece[...] + self.land[half, 1, b] + self.land[half, 2, b]


WAYS = ("far", "right", "left")


def split(x):
    hi = x.astype(BF16)
    return hi, (x - hi.astype(F32)).astype(BF16)


def growth(delta_all, lift, o, first, second, r):
    hi, lo = split(jnp.concatenate([delta_all[o, c, first, second] for c in (0, 1)], axis=1))
    add = jnp.dot(lift[r, o], jnp.concatenate([hi, lo, hi], axis=0), preferred_element_type=F32)
    return [add[:, c * 128 : (c + 1) * 128].reshape(hi.shape[0], 8, 128) for c in (0, 1)]


def exchange_kernel(
    wq_hbm,
    wk_hbm,
    wd_hbm,
    wb_hbm,
    decay_log,
    dt_bias,
    gain,
    hid_hbm,
    wv_hbm,
    wz_hbm,
    w_out_hbm,
    state,
    held,
    delta_all,
    lift,
    outs_land,
    wq,
    wk,
    wd,
    wb,
    hid,
    wv,
    wz,
    w_out,
    proj,
    decay_all,
    part,
    land1,
    land2,
    small,
    small_land1,
    small_land2,
    scales,
    normed,
    outs,
    load_sem,
    weight_sem,
    send_sem,
    recv_sem,
):
    row = lax.axis_index("row")
    head = lax.axis_index("head")
    x, z = row // SIDE, lax.rem(row, SIDE)
    rows = SIDE * SIDE
    blk = held.shape[0] // rows

    def row_at(o, first, second):
        return first * SIDE + second if o == 0 else second * SIDE + first

    first = []
    small_weights = ((wq_hbm, wq), (wk_hbm, wk), (wd_hbm, wd), (wb_hbm, wb))
    quarter = hid.shape[0] // 4
    pieces = tuple((hid_hbm.at[pl.ds(n * quarter, quarter)], hid.at[pl.ds(n * quarter, quarter)]) for n in range(4))
    for src, dst in pieces:
        pltpu.make_async_copy(src, dst, weight_sem.at[4]).start()
    for n, (src, dst) in enumerate(small_weights):
        first.append(pltpu.make_async_copy(src, dst, weight_sem.at[n]))
        first[-1].start()
    all_hid = pltpu.make_async_copy(hid, hid, weight_sem.at[4])

    barrier = pltpu.get_barrier_semaphore()
    peers = []
    for d in (1, 2, 3):
        peers.append({"row": lax.rem(x + d, SIDE) * SIDE + z})
        peers.append({"row": x * SIDE + lax.rem(z + d, SIDE)})
    for d in range(1, HEADS):
        peers.append({"head": lax.rem(head + d, HEADS)})
    for peer in peers:
        pl.semaphore_signal(barrier, inc=1, device_id=peer, device_id_type=pl.DeviceIdType.MESH)

    rings1 = [
        Ring(x, lambda a: row_at(0, a, z)),
        Ring(z, lambda a: row_at(1, a, x)),
    ]
    rings2 = [
        Ring(z, lambda b: row_at(0, x, b)),
        Ring(x, lambda b: row_at(1, z, b)),
    ]
    order = [[r.far, r.right, r.left, r.me] for r in rings1]

    def load(j, o):
        for b in range(SIDE):
            at = row_at(o, order[o][j], b) * blk
            pltpu.make_async_copy(
                state.at[pl.ds(at, blk), pl.ds(2 * o, 2)],
                held.at[pl.ds(at, blk), pl.ds(2 * o, 2)],
                load_sem.at[j * 2 + o],
            ).start()

    def await_load(j, o):
        ref = held.at[pl.ds(0, SIDE * blk // 2), pl.ds(0, 4)]
        pltpu.make_async_copy(ref, ref, load_sem.at[j * 2 + o]).wait()

    proj[...] = jnp.zeros_like(proj)
    for copy in first:
        copy.wait()
    load(0, 0)
    w = jnp.concatenate(
        [
            wq[0].astype(F32),
            wq[1].astype(F32),
            wk[0].astype(F32),
            wk[1].astype(F32),
            wd[...].astype(F32),
            wb[...].astype(F32),
        ],
        axis=0,
    ).astype(BF16)
    all_hid.wait()
    load(0, 1)
    for j in (1, 2, 3):
        for o in (0, 1):
            load(j, o)
    proj[:, :COLS] = lax.dot_general(hid[...], w, NT, preferred_element_type=F32)

    copies = Copies(held, small_land1, send_sem, recv_sem)
    flat = held.reshape(held.shape[0] * PITCH, 128)

    def read_block(o, first, second):
        at = pl.multiple_of(row_at(o, first, second) * blk, blk)
        for g in range(blk // 8):
            vec = proj[pl.ds(at + g * 8, 8), :]
            sums = [[None, None], [None, None]]
            for i in range(8):
                for c in (0, 1):
                    start = (at + g * 8) * PITCH + (2 * o + c) * 8 + i
                    values = flat[pl.ds(start, 8, stride=PITCH), :]
                    for t, base in ((0, 16), (1, 0)):
                        n = base + 8 * o + i
                        term = jnp.broadcast_to(vec[:, n : n + 1], (8, 128)) * values
                        sums[t][c] = term if i == 0 else sums[t][c] + term
            for c in (0, 1):
                for t in (0, 1):
                    part[o, c, t, first, second, g * 8 : (g + 1) * 8] = sums[t][c]

    def send_sums():
        for a in range(SIDE):
            cols = proj[a * 128 : (a + 1) * 128, :].T
            terms = []
            for u, v in ((0, 0), (16, 16), (0, 16)):
                for hk in (0, 8):
                    product = cols[u + hk : u + hk + 8] * cols[v + hk : v + hk + 8]
                    terms.append(jnp.sum(product, axis=0, keepdims=True))
            terms.append(jnp.zeros((2, 128), F32))
            small[a] = jnp.concatenate(terms, axis=0)
        group = copies.group(small_land1)
        for n, name in enumerate(WAYS):
            group.start(small.at[rings1[0].at[name]], small_land1.at[n], rings1[0].to[name])
        return group

    def scatter1(o, t):
        r = rings2[o]
        pieces = (r.far, r.right, r.left, r.me)
        return Scatter(copies, rings1[o], pieces, lambda c, a: part.at[o, c, t, a], land1.at[o, t], t == 0)

    def own_piece(o, c, t):
        return part.at[o, c, t, rings1[o].me, rings2[o].me]

    def finish1(o, t, s):
        r = rings2[o]
        group = copies.group()
        for n, name in enumerate(WAYS):
            s.finish(n)
            group.start(part.at[o, :, t, rings1[o].me, r.at[name]], land2.at[o, t, n], r.to[name])
        return group

    def finish2(o, t, first, s):
        first.finish(3)
        s.wait()
        for c in (0, 1):
            piece = own_piece(o, c, t)
            piece[...] = piece[...] + land2[o, t, 0, c] + land2[o, t, 1, c] + land2[o, t, 2, c]

    k1 = [scatter1(o, 0) for o in (0, 1)]
    q1 = [scatter1(o, 1) for o in (0, 1)]

    for j in range(SIDE):
        for o in (0, 1):
            await_load(j, o)
            if j == 0:
                for b in range(SIDE):
                    read_block(o, order[o][j], b)
                if o == 0:
                    pl.semaphore_wait(barrier, len(peers))
                k1[o].send_far()
        if j == 0:
            small1 = send_sums()
            for o in (0, 1):
                q1[o].send_far()
        else:
            for o in (0, 1):
                for b in range(SIDE):
                    read_block(o, order[o][j], b)
        if j == 1:
            for o in (0, 1):
                k1[o].send_right()
            load_weights = []
            for n, (src, dst) in enumerate(((wv_hbm, wv), (wz_hbm, wz), (w_out_hbm, w_out))):
                load_weights.append(pltpu.make_async_copy(src, dst, weight_sem.at[n + 5]))
                load_weights[-1].start()
        if j == 2:
            for o in (0, 1):
                k1[o].send_left()
    for s in k1:
        s.forward()
    for s in q1:
        s.send_right()
        s.send_left()
    small1.wait()
    small[x] = small[x] + small_land1[0] + small_land1[1] + small_land1[2]
    small2 = copies.group(small_land2)
    for n, name in enumerate(WAYS):
        small2.start(small.at[x], small_land2.at[n], rings2[0].to[name])

    mine = pl.ds(pl.multiple_of(row * blk, blk), blk)
    own_hid = hid[mine, :]
    chunks = own_hid.shape[1] // 256
    tall = jnp.concatenate([own_hid[:, n * 256 : (n + 1) * 256] for n in range(chunks)], axis=0)
    repeat = (
        lax.broadcasted_iota(jnp.int32, (256, 1024), 1) // 4 == lax.broadcasted_iota(jnp.int32, (256, 1024), 0)
    ).astype(F32).astype(BF16)
    tall = jnp.dot(tall, repeat, preferred_element_type=F32)
    at_head = lax.broadcasted_iota(jnp.int32, (blk, 1024), 1) % 4
    load_weights[0].wait()
    load_weights[1].wait()
    both = jnp.zeros((4 * blk, 256), F32)
    for n in range(chunks):
        piece = tall[n * blk : (n + 1) * blk]
        piece = jnp.concatenate([jnp.where(at_head == h, piece, 0.0).astype(BF16) for h in range(4)], axis=0)
        at = slice(n * 1024, (n + 1) * 1024)
        weights = jnp.concatenate([wv[at, :], wz[at, :]], axis=1)
        both = both + jnp.dot(piece, weights, preferred_element_type=F32)

    for s in q1:
        s.forward()
    k2 = [finish1(o, 0, k1[o]) for o in (0, 1)]

    decay_all[...] = jnp.exp(-jnp.exp(decay_log[...]) * softplus(proj[:, 32:36] + dt_bias[...]))
    own_t = lax.broadcasted_iota(jnp.int32, (8 * blk, 3 * blk), 0) // 8 == lax.rem(
        lax.broadcasted_iota(jnp.int32, (8 * blk, 3 * blk), 1), blk
    )
    picks = [
        (
            lax.broadcasted_iota(jnp.int32, (8 * blk, COLS), 1)
            == 16 + 8 * o + lax.broadcasted_iota(jnp.int32, (8 * blk, COLS), 0) % 8
        )
        .astype(F32)
        .astype(BF16)
        for o in (0, 1)
    ]

    def prepare(r, carry):
        at = pl.ds(pl.multiple_of(r * blk, blk), blk)
        hi, lo = split(proj[at, :COLS])
        three = jnp.concatenate([hi.astype(F32), hi.astype(F32), lo.astype(F32)], axis=0).astype(BF16)
        decay = decay_all[at, :]
        for o in (0, 1):
            wide = lax.dot_general(picks[o], three, NT, preferred_element_type=F32)
            lift[r, o] = jnp.where(own_t, wide, 0.0).astype(BF16)
            pair = held[at, pl.ds(2 * o, 2)]
            keep = [jnp.broadcast_to(decay[:, h : h + 1], (blk, 128))[:, None, :] for h in (2 * o, 2 * o + 1)]
            held[at, pl.ds(2 * o, 2)] = jnp.stack([keep[c] * pair[:, c] for c in (0, 1)], axis=1)
        return carry

    lax.fori_loop(0, rows // 2, prepare, 0)

    q2 = [finish1(o, 1, q1[o]) for o in (0, 1)]

    small2.wait()
    total = small[x] + small_land2[0] + small_land2[1] + small_land2[2]
    scales[...] = jnp.concatenate([total, jnp.zeros((120, 128), F32)], axis=0).T
    raw = scales[pl.ds(pl.multiple_of(z * blk, blk), blk), :]
    q_scale = lax.rsqrt(1.0 + raw[:, 0:2])
    k_scale = lax.rsqrt(1.0 + raw[:, 2:4])
    unit_dot = raw[:, 4:6] * q_scale * k_scale
    decay = decay_all[mine, :]
    beta = 1.0 / (1.0 + jnp.exp(-proj[mine, 36:40]))

    g2 = {(o, name): copies.group() for o in (0, 1) for name in WAYS}
    near = {(o, name): copies.group() for o in (0, 1) for name in ("me", "left", "right", "far")}
    onward = [copies.group() for _ in (0, 1)]
    straight = [copies.group() for _ in (0, 1)]

    def send_near(o, name):
        r = rings1[o]
        b = rings2[o].me if name == "me" else rings2[o].at[name]
        piece = delta_all.at[o, :, r.me, b]
        for way in ("right", "left"):
            near[o, name].start(piece, piece, r.to[way])
        if name == "far":
            straight[o].start(piece, piece, r.to_far)

    def send_on(o, name):
        r = rings1[o]
        b = rings2[o].me if name == "me" else rings2[o].at[name]
        near[o, name].wait()
        for half, at, peer in ((0, r.left, r.to_right), (1, r.right, r.to_left)):
            piece = delta_all.at[o, half, at, b]
            onward[o].start(piece, piece, peer)

    deltas = []
    for o in (0, 1):
        finish2(o, 0, k1[o], k2[o])
        for c in (0, 1):
            h = 2 * o + c
            readk = own_piece(o, c, 0)[...] * k_scale[:, o : o + 1]
            value = both[h * blk : (h + 1) * blk, :128]
            delta = beta[:, h : h + 1] * (value - decay[:, h : h + 1] * readk)
            delta_all[o, c, rings1[o].me, rings2[o].me] = delta * k_scale[:, o : o + 1]
            deltas.append(delta)
        here = delta_all.at[o, :, rings1[o].me, rings2[o].me]
        for name in ("right", "left", "far"):
            g2[o, name].start(here, here, rings2[o].to[name])
    for o in (0, 1):
        send_near(o, "me")

    lax.fori_loop(rows // 2, rows, prepare, 0)
    for o in (0, 1):
        for sent, name in (("right", "left"), ("left", "right")):
            g2[o, sent].wait()
            send_near(o, name)
    for o in (0, 1):
        finish2(o, 1, q1[o], q2[o])
        for c in (0, 1):
            h = 2 * o + c
            old = own_piece(o, c, 1)[...] * q_scale[:, o : o + 1]
            readq = decay[:, h : h + 1] * old + unit_dot[:, o : o + 1] * deltas[h]
            meansq = jnp.mean(readq * readq, axis=-1, keepdims=True)
            gate = both[h * blk : (h + 1) * blk, 128:]
            gate = gate / (1.0 + jnp.exp(-gate))
            normed[:, h * 128 : (h + 1) * 128] = (readq * lax.rsqrt(meansq + 0.5) * gain[...] * gate).astype(BF16)

    load_weights[2].wait()
    width = outs.shape[-1]
    for n in range(HEADS):
        outs[n] = jnp.dot(normed[...], w_out[:, n * width : (n + 1) * width], preferred_element_type=F32)
    out_group = copies.group()
    for d in range(1, HEADS):
        to = lax.rem(head + d, HEADS)
        out_group.start(outs.at[to], outs_land.at[head], {"head": to})
    outs_land[head] = outs[head]

    for o in (0, 1):
        send_on(o, "me")
        g2[o, "far"].wait()
        send_near(o, "far")
    for o in (0, 1):
        for name in ("left", "right"):
            send_on(o, name)

    def update_rows(o, first):
        for b in range(SIDE):
            r = row_at(o, first, b)
            at = pl.ds(pl.multiple_of(r * blk, blk), blk)
            add = growth(delta_all, lift, o, first, b, r)
            pair = held[at, pl.ds(2 * o, 2)]
            held[at, pl.ds(2 * o, 2)] = jnp.stack([pair[:, c] + add[c] for c in (0, 1)], axis=1)

    for o in (0, 1):
        update_rows(o, rings1[o].me)
    for o in (0, 1):
        near[o, "far"].wait()
    for o in (0, 1):
        update_rows(o, rings1[o].left)
        update_rows(o, rings1[o].right)
    out_group.wait()
    for o in (0, 1):
        onward[o].wait()
        straight[o].wait()
    copies.drain()


def finish_kernel(held, delta_all, lift, outs_land, layer_out, new_state, last, layer, sems):
    row = lax.axis_index("row")
    spots = (row // SIDE, lax.rem(row, SIDE))
    blk = held.shape[0] // (SIDE * SIDE)

    def store(src, o, r, count=1):
        dst = new_state.at[pl.ds(pl.multiple_of(r * blk, blk), count * blk), pl.ds(2 * o, 2)]
        pltpu.make_async_copy(src, dst, sems.at[0]).start()

    for d in (0, 1, 3):
        first = lax.rem(spots[0] + d, SIDE)
        at = pl.ds(pl.multiple_of(first * SIDE * blk, blk), SIDE * blk)
        store(held.at[at, pl.ds(0, 2)], 0, first * SIDE, SIDE)
        for b in range(SIDE):
            r = b * SIDE + lax.rem(spots[1] + d, SIDE)
            store(held.at[pl.ds(pl.multiple_of(r * blk, blk), blk), pl.ds(2, 2)], 1, r)
    total = outs_land[0]
    for n in range(1, HEADS):
        total = total + outs_land[n]
    layer[...] = total.astype(BF16)
    layer_copy = pltpu.make_async_copy(layer, layer_out, sems.at[1])
    layer_copy.start()
    for o in (0, 1):
        first = lax.rem(spots[o] + 2, SIDE)
        for b in range(SIDE):
            r = first * SIDE + b if o == 0 else b * SIDE + first
            at = pl.ds(pl.multiple_of(r * blk, blk), blk)
            add = growth(delta_all, lift, o, first, b, r)
            pair = held[at, pl.ds(2 * o, 2)]
            last[o * SIDE + b] = jnp.stack([pair[:, c] + add[c] for c in (0, 1)], axis=1)
            store(last.at[o * SIDE + b], o, r)
    layer_copy.wait()
    pltpu.make_async_copy(new_state, new_state, sems.at[0]).wait()


def local(
    hidden_in,
    w_query,
    w_key,
    w_value,
    w_zgate,
    w_decay,
    w_beta,
    decay_log,
    dt_bias,
    norm_gain,
    w_out,
    state,
):
    seqs, width = hidden_in.shape
    rows = SIDE * SIDE
    blk = seqs // rows
    vmem = pl.BlockSpec(memory_space=pltpu.VMEM)
    anywhere = pl.BlockSpec(memory_space=pltpu.HBM)
    held, delta_all, lift, outs_land = pl.pallas_call(
        exchange_kernel,
        out_shape=(
            pltpu.VMEM((seqs, PITCH // 8, 8, 128), F32),
            pltpu.VMEM((2, 2, SIDE, SIDE, blk, 128), F32),
            pltpu.VMEM((rows, 2, 8 * blk, 3 * blk), BF16),
            pltpu.VMEM((HEADS, blk, 256), F32),
        ),
        in_specs=[anywhere] * 4 + [vmem] * 3 + [anywhere] * 5,
        out_specs=(vmem,) * 4,
        scratch_shapes=[
            pltpu.VMEM((2, 8, width), BF16),
            pltpu.VMEM((2, 8, width), BF16),
            pltpu.VMEM((4, width), BF16),
            pltpu.VMEM((4, width), BF16),
            pltpu.VMEM((seqs, width), BF16),
            pltpu.VMEM((4 * width, 128), BF16),
            pltpu.VMEM((4 * width, 128), BF16),
            pltpu.VMEM((512, width), BF16),
            pltpu.VMEM((seqs, 128), F32),
            pltpu.VMEM((seqs, 4), F32),
            pltpu.VMEM((2, 2, 2, SIDE, SIDE, blk, 128), F32),
            pltpu.VMEM((2, 2, 2, 3, SIDE, blk, 128), F32),
            pltpu.VMEM((2, 2, 3, 2, blk, 128), F32),
            pltpu.VMEM((SIDE, 8, 128), F32),
            pltpu.VMEM((6, 8, 128), F32),
            pltpu.VMEM((3, 8, 128), F32),
            pltpu.VMEM((128, 128), F32),
            pltpu.VMEM((blk, 512), BF16),
            pltpu.VMEM((HEADS, blk, 256), F32),
            pltpu.SemaphoreType.DMA((2 * SIDE,)),
            pltpu.SemaphoreType.DMA((8,)),
            pltpu.SemaphoreType.DMA((2,)),
            pltpu.SemaphoreType.DMA((45,)),
        ],
        compiler_params=pltpu.CompilerParams(
            collective_id=0, has_side_effects=True, vmem_limit_bytes=36 * 1024 * 1024
        ),
        name="exchange",
    )(
        *(
            pltpu.with_memory_space_constraint(operand, pltpu.HBM)
            for operand in (
                jnp.transpose(w_query, (1, 2, 0)),
                jnp.transpose(w_key, (1, 2, 0)),
                jnp.transpose(w_decay, (1, 0)),
                jnp.transpose(w_beta, (1, 0)),
                decay_log.reshape(1, 4),
                dt_bias.reshape(1, 4),
                norm_gain.reshape(1, 128),
                hidden_in,
                w_value.reshape(4 * width, 128),
                w_zgate.reshape(4 * width, 128),
                w_out.reshape(512, width),
                state,
            )
        )
    )
    layer_out, new_state = pl.pallas_call(
        finish_kernel,
        out_shape=(
            jax.ShapeDtypeStruct((blk, 256), BF16),
            jax.ShapeDtypeStruct(state.shape, F32),
        ),
        in_specs=[vmem] * 4,
        out_specs=(anywhere, anywhere),
        scratch_shapes=[
            pltpu.VMEM((2 * SIDE, blk, 2, 8, 128), F32),
            pltpu.VMEM((blk, 256), BF16),
            pltpu.SemaphoreType.DMA((2,)),
        ],
        compiler_params=pltpu.CompilerParams(vmem_limit_bytes=16 * 1024 * 1024),
        name="finish",
    )(*(pltpu.with_memory_space_constraint(a, pltpu.VMEM) for a in (held, delta_all, lift, outs_land)))
    return layer_out, new_state


def solution(mesh):
    in_specs = (
        P(),
        P(None, "head", "row"),
        P(None, "head", "row"),
        P(None, "head", None),
        P(None, "head", None),
        P(None, "head"),
        P(None, "head"),
        P("head"),
        P("head"),
        P(),
        P("head", None, None),
        P(None, "head", "row", None),
    )
    out_specs = (P("row", "head"), P(None, "head", "row", None))
    return jax.shard_map(local, mesh=mesh, in_specs=in_specs, out_specs=out_specs, check_vma=False)
```

```python
import math

import jax
import jax.numpy as jnp
from jax import lax
from jax.experimental import pallas as pl
from jax.experimental.pallas import tpu as pltpu
from jax.sharding import PartitionSpec as P

F32 = jnp.float32
BF16 = jnp.bfloat16
NT = (((1,), (1,)), ((), ()))
SIDE = 4
COLS = 40
HEADS = 8
PITCH = 40


def softplus(x):
    return jnp.maximum(x, 0.0) + jnp.log1p(jnp.exp(-jnp.abs(x)))


def size(ref):
    return math.prod(ref.shape) * jnp.dtype(ref.dtype).itemsize


class Group:
    def __init__(self, copies, sem, like):
        self.copies, self.sem, self.like, self.bytes = copies, sem, like, 0

    def start(self, src, dst, peer, count=True):
        if count:
            self.bytes += size(src)
            self.copies.sent[self.like is None].bytes += size(src)
        pltpu.make_async_remote_copy(
            src_ref=src,
            dst_ref=dst,
            send_sem=self.copies.sent[self.like is None].sem,
            recv_sem=self.sem,
            device_id=peer,
            device_id_type=pl.DeviceIdType.MESH,
        ).start()

    def wait(self):
        if self.like is None:
            rows = self.bytes // size(self.copies.held.at[0, pl.ds(0, 4)])
            ref = self.copies.held.at[pl.ds(0, rows), pl.ds(0, 4)]
        else:
            ref = self.like.at[pl.ds(0, self.bytes // size(self.like.at[0]))]
        pltpu.make_async_copy(ref, ref, self.sem).wait()


class Copies:
    def __init__(self, held, little, send, recv):
        self.held, self.recv, self.used = held, recv, 0
        self.sent = {True: Group(self, send.at[0], None), False: Group(self, send.at[1], little)}

    def group(self, like=None):
        self.used += 1
        return Group(self, self.recv.at[self.used - 1], like)

    def drain(self):
        for group in self.sent.values():
            group.wait()


class Ring:
    def __init__(self, me, row_of):
        self.me = me
        self.right = lax.rem(me + 1, SIDE)
        self.far = lax.rem(me + 2, SIDE)
        self.left = lax.rem(me + 3, SIDE)
        self.to_right = {"row": row_of(self.right)}
        self.to_far = {"row": row_of(self.far)}
        self.to_left = {"row": row_of(self.left)}
        self.at = {"far": self.far, "right": self.right, "left": self.left}
        self.to = {"far": self.to_far, "right": self.to_right, "left": self.to_left}


class Scatter:
    def __init__(self, copies, ring, pieces, part, land, fine):
        self.ring, self.pieces, self.part, self.land = ring, pieces, part, land
        self.relay = [copies.group() for _ in pieces] if fine else [copies.group()] * len(pieces)
        self.joint = [copies.group() for _ in pieces]

    def send_far(self, count=True):
        r = self.ring
        for n, b in enumerate(self.pieces):
            for half, peer in ((0, r.to_left), (1, r.to_right)):
                self.relay[n].start(self.part(half, r.far).at[b], self.land.at[half, 0, b], peer, count)

    def send_right(self):
        r = self.ring
        self.joint[0].start(self.part(0, r.right), self.land.at[0, 1], r.to_right)

    def send_left(self):
        r = self.ring
        self.joint[0].start(self.part(1, r.left), self.land.at[1, 1], r.to_left)

    def forward(self):
        r = self.ring
        for n, b in enumerate(self.pieces):
            if self.relay[n] not in self.relay[:n]:
                self.relay[n].wait()
            for half, to, peer in ((0, r.left, r.to_left), (1, r.right, r.to_right)):
                piece = self.part(half, to).at[b]
                piece[...] = piece[...] + self.land[half, 0, b]
                self.joint[n].start(piece, self.land.at[half, 2, b], peer)

    def finish(self, n):
        b = self.pieces[n]
        if self.joint[n] not in self.joint[:n]:
            self.joint[n].wait()
        for half in (0, 1):
            piece = self.part(half, self.ring.me).at[b]
            piece[...] = piece[...] + self.land[half, 1, b] + self.land[half, 2, b]


WAYS = ("far", "right", "left")


def split(x):
    hi = x.astype(BF16)
    return hi, (x - hi.astype(F32)).astype(BF16)


def growth(delta_all, lift, o, first, second, r):
    hi, lo = split(jnp.concatenate([delta_all[o, c, first, second] for c in (0, 1)], axis=1))
    add = jnp.dot(lift[r, o], jnp.concatenate([hi, lo, hi], axis=0), preferred_element_type=F32)
    return [add[:, c * 128 : (c + 1) * 128].reshape(hi.shape[0], 8, 128) for c in (0, 1)]


def exchange_kernel(
    wq_hbm,
    wk_hbm,
    wd_hbm,
    wb_hbm,
    decay_log_hbm,
    dt_bias_hbm,
    gain_hbm,
    hid_hbm,
    wv_hbm,
    wz_hbm,
    w_out_hbm,
    state,
    held,
    delta_all,
    lift,
    outs_land,
    wq,
    wk,
    wd,
    wb,
    decay_log,
    dt_bias,
    gain,
    hid,
    wv,
    wz,
    w_out,
    proj,
    decay_all,
    part,
    land1,
    land2,
    small,
    small_land1,
    small_land2,
    scales,
    normed,
    outs,
    load_sem,
    weight_sem,
    send_sem,
    recv_sem,
):
    row = lax.axis_index("row")
    head = lax.axis_index("head")
    x, z = row // SIDE, lax.rem(row, SIDE)
    rows = SIDE * SIDE
    blk = held.shape[0] // rows

    def row_at(o, first, second):
        return first * SIDE + second if o == 0 else second * SIDE + first

    first = []
    small_weights = ((wq_hbm, wq), (wk_hbm, wk), (wd_hbm, wd), (wb_hbm, wb))
    quarter = hid.shape[0] // 4
    pieces = tuple((hid_hbm.at[pl.ds(n * quarter, quarter)], hid.at[pl.ds(n * quarter, quarter)]) for n in range(4))
    for src, dst in pieces:
        pltpu.make_async_copy(src, dst, weight_sem.at[4]).start()
    for n, (src, dst) in enumerate(small_weights):
        first.append(pltpu.make_async_copy(src, dst, weight_sem.at[n]))
        first[-1].start()
    params = []
    for n, (src, dst) in enumerate(((decay_log_hbm, decay_log), (dt_bias_hbm, dt_bias), (gain_hbm, gain))):
        params.append(pltpu.make_async_copy(src, dst, weight_sem.at[8 + n]))
        params[-1].start()
    all_hid = pltpu.make_async_copy(hid, hid, weight_sem.at[4])

    barrier = pltpu.get_barrier_semaphore()
    peers = []
    for d in (1, 2, 3):
        peers.append({"row": lax.rem(x + d, SIDE) * SIDE + z})
        peers.append({"row": x * SIDE + lax.rem(z + d, SIDE)})
    for d in range(1, HEADS):
        peers.append({"head": lax.rem(head + d, HEADS)})
    for peer in peers:
        pl.semaphore_signal(barrier, inc=1, device_id=peer, device_id_type=pl.DeviceIdType.MESH)

    rings1 = [
        Ring(x, lambda a: row_at(0, a, z)),
        Ring(z, lambda a: row_at(1, a, x)),
    ]
    rings2 = [
        Ring(z, lambda b: row_at(0, x, b)),
        Ring(x, lambda b: row_at(1, z, b)),
    ]
    order = [[r.far, r.right, r.left, r.me] for r in rings1]

    def load(j, o):
        for b in range(SIDE):
            at = row_at(o, order[o][j], b) * blk
            pltpu.make_async_copy(
                state.at[pl.ds(at, blk), pl.ds(2 * o, 2)],
                held.at[pl.ds(at, blk), pl.ds(2 * o, 2)],
                load_sem.at[j * 2 + o],
            ).start()

    def await_load(j, o):
        ref = held.at[pl.ds(0, SIDE * blk // 2), pl.ds(0, 4)]
        pltpu.make_async_copy(ref, ref, load_sem.at[j * 2 + o]).wait()

    proj[...] = jnp.zeros_like(proj)
    for copy in first:
        copy.wait()
    load(0, 0)
    w = jnp.concatenate(
        [
            wq[0].astype(F32),
            wq[1].astype(F32),
            wk[0].astype(F32),
            wk[1].astype(F32),
            wd[...].astype(F32),
            wb[...].astype(F32),
        ],
        axis=0,
    ).astype(BF16)
    all_hid.wait()
    load(0, 1)
    half = hid.shape[1] // 2
    proj[:, :COLS] = sum(
        lax.dot_general(hid[:, at], w[:, at], NT, preferred_element_type=F32)
        for at in (slice(0, half), slice(half, 2 * half))
    )
    for j in (1, 2, 3):
        for o in (0, 1):
            load(j, o)

    copies = Copies(held, small_land1, send_sem, recv_sem)
    flat = held.reshape(held.shape[0] * PITCH, 128)

    def read_block(o, first, second):
        at = pl.multiple_of(row_at(o, first, second) * blk, blk)
        for g in range(blk // 8):
            vec = proj[pl.ds(at + g * 8, 8), :]
            sums = [[None, None], [None, None]]
            for i in range(8):
                for c in (0, 1):
                    start = (at + g * 8) * PITCH + (2 * o + c) * 8 + i
                    values = flat[pl.ds(start, 8, stride=PITCH), :]
                    for t, base in ((0, 16), (1, 0)):
                        n = base + 8 * o + i
                        term = jnp.broadcast_to(vec[:, n : n + 1], (8, 128)) * values
                        sums[t][c] = term if i == 0 else sums[t][c] + term
            for c in (0, 1):
                for t in (0, 1):
                    part[o, c, t, first, second, g * 8 : (g + 1) * 8] = sums[t][c]

    def send_sums():
        for a in range(SIDE):
            cols = proj[a * 128 : (a + 1) * 128, :].T
            terms = []
            for u, v in ((0, 0), (16, 16), (0, 16)):
                for hk in (0, 8):
                    product = cols[u + hk : u + hk + 8] * cols[v + hk : v + hk + 8]
                    terms.append(jnp.sum(product, axis=0, keepdims=True))
            terms.append(jnp.zeros((2, 128), F32))
            small[a] = jnp.concatenate(terms, axis=0)
        group = copies.group(small_land1)
        for n, name in enumerate(WAYS):
            group.start(small.at[rings1[0].at[name]], small_land1.at[n], rings1[0].to[name])
        return group

    def scatter1(o, t):
        r = rings2[o]
        pieces = (r.far, r.right, r.left, r.me)
        return Scatter(copies, rings1[o], pieces, lambda c, a: part.at[o, c, t, a], land1.at[o, t], t == 0)

    def own_piece(o, c, t):
        return part.at[o, c, t, rings1[o].me, rings2[o].me]

    def finish1(t, scatters):
        groups = [copies.group() for _ in scatters]
        for n, name in enumerate(WAYS):
            for o, s in enumerate(scatters):
                r = rings2[o]
                s.finish(n)
                groups[o].start(part.at[o, :, t, rings1[o].me, r.at[name]], land2.at[o, t, n], r.to[name])
        return groups

    def finish2(o, t, first, s):
        first.finish(3)
        s.wait()
        for c in (0, 1):
            piece = own_piece(o, c, t)
            piece[...] = piece[...] + land2[o, t, 0, c] + land2[o, t, 1, c] + land2[o, t, 2, c]

    k1 = [scatter1(o, 0) for o in (0, 1)]
    q1 = [scatter1(o, 1) for o in (0, 1)]

    for j in range(SIDE):
        for o in (0, 1):
            await_load(j, o)
            if j == 0:
                for b in range(SIDE):
                    read_block(o, order[o][j], b)
                if o == 0:
                    pl.semaphore_wait(barrier, len(peers))
                k1[o].send_far()
        if j == 0:
            small1 = send_sums()

            @pl.when(lax.rem(head, 2) == 0)
            def _():
                for o in (0, 1):
                    q1[o].send_far()

        else:
            for o in (0, 1):
                for b in range(SIDE):
                    read_block(o, order[o][j], b)
        if j == 1:
            for o in (0, 1):
                k1[o].send_right()
            load_weights = []
            for n, (src, dst) in enumerate(((wv_hbm, wv), (wz_hbm, wz), (w_out_hbm, w_out))):
                load_weights.append(pltpu.make_async_copy(src, dst, weight_sem.at[n + 5]))
                load_weights[-1].start()
        if j == 2:
            for o in (0, 1):
                k1[o].send_left()
    for s in k1:
        s.forward()

    @pl.when(lax.rem(head, 2) == 1)
    def _():
        for o in (0, 1):
            q1[o].send_far(count=False)

    for s in q1:
        s.send_right()
        s.send_left()
    small1.wait()
    small[x] = small[x] + small_land1[0] + small_land1[1] + small_land1[2]
    small2 = copies.group(small_land2)
    for n, name in enumerate(WAYS):
        small2.start(small.at[x], small_land2.at[n], rings2[0].to[name])

    mine = pl.ds(pl.multiple_of(row * blk, blk), blk)
    own_hid = hid[mine, :]
    chunks = own_hid.shape[1] // 256
    tall = jnp.concatenate([own_hid[:, n * 256 : (n + 1) * 256] for n in range(chunks)], axis=0)
    repeat = (
        lax.broadcasted_iota(jnp.int32, (256, 1024), 1) // 4 == lax.broadcasted_iota(jnp.int32, (256, 1024), 0)
    ).astype(F32).astype(BF16)
    tall = jnp.dot(tall, repeat, preferred_element_type=F32)
    at_head = lax.broadcasted_iota(jnp.int32, (blk, 1024), 1) % 4
    load_weights[0].wait()
    load_weights[1].wait()
    both = jnp.zeros((4 * blk, 256), F32)
    for n in range(chunks):
        piece = tall[n * blk : (n + 1) * blk]
        piece = jnp.concatenate([jnp.where(at_head == h, piece, 0.0).astype(BF16) for h in range(4)], axis=0)
        at = slice(n * 1024, (n + 1) * 1024)
        weights = jnp.concatenate([wv[at, :], wz[at, :]], axis=1)
        both = both + jnp.dot(piece, weights, preferred_element_type=F32)

    for s in q1:
        s.forward()
    k2 = finish1(0, k1)

    for copy in params:
        copy.wait()
    decay_all[...] = jnp.exp(-jnp.exp(decay_log[...]) * softplus(proj[:, 32:36] + dt_bias[...]))
    own_t = lax.broadcasted_iota(jnp.int32, (8 * blk, 3 * blk), 0) // 8 == lax.rem(
        lax.broadcasted_iota(jnp.int32, (8 * blk, 3 * blk), 1), blk
    )
    picks = [
        (
            lax.broadcasted_iota(jnp.int32, (8 * blk, COLS), 1)
            == 16 + 8 * o + lax.broadcasted_iota(jnp.int32, (8 * blk, COLS), 0) % 8
        )
        .astype(F32)
        .astype(BF16)
        for o in (0, 1)
    ]

    def prepare(r, carry):
        at = pl.ds(pl.multiple_of(r * blk, blk), blk)
        hi, lo = split(proj[at, :COLS])
        three = jnp.concatenate([hi.astype(F32), hi.astype(F32), lo.astype(F32)], axis=0).astype(BF16)
        decay = decay_all[at, :]
        for o in (0, 1):
            wide = lax.dot_general(picks[o], three, NT, preferred_element_type=F32)
            lift[r, o] = jnp.where(own_t, wide, 0.0).astype(BF16)
            pair = held[at, pl.ds(2 * o, 2)]
            keep = [jnp.broadcast_to(decay[:, h : h + 1], (blk, 128))[:, None, :] for h in (2 * o, 2 * o + 1)]
            held[at, pl.ds(2 * o, 2)] = jnp.stack([keep[c] * pair[:, c] for c in (0, 1)], axis=1)
        return carry

    lax.fori_loop(0, rows // 2, prepare, 0)

    q2 = finish1(1, q1)

    small2.wait()
    total = small[x] + small_land2[0] + small_land2[1] + small_land2[2]
    scales[...] = jnp.concatenate([total, jnp.zeros((120, 128), F32)], axis=0).T
    raw = scales[pl.ds(pl.multiple_of(z * blk, blk), blk), :]
    q_scale = lax.rsqrt(1.0 + raw[:, 0:2])
    k_scale = lax.rsqrt(1.0 + raw[:, 2:4])
    unit_dot = raw[:, 4:6] * q_scale * k_scale
    decay = decay_all[mine, :]
    beta = 1.0 / (1.0 + jnp.exp(-proj[mine, 36:40]))

    g2 = {(o, name): copies.group() for o in (0, 1) for name in WAYS}
    near = {(o, name): copies.group() for o in (0, 1) for name in ("me", "left", "right", "far")}
    onward = [copies.group() for _ in (0, 1)]
    straight = [copies.group() for _ in (0, 1)]

    def send_near(o, name):
        r = rings1[o]
        b = rings2[o].me if name == "me" else rings2[o].at[name]
        piece = delta_all.at[o, :, r.me, b]
        for way in ("right", "left"):
            near[o, name].start(piece, piece, r.to[way])
        if name == "far":
            straight[o].start(piece, piece, r.to_far)

    def send_on(o, name):
        r = rings1[o]
        b = rings2[o].me if name == "me" else rings2[o].at[name]
        near[o, name].wait()
        for half, at, peer in ((0, r.left, r.to_right), (1, r.right, r.to_left)):
            piece = delta_all.at[o, half, at, b]
            onward[o].start(piece, piece, peer)

    deltas = []
    for o in (0, 1):
        finish2(o, 0, k1[o], k2[o])
        for c in (0, 1):
            h = 2 * o + c
            readk = own_piece(o, c, 0)[...] * k_scale[:, o : o + 1]
            value = both[h * blk : (h + 1) * blk, :128]
            delta = beta[:, h : h + 1] * (value - decay[:, h : h + 1] * readk)
            delta_all[o, c, rings1[o].me, rings2[o].me] = delta * k_scale[:, o : o + 1]
            deltas.append(delta)
        here = delta_all.at[o, :, rings1[o].me, rings2[o].me]
        for name in ("right", "left", "far"):
            g2[o, name].start(here, here, rings2[o].to[name])
    for o in (0, 1):
        send_near(o, "me")

    lax.fori_loop(rows // 2, rows, prepare, 0)
    for o in (0, 1):
        finish2(o, 1, q1[o], q2[o])
        for c in (0, 1):
            h = 2 * o + c
            old = own_piece(o, c, 1)[...] * q_scale[:, o : o + 1]
            readq = decay[:, h : h + 1] * old + unit_dot[:, o : o + 1] * deltas[h]
            meansq = jnp.mean(readq * readq, axis=-1, keepdims=True)
            gate = both[h * blk : (h + 1) * blk, 128:]
            gate = gate / (1.0 + jnp.exp(-gate))
            normed[:, h * 128 : (h + 1) * 128] = (readq * lax.rsqrt(meansq + 0.5) * gain[...] * gate).astype(BF16)

    load_weights[2].wait()
    width = outs.shape[-1]
    out_group = copies.group()
    chip, core = head // 2, lax.rem(head, 2)
    order_out = []
    for up, other in ((2, 0), (2, 1), (1, 0), (1, 1), (3, 0), (3, 1), (0, 1), (0, 0)):
        order_out.append(lax.rem(chip + up, HEADS // 2) * 2 + lax.rem(core + other, 2))
    for some in ((0, 1, 2, 3), (4, 5, 6, 7)):
        pieces = []
        for n in some:
            at = pl.ds(pl.multiple_of(order_out[n] * width, width), width)
            pieces.append(jnp.dot(normed[...], w_out[:, at], preferred_element_type=F32))
        for n, piece in zip(some, pieces):
            if n == 7:
                outs_land[head] = piece
            else:
                outs[n] = piece
        for n in some:
            if n == 7:
                continue
            out_group.start(outs.at[n], outs_land.at[head], {"head": order_out[n]})

    for o in (0, 1):
        for sent, name in (("right", "left"), ("left", "right")):
            g2[o, sent].wait()
            send_near(o, name)
    for o in (0, 1):
        send_on(o, "me")
        g2[o, "far"].wait()
        send_near(o, "far")
    for o in (0, 1):
        for name in ("left", "right"):
            send_on(o, name)

    def update_rows(o, first):
        for b in range(SIDE):
            r = row_at(o, first, b)
            at = pl.ds(pl.multiple_of(r * blk, blk), blk)
            add = growth(delta_all, lift, o, first, b, r)
            pair = held[at, pl.ds(2 * o, 2)]
            held[at, pl.ds(2 * o, 2)] = jnp.stack([pair[:, c] + add[c] for c in (0, 1)], axis=1)

    for o in (0, 1):
        update_rows(o, rings1[o].me)
    for o in (0, 1):
        near[o, "far"].wait()
    for o in (0, 1):
        update_rows(o, rings1[o].left)
        update_rows(o, rings1[o].right)
    out_group.wait()
    for o in (0, 1):
        onward[o].wait()
        straight[o].wait()
    copies.drain()


def finish_kernel(held, delta_all, lift, outs_land, layer_out, new_state, last, layer, sems):
    row = lax.axis_index("row")
    spots = (row // SIDE, lax.rem(row, SIDE))
    blk = held.shape[0] // (SIDE * SIDE)

    def store(src, o, r, count=1):
        dst = new_state.at[pl.ds(pl.multiple_of(r * blk, blk), count * blk), pl.ds(2 * o, 2)]
        pltpu.make_async_copy(src, dst, sems.at[0]).start()

    for d in (0, 1, 3):
        first = lax.rem(spots[0] + d, SIDE)
        at = pl.ds(pl.multiple_of(first * SIDE * blk, blk), SIDE * blk)
        store(held.at[at, pl.ds(0, 2)], 0, first * SIDE, SIDE)
        for b in range(SIDE):
            r = b * SIDE + lax.rem(spots[1] + d, SIDE)
            store(held.at[pl.ds(pl.multiple_of(r * blk, blk), blk), pl.ds(2, 2)], 1, r)
    total = outs_land[0]
    for n in range(1, HEADS):
        total = total + outs_land[n]
    layer[...] = total.astype(BF16)
    layer_copy = pltpu.make_async_copy(layer, layer_out, sems.at[1])
    layer_copy.start()
    for o in (0, 1):
        first = lax.rem(spots[o] + 2, SIDE)
        for b in range(SIDE):
            r = first * SIDE + b if o == 0 else b * SIDE + first
            at = pl.ds(pl.multiple_of(r * blk, blk), blk)
            add = growth(delta_all, lift, o, first, b, r)
            pair = held[at, pl.ds(2 * o, 2)]
            last[o * SIDE + b] = jnp.stack([pair[:, c] + add[c] for c in (0, 1)], axis=1)
            store(last.at[o * SIDE + b], o, r)
    layer_copy.wait()
    pltpu.make_async_copy(new_state, new_state, sems.at[0]).wait()


def local(
    hidden_in,
    w_query,
    w_key,
    w_value,
    w_zgate,
    w_decay,
    w_beta,
    decay_log,
    dt_bias,
    norm_gain,
    w_out,
    state,
):
    seqs, width = hidden_in.shape
    rows = SIDE * SIDE
    blk = seqs // rows
    vmem = pl.BlockSpec(memory_space=pltpu.VMEM)
    anywhere = pl.BlockSpec(memory_space=pltpu.HBM)
    held, delta_all, lift, outs_land = pl.pallas_call(
        exchange_kernel,
        out_shape=(
            pltpu.VMEM((seqs, PITCH // 8, 8, 128), F32),
            pltpu.VMEM((2, 2, SIDE, SIDE, blk, 128), F32),
            pltpu.VMEM((rows, 2, 8 * blk, 3 * blk), BF16),
            pltpu.VMEM((HEADS, blk, 256), F32),
        ),
        in_specs=[anywhere] * 12,
        out_specs=(vmem,) * 4,
        scratch_shapes=[
            pltpu.VMEM((2, 8, width), BF16),
            pltpu.VMEM((2, 8, width), BF16),
            pltpu.VMEM((4, width), BF16),
            pltpu.VMEM((4, width), BF16),
            pltpu.VMEM((1, 4), F32),
            pltpu.VMEM((1, 4), F32),
            pltpu.VMEM((1, 128), F32),
            pltpu.VMEM((seqs, width), BF16),
            pltpu.VMEM((4 * width, 128), BF16),
            pltpu.VMEM((4 * width, 128), BF16),
            pltpu.VMEM((512, width), BF16),
            pltpu.VMEM((seqs, 128), F32),
            pltpu.VMEM((seqs, 4), F32),
            pltpu.VMEM((2, 2, 2, SIDE, SIDE, blk, 128), F32),
            pltpu.VMEM((2, 2, 2, 3, SIDE, blk, 128), F32),
            pltpu.VMEM((2, 2, 3, 2, blk, 128), F32),
            pltpu.VMEM((SIDE, 8, 128), F32),
            pltpu.VMEM((6, 8, 128), F32),
            pltpu.VMEM((3, 8, 128), F32),
            pltpu.VMEM((128, 128), F32),
            pltpu.VMEM((blk, 512), BF16),
            pltpu.VMEM((HEADS, blk, 256), F32),
            pltpu.SemaphoreType.DMA((2 * SIDE,)),
            pltpu.SemaphoreType.DMA((11,)),
            pltpu.SemaphoreType.DMA((2,)),
            pltpu.SemaphoreType.DMA((51,)),
        ],
        compiler_params=pltpu.CompilerParams(
            collective_id=0, has_side_effects=True, vmem_limit_bytes=36 * 1024 * 1024
        ),
        name="exchange",
    )(
        *(
            pltpu.with_memory_space_constraint(operand, pltpu.HBM)
            for operand in (
                jnp.transpose(w_query, (1, 2, 0)),
                jnp.transpose(w_key, (1, 2, 0)),
                jnp.transpose(w_decay, (1, 0)),
                jnp.transpose(w_beta, (1, 0)),
                decay_log.reshape(1, 4),
                dt_bias.reshape(1, 4),
                norm_gain.reshape(1, 128),
                hidden_in,
                w_value.reshape(4 * width, 128),
                w_zgate.reshape(4 * width, 128),
                w_out.reshape(512, width),
                state,
            )
        )
    )
    layer_out, new_state = pl.pallas_call(
        finish_kernel,
        out_shape=(
            jax.ShapeDtypeStruct((blk, 256), BF16),
            jax.ShapeDtypeStruct(state.shape, F32),
        ),
        in_specs=[vmem] * 4,
        out_specs=(anywhere, anywhere),
        scratch_shapes=[
            pltpu.VMEM((2 * SIDE, blk, 2, 8, 128), F32),
            pltpu.VMEM((blk, 256), BF16),
            pltpu.SemaphoreType.DMA((2,)),
        ],
        compiler_params=pltpu.CompilerParams(vmem_limit_bytes=16 * 1024 * 1024),
        name="finish",
    )(*(pltpu.with_memory_space_constraint(a, pltpu.VMEM) for a in (held, delta_all, lift, outs_land)))
    return layer_out, new_state


def solution(mesh):
    in_specs = (
        P(),
        P(None, "head", "row"),
        P(None, "head", "row"),
        P(None, "head", None),
        P(None, "head", None),
        P(None, "head"),
        P(None, "head"),
        P("head"),
        P("head"),
        P(),
        P("head", None, None),
        P(None, "head", "row", None),
    )
    out_specs = (P("row", "head"), P(None, "head", "row", None))
    return jax.shard_map(local, mesh=mesh, in_specs=in_specs, out_specs=out_specs, check_vma=False)
```

```python
import math

import jax
import jax.numpy as jnp
from jax import lax
from jax.experimental import pallas as pl
from jax.experimental.pallas import tpu as pltpu
from jax.sharding import PartitionSpec as P

F32 = jnp.float32
BF16 = jnp.bfloat16
NT = (((1,), (1,)), ((), ()))
SIDE = 4
COLS = 40
HEADS = 8
PITCH = 40


def softplus(x):
    return jnp.maximum(x, 0.0) + jnp.log1p(jnp.exp(-jnp.abs(x)))


def size(ref):
    return math.prod(ref.shape) * jnp.dtype(ref.dtype).itemsize


class Group:
    def __init__(self, copies, sem, like):
        self.copies, self.sem, self.like, self.bytes = copies, sem, like, 0

    def start(self, src, dst, peer, count=True):
        if count:
            self.bytes += size(src)
            self.copies.sent[self.like is None].bytes += size(src)
        pltpu.make_async_remote_copy(
            src_ref=src,
            dst_ref=dst,
            send_sem=self.copies.sent[self.like is None].sem,
            recv_sem=self.sem,
            device_id=peer,
            device_id_type=pl.DeviceIdType.MESH,
        ).start()

    def wait(self):
        if self.like is None:
            rows = self.bytes // size(self.copies.held.at[0, pl.ds(0, 4)])
            ref = self.copies.held.at[pl.ds(0, rows), pl.ds(0, 4)]
        else:
            ref = self.like.at[pl.ds(0, self.bytes // size(self.like.at[0]))]
        pltpu.make_async_copy(ref, ref, self.sem).wait()


class Copies:
    def __init__(self, held, little, send, recv):
        self.held, self.recv, self.used = held, recv, 0
        self.sent = {True: Group(self, send.at[0], None), False: Group(self, send.at[1], little)}

    def group(self, like=None):
        self.used += 1
        return Group(self, self.recv.at[self.used - 1], like)

    def drain(self):
        for group in self.sent.values():
            group.wait()


class Ring:
    def __init__(self, me, row_of):
        self.me = me
        self.right = lax.rem(me + 1, SIDE)
        self.far = lax.rem(me + 2, SIDE)
        self.left = lax.rem(me + 3, SIDE)
        self.to_right = {"row": row_of(self.right)}
        self.to_far = {"row": row_of(self.far)}
        self.to_left = {"row": row_of(self.left)}
        self.at = {"far": self.far, "right": self.right, "left": self.left}
        self.to = {"far": self.to_far, "right": self.to_right, "left": self.to_left}


class Scatter:
    def __init__(self, copies, ring, pieces, part, land, fine):
        self.ring, self.pieces, self.part, self.land = ring, pieces, part, land
        self.relay = [copies.group() for _ in pieces] if fine else [copies.group()] * len(pieces)
        self.joint = [copies.group() for _ in pieces]

    def send_far(self, count=True):
        r = self.ring
        for n, b in enumerate(self.pieces):
            for half, peer in ((0, r.to_left), (1, r.to_right)):
                self.relay[n].start(self.part(half, r.far).at[b], self.land.at[half, 0, b], peer, count)

    def send_right(self):
        r = self.ring
        self.joint[0].start(self.part(0, r.right), self.land.at[0, 1], r.to_right)

    def send_left(self):
        r = self.ring
        self.joint[0].start(self.part(1, r.left), self.land.at[1, 1], r.to_left)

    def forward(self):
        r = self.ring
        for n, b in enumerate(self.pieces):
            if self.relay[n] not in self.relay[:n]:
                self.relay[n].wait()
            for half, to, peer in ((0, r.left, r.to_left), (1, r.right, r.to_right)):
                piece = self.part(half, to).at[b]
                piece[...] = piece[...] + self.land[half, 0, b]
                self.joint[n].start(piece, self.land.at[half, 2, b], peer)

    def finish(self, n):
        b = self.pieces[n]
        if self.joint[n] not in self.joint[:n]:
            self.joint[n].wait()
        for half in (0, 1):
            piece = self.part(half, self.ring.me).at[b]
            piece[...] = piece[...] + self.land[half, 1, b] + self.land[half, 2, b]


WAYS = ("far", "right", "left")


def split(x):
    hi = x.astype(BF16)
    return hi, (x - hi.astype(F32)).astype(BF16)


def growth(delta_all, lift, o, first, second, r):
    hi, lo = split(jnp.concatenate([delta_all[o, c, first, second] for c in (0, 1)], axis=1))
    add = jnp.dot(lift[r, o], jnp.concatenate([hi, lo, hi], axis=0), preferred_element_type=F32)
    return [add[:, c * 128 : (c + 1) * 128].reshape(hi.shape[0], 8, 128) for c in (0, 1)]


def exchange_kernel(
    wq_hbm,
    wk_hbm,
    wd_hbm,
    wb_hbm,
    decay_log_hbm,
    dt_bias_hbm,
    gain_hbm,
    hid_hbm,
    wv_hbm,
    wz_hbm,
    w_out_hbm,
    state,
    held,
    delta_all,
    lift,
    outs_land,
    wq,
    wk,
    wd,
    wb,
    decay_log,
    dt_bias,
    gain,
    hid,
    wv,
    wz,
    w_out,
    proj,
    decay_all,
    part,
    land1,
    land2,
    small,
    small_land1,
    small_land2,
    scales,
    normed,
    outs,
    picked,
    wide,
    load_sem,
    weight_sem,
    send_sem,
    recv_sem,
):
    row = lax.axis_index("row")
    head = lax.axis_index("head")
    x, z = row // SIDE, lax.rem(row, SIDE)
    rows = SIDE * SIDE
    blk = held.shape[0] // rows

    def row_at(o, first, second):
        return first * SIDE + second if o == 0 else second * SIDE + first

    first = []
    small_weights = ((wq_hbm, wq), (wk_hbm, wk), (wd_hbm, wd), (wb_hbm, wb))
    quarter = hid.shape[0] // 4
    pieces = tuple((hid_hbm.at[pl.ds(n * quarter, quarter)], hid.at[pl.ds(n * quarter, quarter)]) for n in range(4))
    for src, dst in pieces:
        pltpu.make_async_copy(src, dst, weight_sem.at[4]).start()
    for n, (src, dst) in enumerate(small_weights):
        first.append(pltpu.make_async_copy(src, dst, weight_sem.at[n]))
        first[-1].start()
    params = []
    for n, (src, dst) in enumerate(((decay_log_hbm, decay_log), (dt_bias_hbm, dt_bias), (gain_hbm, gain))):
        params.append(pltpu.make_async_copy(src, dst, weight_sem.at[8 + n]))
        params[-1].start()
    all_hid = pltpu.make_async_copy(hid, hid, weight_sem.at[4])

    barrier = pltpu.get_barrier_semaphore()
    peers = []
    for d in (1, 2, 3):
        peers.append({"row": lax.rem(x + d, SIDE) * SIDE + z})
        peers.append({"row": x * SIDE + lax.rem(z + d, SIDE)})
    for d in range(1, HEADS):
        peers.append({"head": lax.rem(head + d, HEADS)})
    for peer in peers:
        pl.semaphore_signal(barrier, inc=1, device_id=peer, device_id_type=pl.DeviceIdType.MESH)

    rings1 = [
        Ring(x, lambda a: row_at(0, a, z)),
        Ring(z, lambda a: row_at(1, a, x)),
    ]
    rings2 = [
        Ring(z, lambda b: row_at(0, x, b)),
        Ring(x, lambda b: row_at(1, z, b)),
    ]
    order = [[r.far, r.right, r.left, r.me] for r in rings1]

    def load(j, o):
        for b in range(SIDE):
            at = row_at(o, order[o][j], b) * blk
            pltpu.make_async_copy(
                state.at[pl.ds(at, blk), pl.ds(2 * o, 2)],
                held.at[pl.ds(at, blk), pl.ds(2 * o, 2)],
                load_sem.at[j * 2 + o],
            ).start()

    def await_load(j, o):
        ref = held.at[pl.ds(0, SIDE * blk // 2), pl.ds(0, 4)]
        pltpu.make_async_copy(ref, ref, load_sem.at[j * 2 + o]).wait()

    proj[...] = jnp.zeros_like(proj)
    for o in (0, 1):
        source = lax.broadcasted_iota(jnp.int32, (128, 1024), 0) % 64
        picked[o] = (source == 8 * o + lax.broadcasted_iota(jnp.int32, (128, 1024), 1) // 128).astype(F32).astype(BF16)
    for copy in first:
        copy.wait()
    load(0, 0)
    parts = [ref[n].astype(F32) for ref in (wq, wk) for n in (0, 1)] + [wd[...].astype(F32), wb[...].astype(F32)]
    w = jnp.concatenate(parts, axis=0).astype(BF16)
    swapped = jnp.concatenate(parts[2:4] + parts[:2] + parts[4:], axis=0).astype(BF16)
    all_hid.wait()
    load(0, 1)
    half = hid.shape[0] // 2
    upper = lax.dot_general(hid[:half, :], w, NT, preferred_element_type=F32)
    lower = lax.dot_general(hid[half:, :], swapped, NT, preferred_element_type=F32)
    proj[:half, :COLS] = upper
    proj[half:, 0:16] = lower[:, 16:32]
    proj[half:, 16:32] = lower[:, 0:16]
    proj[half:, 32:COLS] = lower[:, 32:COLS]
    for j in (1, 2, 3):
        for o in (0, 1):
            load(j, o)

    copies = Copies(held, small_land1, send_sem, recv_sem)
    flat = held.reshape(held.shape[0] * PITCH, 128)

    def read_blocks(o, first):
        starts = [pl.multiple_of(row_at(o, first, b) * blk, blk) for b in range(SIDE)]
        vecs = [proj[pl.ds(at, blk), :] for at in starts]
        hi, lo = split(jnp.concatenate(vecs, axis=0))
        both_terms = (hi.astype(F32) + pltpu.roll(lo.astype(F32), 64, 1)).astype(BF16)
        wide[...] = jnp.dot(both_terms, picked[o], preferred_element_type=F32)
        for b, at in enumerate(starts):
            for g in range(blk // 8):
                mine = slice(g * 8, (g + 1) * 8)
                sums = [[None, None], [None, None]]
                for i in range(8):
                    n = 16 + 8 * o + i
                    key = jnp.broadcast_to(vecs[b][mine, n : n + 1], (8, 128))
                    query = wide[b * blk + g * 8 : b * blk + (g + 1) * 8, i * 128 : (i + 1) * 128]
                    for c in (0, 1):
                        start = (at + g * 8) * PITCH + (2 * o + c) * 8 + i
                        values = flat[pl.ds(start, 8, stride=PITCH), :]
                        for t, vector in ((0, key), (1, query)):
                            term = vector * values
                            sums[t][c] = term if i == 0 else sums[t][c] + term
                for c in (0, 1):
                    for t in (0, 1):
                        part[o, c, t, first, b, mine] = sums[t][c]

    def send_sums():
        for a in range(SIDE):
            cols = proj[a * 128 : (a + 1) * 128, :].T
            terms = []
            for u, v in ((0, 0), (16, 16), (0, 16)):
                for hk in (0, 8):
                    product = cols[u + hk : u + hk + 8] * cols[v + hk : v + hk + 8]
                    terms.append(jnp.sum(product, axis=0, keepdims=True))
            terms.append(jnp.zeros((2, 128), F32))
            small[a] = jnp.concatenate(terms, axis=0)
        group = copies.group(small_land1)
        for n, name in enumerate(WAYS):
            group.start(small.at[rings1[0].at[name]], small_land1.at[n], rings1[0].to[name])
        return group

    def scatter1(o, t):
        r = rings2[o]
        pieces = (r.far, r.right, r.left, r.me)
        return Scatter(copies, rings1[o], pieces, lambda c, a: part.at[o, c, t, a], land1.at[o, t], t == 0)

    def own_piece(o, c, t):
        return part.at[o, c, t, rings1[o].me, rings2[o].me]

    def finish1(t, scatters):
        groups = [copies.group() for _ in scatters]
        for n, name in enumerate(WAYS):
            for o, s in enumerate(scatters):
                r = rings2[o]
                s.finish(n)
                groups[o].start(part.at[o, :, t, rings1[o].me, r.at[name]], land2.at[o, t, n], r.to[name])
        return groups

    def finish2(o, t, first, s):
        first.finish(3)
        s.wait()
        for c in (0, 1):
            piece = own_piece(o, c, t)
            piece[...] = piece[...] + land2[o, t, 0, c] + land2[o, t, 1, c] + land2[o, t, 2, c]

    k1 = [scatter1(o, 0) for o in (0, 1)]
    q1 = [scatter1(o, 1) for o in (0, 1)]

    for j in range(SIDE):
        for o in (0, 1):
            await_load(j, o)
            if j == 0:
                read_blocks(o, order[o][j])
                if o == 0:
                    pl.semaphore_wait(barrier, len(peers))
                k1[o].send_far()
        if j == 0:
            small1 = send_sums()

            @pl.when(lax.rem(head, 2) == 0)
            def _():
                for o in (0, 1):
                    q1[o].send_far()

        else:
            for o in (0, 1):
                read_blocks(o, order[o][j])
        if j == 1:
            for o in (0, 1):
                k1[o].send_right()
            load_weights = []
            for n, (src, dst) in enumerate(((wv_hbm, wv), (wz_hbm, wz), (w_out_hbm, w_out))):
                load_weights.append(pltpu.make_async_copy(src, dst, weight_sem.at[n + 5]))
                load_weights[-1].start()
        if j == 2:
            for o in (0, 1):
                k1[o].send_left()
    for s in k1:
        s.forward()

    @pl.when(lax.rem(head, 2) == 1)
    def _():
        for o in (0, 1):
            q1[o].send_far(count=False)

    for s in q1:
        s.send_right()
        s.send_left()
    small1.wait()
    small[x] = small[x] + small_land1[0] + small_land1[1] + small_land1[2]
    small2 = copies.group(small_land2)
    for n, name in enumerate(WAYS):
        small2.start(small.at[x], small_land2.at[n], rings2[0].to[name])

    mine = pl.ds(pl.multiple_of(row * blk, blk), blk)
    own_hid = hid[mine, :]
    chunks = own_hid.shape[1] // 256
    tall = jnp.concatenate([own_hid[:, n * 256 : (n + 1) * 256] for n in range(chunks)], axis=0)
    repeat = (
        lax.broadcasted_iota(jnp.int32, (256, 1024), 1) // 4 == lax.broadcasted_iota(jnp.int32, (256, 1024), 0)
    ).astype(F32).astype(BF16)
    tall = jnp.dot(tall, repeat, preferred_element_type=F32)
    at_head = lax.broadcasted_iota(jnp.int32, (blk, 1024), 1) % 4
    load_weights[0].wait()
    load_weights[1].wait()
    both = jnp.zeros((4 * blk, 256), F32)
    for n in range(chunks):
        piece = tall[n * blk : (n + 1) * blk]
        piece = jnp.concatenate([jnp.where(at_head == h, piece, 0.0).astype(BF16) for h in range(4)], axis=0)
        at = slice(n * 1024, (n + 1) * 1024)
        weights = jnp.concatenate([wv[at, :], wz[at, :]], axis=1)
        both = both + jnp.dot(piece, weights, preferred_element_type=F32)

    for s in q1:
        s.forward()
    k2 = finish1(0, k1)

    for copy in params:
        copy.wait()
    decay_all[...] = jnp.exp(-jnp.exp(decay_log[...]) * softplus(proj[:, 32:36] + dt_bias[...]))
    own_t = lax.broadcasted_iota(jnp.int32, (8 * blk, 3 * blk), 0) // 8 == lax.rem(
        lax.broadcasted_iota(jnp.int32, (8 * blk, 3 * blk), 1), blk
    )
    picks = [
        (
            lax.broadcasted_iota(jnp.int32, (8 * blk, COLS), 1)
            == 16 + 8 * o + lax.broadcasted_iota(jnp.int32, (8 * blk, COLS), 0) % 8
        )
        .astype(F32)
        .astype(BF16)
        for o in (0, 1)
    ]

    def prepare(r, carry):
        at = pl.ds(pl.multiple_of(r * blk, blk), blk)
        hi, lo = split(proj[at, :COLS])
        three = jnp.concatenate([hi.astype(F32), hi.astype(F32), lo.astype(F32)], axis=0).astype(BF16)
        decay = decay_all[at, :]
        for o in (0, 1):
            wide = lax.dot_general(picks[o], three, NT, preferred_element_type=F32)
            lift[r, o] = jnp.where(own_t, wide, 0.0).astype(BF16)
            pair = held[at, pl.ds(2 * o, 2)]
            keep = [jnp.broadcast_to(decay[:, h : h + 1], (blk, 128))[:, None, :] for h in (2 * o, 2 * o + 1)]
            held[at, pl.ds(2 * o, 2)] = jnp.stack([keep[c] * pair[:, c] for c in (0, 1)], axis=1)
        return carry

    lax.fori_loop(0, rows // 2, prepare, 0)

    q2 = finish1(1, q1)

    small2.wait()
    total = small[x] + small_land2[0] + small_land2[1] + small_land2[2]
    scales[...] = jnp.concatenate([total, jnp.zeros((120, 128), F32)], axis=0).T
    raw = scales[pl.ds(pl.multiple_of(z * blk, blk), blk), :]
    q_scale = lax.rsqrt(1.0 + raw[:, 0:2])
    k_scale = lax.rsqrt(1.0 + raw[:, 2:4])
    unit_dot = raw[:, 4:6] * q_scale * k_scale
    decay = decay_all[mine, :]
    beta = 1.0 / (1.0 + jnp.exp(-proj[mine, 36:40]))

    g2 = {(o, name): copies.group() for o in (0, 1) for name in WAYS}
    near = {(o, name): copies.group() for o in (0, 1) for name in ("me", "left", "right", "far")}
    onward = [copies.group() for _ in (0, 1)]
    straight = [copies.group() for _ in (0, 1)]

    def send_near(o, name):
        r = rings1[o]
        b = rings2[o].me if name == "me" else rings2[o].at[name]
        piece = delta_all.at[o, :, r.me, b]
        for way in ("right", "left"):
            near[o, name].start(piece, piece, r.to[way])
        if name == "far":
            straight[o].start(piece, piece, r.to_far)

    def send_on(o, name):
        r = rings1[o]
        b = rings2[o].me if name == "me" else rings2[o].at[name]
        near[o, name].wait()
        for half, at, peer in ((0, r.left, r.to_right), (1, r.right, r.to_left)):
            piece = delta_all.at[o, half, at, b]
            onward[o].start(piece, piece, peer)

    deltas = []
    for o in (0, 1):
        finish2(o, 0, k1[o], k2[o])
        for c in (0, 1):
            h = 2 * o + c
            readk = own_piece(o, c, 0)[...] * k_scale[:, o : o + 1]
            value = both[h * blk : (h + 1) * blk, :128]
            delta = beta[:, h : h + 1] * (value - decay[:, h : h + 1] * readk)
            delta_all[o, c, rings1[o].me, rings2[o].me] = delta * k_scale[:, o : o + 1]
            deltas.append(delta)
        here = delta_all.at[o, :, rings1[o].me, rings2[o].me]
        for name in ("right", "left", "far"):
            g2[o, name].start(here, here, rings2[o].to[name])
    for o in (0, 1):
        send_near(o, "me")

    lax.fori_loop(rows // 2, rows, prepare, 0)
    for o in (0, 1):
        finish2(o, 1, q1[o], q2[o])
        for c in (0, 1):
            h = 2 * o + c
            old = own_piece(o, c, 1)[...] * q_scale[:, o : o + 1]
            readq = decay[:, h : h + 1] * old + unit_dot[:, o : o + 1] * deltas[h]
            meansq = jnp.mean(readq * readq, axis=-1, keepdims=True)
            gate = both[h * blk : (h + 1) * blk, 128:]
            gate = gate / (1.0 + jnp.exp(-gate))
            normed[:, h * 128 : (h + 1) * 128] = (readq * lax.rsqrt(meansq + 0.5) * gain[...] * gate).astype(BF16)

    load_weights[2].wait()
    width = outs.shape[-1]
    out_group = copies.group()
    chip, core = head // 2, lax.rem(head, 2)
    order_out = []
    for up, other in ((2, 0), (2, 1), (1, 0), (1, 1), (3, 0), (3, 1), (0, 1), (0, 0)):
        order_out.append(lax.rem(chip + up, HEADS // 2) * 2 + lax.rem(core + other, 2))
    for some in ((0, 1, 2, 3), (4, 5, 6, 7)):
        pieces = []
        for n in some:
            at = pl.ds(pl.multiple_of(order_out[n] * width, width), width)
            pieces.append(jnp.dot(normed[...], w_out[:, at], preferred_element_type=F32))
        for n, piece in zip(some, pieces):
            if n == 7:
                outs_land[head] = piece
            else:
                outs[n] = piece
        for n in some:
            if n == 7:
                continue
            out_group.start(outs.at[n], outs_land.at[head], {"head": order_out[n]})

    for o in (0, 1):
        for sent, name in (("right", "left"), ("left", "right")):
            g2[o, sent].wait()
            send_near(o, name)
    for o in (0, 1):
        send_on(o, "me")
        g2[o, "far"].wait()
        send_near(o, "far")
    for o in (0, 1):
        for name in ("left", "right"):
            send_on(o, name)

    def update_rows(o, first):
        for b in range(SIDE):
            r = row_at(o, first, b)
            at = pl.ds(pl.multiple_of(r * blk, blk), blk)
            add = growth(delta_all, lift, o, first, b, r)
            pair = held[at, pl.ds(2 * o, 2)]
            held[at, pl.ds(2 * o, 2)] = jnp.stack([pair[:, c] + add[c] for c in (0, 1)], axis=1)

    for o in (0, 1):
        update_rows(o, rings1[o].me)
    for o in (0, 1):
        near[o, "far"].wait()
    for o in (0, 1):
        update_rows(o, rings1[o].left)
        update_rows(o, rings1[o].right)
    out_group.wait()
    for o in (0, 1):
        onward[o].wait()
        straight[o].wait()
    copies.drain()


def finish_kernel(held, delta_all, lift, outs_land, layer_out, new_state, last, layer, sems):
    row = lax.axis_index("row")
    spots = (row // SIDE, lax.rem(row, SIDE))
    blk = held.shape[0] // (SIDE * SIDE)

    def store(src, o, r, count=1):
        dst = new_state.at[pl.ds(pl.multiple_of(r * blk, blk), count * blk), pl.ds(2 * o, 2)]
        pltpu.make_async_copy(src, dst, sems.at[0]).start()

    for d in (0, 1, 3):
        first = lax.rem(spots[0] + d, SIDE)
        at = pl.ds(pl.multiple_of(first * SIDE * blk, blk), SIDE * blk)
        store(held.at[at, pl.ds(0, 2)], 0, first * SIDE, SIDE)
        for b in range(SIDE):
            r = b * SIDE + lax.rem(spots[1] + d, SIDE)
            store(held.at[pl.ds(pl.multiple_of(r * blk, blk), blk), pl.ds(2, 2)], 1, r)
    total = outs_land[0]
    for n in range(1, HEADS):
        total = total + outs_land[n]
    layer[...] = total.astype(BF16)
    layer_copy = pltpu.make_async_copy(layer, layer_out, sems.at[1])
    layer_copy.start()
    for o in (0, 1):
        first = lax.rem(spots[o] + 2, SIDE)
        for b in range(SIDE):
            r = first * SIDE + b if o == 0 else b * SIDE + first
            at = pl.ds(pl.multiple_of(r * blk, blk), blk)
            add = growth(delta_all, lift, o, first, b, r)
            pair = held[at, pl.ds(2 * o, 2)]
            last[o * SIDE + b] = jnp.stack([pair[:, c] + add[c] for c in (0, 1)], axis=1)
            store(last.at[o * SIDE + b], o, r)
    layer_copy.wait()
    pltpu.make_async_copy(new_state, new_state, sems.at[0]).wait()


def local(
    hidden_in,
    w_query,
    w_key,
    w_value,
    w_zgate,
    w_decay,
    w_beta,
    decay_log,
    dt_bias,
    norm_gain,
    w_out,
    state,
):
    seqs, width = hidden_in.shape
    rows = SIDE * SIDE
    blk = seqs // rows
    vmem = pl.BlockSpec(memory_space=pltpu.VMEM)
    anywhere = pl.BlockSpec(memory_space=pltpu.HBM)
    held, delta_all, lift, outs_land = pl.pallas_call(
        exchange_kernel,
        out_shape=(
            pltpu.VMEM((seqs, PITCH // 8, 8, 128), F32),
            pltpu.VMEM((2, 2, SIDE, SIDE, blk, 128), F32),
            pltpu.VMEM((rows, 2, 8 * blk, 3 * blk), BF16),
            pltpu.VMEM((HEADS, blk, 256), F32),
        ),
        in_specs=[anywhere] * 12,
        out_specs=(vmem,) * 4,
        scratch_shapes=[
            pltpu.VMEM((2, 8, width), BF16),
            pltpu.VMEM((2, 8, width), BF16),
            pltpu.VMEM((4, width), BF16),
            pltpu.VMEM((4, width), BF16),
            pltpu.VMEM((1, 4), F32),
            pltpu.VMEM((1, 4), F32),
            pltpu.VMEM((1, 128), F32),
            pltpu.VMEM((seqs, width), BF16),
            pltpu.VMEM((4 * width, 128), BF16),
            pltpu.VMEM((4 * width, 128), BF16),
            pltpu.VMEM((512, width), BF16),
            pltpu.VMEM((seqs, 128), F32),
            pltpu.VMEM((seqs, 4), F32),
            pltpu.VMEM((2, 2, 2, SIDE, SIDE, blk, 128), F32),
            pltpu.VMEM((2, 2, 2, 3, SIDE, blk, 128), F32),
            pltpu.VMEM((2, 2, 3, 2, blk, 128), F32),
            pltpu.VMEM((SIDE, 8, 128), F32),
            pltpu.VMEM((6, 8, 128), F32),
            pltpu.VMEM((3, 8, 128), F32),
            pltpu.VMEM((128, 128), F32),
            pltpu.VMEM((blk, 512), BF16),
            pltpu.VMEM((HEADS, blk, 256), F32),
            pltpu.VMEM((2, 128, 1024), BF16),
            pltpu.VMEM((SIDE * blk, 1024), F32),
            pltpu.SemaphoreType.DMA((2 * SIDE,)),
            pltpu.SemaphoreType.DMA((11,)),
            pltpu.SemaphoreType.DMA((2,)),
            pltpu.SemaphoreType.DMA((51,)),
        ],
        compiler_params=pltpu.CompilerParams(
            collective_id=0, has_side_effects=True, vmem_limit_bytes=36 * 1024 * 1024
        ),
        name="exchange",
    )(
        *(
            pltpu.with_memory_space_constraint(operand, pltpu.HBM)
            for operand in (
                jnp.transpose(w_query, (1, 2, 0)),
                jnp.transpose(w_key, (1, 2, 0)),
                jnp.transpose(w_decay, (1, 0)),
                jnp.transpose(w_beta, (1, 0)),
                decay_log.reshape(1, 4),
                dt_bias.reshape(1, 4),
                norm_gain.reshape(1, 128),
                hidden_in,
                w_value.reshape(4 * width, 128),
                w_zgate.reshape(4 * width, 128),
                w_out.reshape(512, width),
                state,
            )
        )
    )
    layer_out, new_state = pl.pallas_call(
        finish_kernel,
        out_shape=(
            jax.ShapeDtypeStruct((blk, 256), BF16),
            jax.ShapeDtypeStruct(state.shape, F32),
        ),
        in_specs=[vmem] * 4,
        out_specs=(anywhere, anywhere),
        scratch_shapes=[
            pltpu.VMEM((2 * SIDE, blk, 2, 8, 128), F32),
            pltpu.VMEM((blk, 256), BF16),
            pltpu.SemaphoreType.DMA((2,)),
        ],
        compiler_params=pltpu.CompilerParams(vmem_limit_bytes=16 * 1024 * 1024),
        name="finish",
    )(*(pltpu.with_memory_space_constraint(a, pltpu.VMEM) for a in (held, delta_all, lift, outs_land)))
    return layer_out, new_state


def solution(mesh):
    in_specs = (
        P(),
        P(None, "head", "row"),
        P(None, "head", "row"),
        P(None, "head", None),
        P(None, "head", None),
        P(None, "head"),
        P(None, "head"),
        P("head"),
        P("head"),
        P(),
        P("head", None, None),
        P(None, "head", "row", None),
    )
    out_specs = (P("row", "head"), P(None, "head", "row", None))
    return jax.shard_map(local, mesh=mesh, in_specs=in_specs, out_specs=out_specs, check_vma=False)
```

```python
import math

import jax
import jax.numpy as jnp
from jax import lax
from jax.experimental import pallas as pl
from jax.experimental.pallas import tpu as pltpu
from jax.sharding import PartitionSpec as P

F32 = jnp.float32
BF16 = jnp.bfloat16
NT = (((1,), (1,)), ((), ()))
SIDE = 4
COLS = 40
HEADS = 8
PITCH = 40


def softplus(x):
    return jnp.maximum(x, 0.0) + jnp.log1p(jnp.exp(-jnp.abs(x)))


def size(ref):
    return math.prod(ref.shape) * jnp.dtype(ref.dtype).itemsize


class Group:
    def __init__(self, copies, sem, like):
        self.copies, self.sem, self.like, self.bytes = copies, sem, like, 0

    def start(self, src, dst, peer, count=True):
        if count:
            self.bytes += size(src)
            self.copies.sent[self.like is None].bytes += size(src)
        pltpu.make_async_remote_copy(
            src_ref=src,
            dst_ref=dst,
            send_sem=self.copies.sent[self.like is None].sem,
            recv_sem=self.sem,
            device_id=peer,
            device_id_type=pl.DeviceIdType.MESH,
        ).start()

    def wait(self):
        if self.like is None:
            rows = self.bytes // size(self.copies.held.at[0, pl.ds(0, 4)])
            ref = self.copies.held.at[pl.ds(0, rows), pl.ds(0, 4)]
        else:
            ref = self.like.at[pl.ds(0, self.bytes // size(self.like.at[0]))]
        pltpu.make_async_copy(ref, ref, self.sem).wait()


class Copies:
    def __init__(self, held, little, send, recv):
        self.held, self.recv, self.used = held, recv, 0
        self.sent = {True: Group(self, send.at[0], None), False: Group(self, send.at[1], little)}

    def group(self, like=None):
        self.used += 1
        return Group(self, self.recv.at[self.used - 1], like)

    def drain(self):
        for group in self.sent.values():
            group.wait()


class Ring:
    def __init__(self, me, row_of):
        self.me = me
        self.right = lax.rem(me + 1, SIDE)
        self.far = lax.rem(me + 2, SIDE)
        self.left = lax.rem(me + 3, SIDE)
        self.to_right = {"row": row_of(self.right)}
        self.to_far = {"row": row_of(self.far)}
        self.to_left = {"row": row_of(self.left)}
        self.at = {"far": self.far, "right": self.right, "left": self.left}
        self.to = {"far": self.to_far, "right": self.to_right, "left": self.to_left}


class Scatter:
    def __init__(self, copies, ring, pieces, part, land, fine):
        self.ring, self.pieces, self.part, self.land = ring, pieces, part, land
        self.relay = [copies.group() for _ in pieces] if fine else [copies.group()] * len(pieces)
        self.joint = [copies.group() for _ in pieces]

    def send_far(self, count=True):
        r = self.ring
        for n, b in enumerate(self.pieces):
            for half, peer in ((0, r.to_left), (1, r.to_right)):
                self.relay[n].start(self.part(half, r.far).at[b], self.land.at[half, 0, b], peer, count)

    def send_right(self):
        r = self.ring
        self.joint[0].start(self.part(0, r.right), self.land.at[0, 1], r.to_right)

    def send_left(self):
        r = self.ring
        self.joint[0].start(self.part(1, r.left), self.land.at[1, 1], r.to_left)

    def forward(self):
        r = self.ring
        for n, b in enumerate(self.pieces):
            if self.relay[n] not in self.relay[:n]:
                self.relay[n].wait()
            for half, to, peer in ((0, r.left, r.to_left), (1, r.right, r.to_right)):
                piece = self.part(half, to).at[b]
                piece[...] = piece[...] + self.land[half, 0, b]
                self.joint[n].start(piece, self.land.at[half, 2, b], peer)

    def finish(self, n):
        b = self.pieces[n]
        if self.joint[n] not in self.joint[:n]:
            self.joint[n].wait()
        for half in (0, 1):
            piece = self.part(half, self.ring.me).at[b]
            piece[...] = piece[...] + self.land[half, 1, b] + self.land[half, 2, b]


WAYS = ("far", "right", "left")


def split(x):
    hi = x.astype(BF16)
    return hi, (x - hi.astype(F32)).astype(BF16)


def growth(delta_all, lift, o, first, second, r):
    hi, lo = split(jnp.concatenate([delta_all[o, c, first, second] for c in (0, 1)], axis=1))
    add = jnp.dot(lift[r, o], jnp.concatenate([hi, lo, hi], axis=0), preferred_element_type=F32)
    return [add[:, c * 128 : (c + 1) * 128].reshape(hi.shape[0], 8, 128) for c in (0, 1)]


def exchange_kernel(
    wq_hbm,
    wk_hbm,
    wd_hbm,
    wb_hbm,
    decay_log_hbm,
    dt_bias_hbm,
    gain_hbm,
    hid_hbm,
    wv_hbm,
    wz_hbm,
    w_out_hbm,
    state,
    held,
    delta_all,
    lift,
    outs_land,
    wq,
    wk,
    wd,
    wb,
    decay_log,
    dt_bias,
    gain,
    hid,
    wv,
    wz,
    w_out,
    proj,
    decay_all,
    part,
    land1,
    land2,
    small,
    small_land1,
    small_land2,
    scales,
    normed,
    outs,
    picked,
    wide,
    load_sem,
    weight_sem,
    send_sem,
    recv_sem,
):
    row = lax.axis_index("row")
    head = lax.axis_index("head")
    x, z = row // SIDE, lax.rem(row, SIDE)
    rows = SIDE * SIDE
    blk = held.shape[0] // rows

    def row_at(o, first, second):
        return first * SIDE + second if o == 0 else second * SIDE + first

    first = []
    small_weights = ((wq_hbm, wq), (wk_hbm, wk), (wd_hbm, wd), (wb_hbm, wb))
    quarter = hid.shape[0] // 4
    pieces = tuple((hid_hbm.at[pl.ds(n * quarter, quarter)], hid.at[pl.ds(n * quarter, quarter)]) for n in range(4))
    for src, dst in pieces:
        pltpu.make_async_copy(src, dst, weight_sem.at[4]).start()
    for n, (src, dst) in enumerate(small_weights):
        first.append(pltpu.make_async_copy(src, dst, weight_sem.at[n]))
        first[-1].start()
    params = []
    for n, (src, dst) in enumerate(((decay_log_hbm, decay_log), (dt_bias_hbm, dt_bias), (gain_hbm, gain))):
        params.append(pltpu.make_async_copy(src, dst, weight_sem.at[8 + n]))
        params[-1].start()
    all_hid = pltpu.make_async_copy(hid, hid, weight_sem.at[4])

    barrier = pltpu.get_barrier_semaphore()
    peers = []
    for d in (1, 2, 3):
        peers.append({"row": lax.rem(x + d, SIDE) * SIDE + z})
        peers.append({"row": x * SIDE + lax.rem(z + d, SIDE)})
    for d in range(1, HEADS):
        peers.append({"head": lax.rem(head + d, HEADS)})
    for peer in peers:
        pl.semaphore_signal(barrier, inc=1, device_id=peer, device_id_type=pl.DeviceIdType.MESH)

    rings1 = [
        Ring(x, lambda a: row_at(0, a, z)),
        Ring(z, lambda a: row_at(1, a, x)),
    ]
    rings2 = [
        Ring(z, lambda b: row_at(0, x, b)),
        Ring(x, lambda b: row_at(1, z, b)),
    ]
    order = [[r.far, r.right, r.left, r.me] for r in rings1]

    def load(j, o):
        for b in range(SIDE):
            at = row_at(o, order[o][j], b) * blk
            pltpu.make_async_copy(
                state.at[pl.ds(at, blk), pl.ds(2 * o, 2)],
                held.at[pl.ds(at, blk), pl.ds(2 * o, 2)],
                load_sem.at[j * 2 + o],
            ).start()

    def await_load(j, o):
        ref = held.at[pl.ds(0, SIDE * blk // 2), pl.ds(0, 4)]
        pltpu.make_async_copy(ref, ref, load_sem.at[j * 2 + o]).wait()

    proj[...] = jnp.zeros_like(proj)
    for o in (0, 1):
        source = lax.broadcasted_iota(jnp.int32, (128, 1024), 0) % 64
        picked[o] = (source == 8 * o + lax.broadcasted_iota(jnp.int32, (128, 1024), 1) // 128).astype(F32).astype(BF16)
    with jax.named_scope("p01"):
        for copy in first:
            copy.wait()
    load(0, 0)
    parts = [ref[n].astype(F32) for ref in (wq, wk) for n in (0, 1)] + [wd[...].astype(F32), wb[...].astype(F32)]
    w = jnp.concatenate(parts, axis=0).astype(BF16)
    swapped = jnp.concatenate(parts[2:4] + parts[:2] + parts[4:], axis=0).astype(BF16)
    with jax.named_scope("p02"):
        all_hid.wait()
    load(0, 1)
    half = hid.shape[0] // 2
    with jax.named_scope("p03"):
        upper = lax.dot_general(hid[:half, :], w, NT, preferred_element_type=F32)
    with jax.named_scope("p04"):
        lower = lax.dot_general(hid[half:, :], swapped, NT, preferred_element_type=F32)
    proj[:half, :COLS] = upper
    proj[half:, 0:16] = lower[:, 16:32]
    proj[half:, 16:32] = lower[:, 0:16]
    proj[half:, 32:COLS] = lower[:, 32:COLS]
    for j in (1, 2, 3):
        for o in (0, 1):
            load(j, o)

    with jax.named_scope("p05"):
        copies = Copies(held, small_land1, send_sem, recv_sem)
    flat = held.reshape(held.shape[0] * PITCH, 128)

    def read_blocks(o, first):
        starts = [pl.multiple_of(row_at(o, first, b) * blk, blk) for b in range(SIDE)]
        vecs = [proj[pl.ds(at, blk), :] for at in starts]
        hi, lo = split(jnp.concatenate(vecs, axis=0))
        both_terms = (hi.astype(F32) + pltpu.roll(lo.astype(F32), 64, 1)).astype(BF16)
        wide[...] = jnp.dot(both_terms, picked[o], preferred_element_type=F32)
        for b, at in enumerate(starts):
            for g in range(blk // 8):
                mine = slice(g * 8, (g + 1) * 8)
                sums = [[None, None], [None, None]]
                for i in range(8):
                    n = 16 + 8 * o + i
                    key = jnp.broadcast_to(vecs[b][mine, n : n + 1], (8, 128))
                    query = wide[b * blk + g * 8 : b * blk + (g + 1) * 8, i * 128 : (i + 1) * 128]
                    for c in (0, 1):
                        start = (at + g * 8) * PITCH + (2 * o + c) * 8 + i
                        values = flat[pl.ds(start, 8, stride=PITCH), :]
                        for t, vector in ((0, key), (1, query)):
                            term = vector * values
                            sums[t][c] = term if i == 0 else sums[t][c] + term
                for c in (0, 1):
                    for t in (0, 1):
                        part[o, c, t, first, b, mine] = sums[t][c]

    def send_sums():
        for a in range(SIDE):
            cols = proj[a * 128 : (a + 1) * 128, :].T
            terms = []
            for u, v in ((0, 0), (16, 16), (0, 16)):
                for hk in (0, 8):
                    product = cols[u + hk : u + hk + 8] * cols[v + hk : v + hk + 8]
                    terms.append(jnp.sum(product, axis=0, keepdims=True))
            terms.append(jnp.zeros((2, 128), F32))
            small[a] = jnp.concatenate(terms, axis=0)
        group = copies.group(small_land1)
        for n, name in enumerate(WAYS):
            group.start(small.at[rings1[0].at[name]], small_land1.at[n], rings1[0].to[name])
        return group

    def scatter1(o, t):
        r = rings2[o]
        pieces = (r.far, r.right, r.left, r.me)
        return Scatter(copies, rings1[o], pieces, lambda c, a: part.at[o, c, t, a], land1.at[o, t], t == 0)

    def own_piece(o, c, t):
        return part.at[o, c, t, rings1[o].me, rings2[o].me]

    def finish1(t, scatters):
        groups = [copies.group() for _ in scatters]
        for n, name in enumerate(WAYS):
            for o, s in enumerate(scatters):
                r = rings2[o]
                s.finish(n)
                groups[o].start(part.at[o, :, t, rings1[o].me, r.at[name]], land2.at[o, t, n], r.to[name])
        return groups

    def finish2(o, t, first, s):
        first.finish(3)
        s.wait()
        for c in (0, 1):
            piece = own_piece(o, c, t)
            piece[...] = piece[...] + land2[o, t, 0, c] + land2[o, t, 1, c] + land2[o, t, 2, c]

    k1 = [scatter1(o, 0) for o in (0, 1)]
    q1 = [scatter1(o, 1) for o in (0, 1)]

    for j in range(SIDE):
        for o in (0, 1):
            with jax.named_scope(f"wait{j}"):
                await_load(j, o)
            if j == 0:
                with jax.named_scope(f"read{j}{o}"):
                    read_blocks(o, order[o][j])
                    if o == 0:
                        pl.semaphore_wait(barrier, len(peers))
                k1[o].send_far()
        if j == 0:
            with jax.named_scope("sums"):
                small1 = send_sums()

            @pl.when(lax.rem(head, 2) == 0)
            def _():
                for o in (0, 1):
                    q1[o].send_far()

        else:
            with jax.named_scope(f"read{j}"):
                for o in (0, 1):
                    read_blocks(o, order[o][j])
        if j == 1:
            for o in (0, 1):
                k1[o].send_right()
            load_weights = []
            for n, (src, dst) in enumerate(((wv_hbm, wv), (wz_hbm, wz), (w_out_hbm, w_out))):
                load_weights.append(pltpu.make_async_copy(src, dst, weight_sem.at[n + 5]))
                load_weights[-1].start()
        if j == 2:
            for o in (0, 1):
                k1[o].send_left()
    with jax.named_scope("p07"):
        for s in k1:
            s.forward()

    @pl.when(lax.rem(head, 2) == 1)
    def _():
        for o in (0, 1):
            q1[o].send_far(count=False)

    with jax.named_scope("p08"):
        for s in q1:
            s.send_right()
            s.send_left()
    with jax.named_scope("p09"):
        small1.wait()
    small[x] = small[x] + small_land1[0] + small_land1[1] + small_land1[2]
    small2 = copies.group(small_land2)
    for n, name in enumerate(WAYS):
        small2.start(small.at[x], small_land2.at[n], rings2[0].to[name])

    mine = pl.ds(pl.multiple_of(row * blk, blk), blk)
    own_hid = hid[mine, :]
    chunks = own_hid.shape[1] // 256
    tall = jnp.concatenate([own_hid[:, n * 256 : (n + 1) * 256] for n in range(chunks)], axis=0)
    repeat = (
        lax.broadcasted_iota(jnp.int32, (256, 1024), 1) // 4 == lax.broadcasted_iota(jnp.int32, (256, 1024), 0)
    ).astype(F32).astype(BF16)
    with jax.named_scope("p10"):
        tall = jnp.dot(tall, repeat, preferred_element_type=F32)
    at_head = lax.broadcasted_iota(jnp.int32, (blk, 1024), 1) % 4
    with jax.named_scope("p11"):
        load_weights[0].wait()
    with jax.named_scope("p12"):
        load_weights[1].wait()
    both = jnp.zeros((4 * blk, 256), F32)
    with jax.named_scope("p13"):
        for n in range(chunks):
            piece = tall[n * blk : (n + 1) * blk]
            piece = jnp.concatenate([jnp.where(at_head == h, piece, 0.0).astype(BF16) for h in range(4)], axis=0)
            at = slice(n * 1024, (n + 1) * 1024)
            weights = jnp.concatenate([wv[at, :], wz[at, :]], axis=1)
            both = both + jnp.dot(piece, weights, preferred_element_type=F32)

    with jax.named_scope("p14"):
        for s in q1:
            s.forward()
    k2 = finish1(0, k1)

    with jax.named_scope("p15"):
        for copy in params:
            copy.wait()
    decay_all[...] = jnp.exp(-jnp.exp(decay_log[...]) * softplus(proj[:, 32:36] + dt_bias[...]))
    own_t = lax.broadcasted_iota(jnp.int32, (8 * blk, 3 * blk), 0) // 8 == lax.rem(
        lax.broadcasted_iota(jnp.int32, (8 * blk, 3 * blk), 1), blk
    )
    picks = [
        (
            lax.broadcasted_iota(jnp.int32, (8 * blk, COLS), 1)
            == 16 + 8 * o + lax.broadcasted_iota(jnp.int32, (8 * blk, COLS), 0) % 8
        )
        .astype(F32)
        .astype(BF16)
        for o in (0, 1)
    ]

    def prepare(r, carry):
        at = pl.ds(pl.multiple_of(r * blk, blk), blk)
        hi, lo = split(proj[at, :COLS])
        three = jnp.concatenate([hi.astype(F32), hi.astype(F32), lo.astype(F32)], axis=0).astype(BF16)
        decay = decay_all[at, :]
        for o in (0, 1):
            wide = lax.dot_general(picks[o], three, NT, preferred_element_type=F32)
            lift[r, o] = jnp.where(own_t, wide, 0.0).astype(BF16)
            pair = held[at, pl.ds(2 * o, 2)]
            keep = [jnp.broadcast_to(decay[:, h : h + 1], (blk, 128))[:, None, :] for h in (2 * o, 2 * o + 1)]
            held[at, pl.ds(2 * o, 2)] = jnp.stack([keep[c] * pair[:, c] for c in (0, 1)], axis=1)
        return carry

    with jax.named_scope("p16"):
        lax.fori_loop(0, rows // 2, prepare, 0)

    q2 = finish1(1, q1)

    with jax.named_scope("p17"):
        small2.wait()
    total = small[x] + small_land2[0] + small_land2[1] + small_land2[2]
    scales[...] = jnp.concatenate([total, jnp.zeros((120, 128), F32)], axis=0).T
    raw = scales[pl.ds(pl.multiple_of(z * blk, blk), blk), :]
    q_scale = lax.rsqrt(1.0 + raw[:, 0:2])
    k_scale = lax.rsqrt(1.0 + raw[:, 2:4])
    with jax.named_scope("p18"):
        unit_dot = raw[:, 4:6] * q_scale * k_scale
    decay = decay_all[mine, :]
    beta = 1.0 / (1.0 + jnp.exp(-proj[mine, 36:40]))

    g2 = {(o, name): copies.group() for o in (0, 1) for name in WAYS}
    near = {(o, name): copies.group() for o in (0, 1) for name in ("me", "left", "right", "far")}
    onward = [copies.group() for _ in (0, 1)]
    straight = [copies.group() for _ in (0, 1)]

    def send_near(o, name):
        r = rings1[o]
        b = rings2[o].me if name == "me" else rings2[o].at[name]
        piece = delta_all.at[o, :, r.me, b]
        for way in ("right", "left"):
            near[o, name].start(piece, piece, r.to[way])
        if name == "far":
            straight[o].start(piece, piece, r.to_far)

    def send_on(o, name):
        r = rings1[o]
        b = rings2[o].me if name == "me" else rings2[o].at[name]
        near[o, name].wait()
        for half, at, peer in ((0, r.left, r.to_right), (1, r.right, r.to_left)):
            piece = delta_all.at[o, half, at, b]
            onward[o].start(piece, piece, peer)

    deltas = []
    with jax.named_scope("p19"):
        for o in (0, 1):
            finish2(o, 0, k1[o], k2[o])
            for c in (0, 1):
                h = 2 * o + c
                readk = own_piece(o, c, 0)[...] * k_scale[:, o : o + 1]
                value = both[h * blk : (h + 1) * blk, :128]
                delta = beta[:, h : h + 1] * (value - decay[:, h : h + 1] * readk)
                delta_all[o, c, rings1[o].me, rings2[o].me] = delta * k_scale[:, o : o + 1]
                deltas.append(delta)
            here = delta_all.at[o, :, rings1[o].me, rings2[o].me]
            for name in ("right", "left", "far"):
                g2[o, name].start(here, here, rings2[o].to[name])
    with jax.named_scope("p20"):
        for o in (0, 1):
            send_near(o, "me")

    with jax.named_scope("p21"):
        lax.fori_loop(rows // 2, rows, prepare, 0)
    with jax.named_scope("p22"):
        for o in (0, 1):
            finish2(o, 1, q1[o], q2[o])
            for c in (0, 1):
                h = 2 * o + c
                old = own_piece(o, c, 1)[...] * q_scale[:, o : o + 1]
                readq = decay[:, h : h + 1] * old + unit_dot[:, o : o + 1] * deltas[h]
                meansq = jnp.mean(readq * readq, axis=-1, keepdims=True)
                gate = both[h * blk : (h + 1) * blk, 128:]
                gate = gate / (1.0 + jnp.exp(-gate))
                normed[:, h * 128 : (h + 1) * 128] = (readq * lax.rsqrt(meansq + 0.5) * gain[...] * gate).astype(BF16)

    with jax.named_scope("p23"):
        load_weights[2].wait()
    width = outs.shape[-1]
    out_group = copies.group()
    chip, core = head // 2, lax.rem(head, 2)
    order_out = []
    for up, other in ((2, 0), (2, 1), (1, 0), (1, 1), (3, 0), (3, 1), (0, 1), (0, 0)):
        order_out.append(lax.rem(chip + up, HEADS // 2) * 2 + lax.rem(core + other, 2))
    with jax.named_scope("p24"):
        for some in ((0, 1, 2, 3), (4, 5, 6, 7)):
            pieces = []
            for n in some:
                at = pl.ds(pl.multiple_of(order_out[n] * width, width), width)
                pieces.append(jnp.dot(normed[...], w_out[:, at], preferred_element_type=F32))
            for n, piece in zip(some, pieces):
                if n == 7:
                    outs_land[head] = piece
                else:
                    outs[n] = piece
            for n in some:
                if n == 7:
                    continue
                out_group.start(outs.at[n], outs_land.at[head], {"head": order_out[n]})

    with jax.named_scope("p25"):
        for o in (0, 1):
            for sent, name in (("right", "left"), ("left", "right")):
                g2[o, sent].wait()
                send_near(o, name)
    with jax.named_scope("p26"):
        for o in (0, 1):
            send_on(o, "me")
            g2[o, "far"].wait()
            send_near(o, "far")
    with jax.named_scope("p27"):
        for o in (0, 1):
            for name in ("left", "right"):
                send_on(o, name)

    def update_rows(o, first):
        for b in range(SIDE):
            r = row_at(o, first, b)
            at = pl.ds(pl.multiple_of(r * blk, blk), blk)
            add = growth(delta_all, lift, o, first, b, r)
            pair = held[at, pl.ds(2 * o, 2)]
            held[at, pl.ds(2 * o, 2)] = jnp.stack([pair[:, c] + add[c] for c in (0, 1)], axis=1)

    with jax.named_scope("p28"):
        for o in (0, 1):
            update_rows(o, rings1[o].me)
    with jax.named_scope("p29"):
        for o in (0, 1):
            near[o, "far"].wait()
    with jax.named_scope("p30"):
        for o in (0, 1):
            update_rows(o, rings1[o].left)
            update_rows(o, rings1[o].right)
    with jax.named_scope("p31"):
        out_group.wait()
    with jax.named_scope("p32"):
        for o in (0, 1):
            onward[o].wait()
            straight[o].wait()
    copies.drain()


def finish_kernel(held, delta_all, lift, outs_land, layer_out, new_state, last, layer, sems):
    row = lax.axis_index("row")
    spots = (row // SIDE, lax.rem(row, SIDE))
    blk = held.shape[0] // (SIDE * SIDE)

    def store(src, o, r, count=1):
        dst = new_state.at[pl.ds(pl.multiple_of(r * blk, blk), count * blk), pl.ds(2 * o, 2)]
        pltpu.make_async_copy(src, dst, sems.at[0]).start()

    for d in (0, 1, 3):
        first = lax.rem(spots[0] + d, SIDE)
        at = pl.ds(pl.multiple_of(first * SIDE * blk, blk), SIDE * blk)
        store(held.at[at, pl.ds(0, 2)], 0, first * SIDE, SIDE)
        for b in range(SIDE):
            r = b * SIDE + lax.rem(spots[1] + d, SIDE)
            store(held.at[pl.ds(pl.multiple_of(r * blk, blk), blk), pl.ds(2, 2)], 1, r)
    total = outs_land[0]
    for n in range(1, HEADS):
        total = total + outs_land[n]
    layer[...] = total.astype(BF16)
    layer_copy = pltpu.make_async_copy(layer, layer_out, sems.at[1])
    layer_copy.start()
    for o in (0, 1):
        first = lax.rem(spots[o] + 2, SIDE)
        for b in range(SIDE):
            r = first * SIDE + b if o == 0 else b * SIDE + first
            at = pl.ds(pl.multiple_of(r * blk, blk), blk)
            add = growth(delta_all, lift, o, first, b, r)
            pair = held[at, pl.ds(2 * o, 2)]
            last[o * SIDE + b] = jnp.stack([pair[:, c] + add[c] for c in (0, 1)], axis=1)
            store(last.at[o * SIDE + b], o, r)
    layer_copy.wait()
    pltpu.make_async_copy(new_state, new_state, sems.at[0]).wait()


def local(
    hidden_in,
    w_query,
    w_key,
    w_value,
    w_zgate,
    w_decay,
    w_beta,
    decay_log,
    dt_bias,
    norm_gain,
    w_out,
    state,
):
    seqs, width = hidden_in.shape
    rows = SIDE * SIDE
    blk = seqs // rows
    vmem = pl.BlockSpec(memory_space=pltpu.VMEM)
    anywhere = pl.BlockSpec(memory_space=pltpu.HBM)
    held, delta_all, lift, outs_land = pl.pallas_call(
        exchange_kernel,
        out_shape=(
            pltpu.VMEM((seqs, PITCH // 8, 8, 128), F32),
            pltpu.VMEM((2, 2, SIDE, SIDE, blk, 128), F32),
            pltpu.VMEM((rows, 2, 8 * blk, 3 * blk), BF16),
            pltpu.VMEM((HEADS, blk, 256), F32),
        ),
        in_specs=[anywhere] * 12,
        out_specs=(vmem,) * 4,
        scratch_shapes=[
            pltpu.VMEM((2, 8, width), BF16),
            pltpu.VMEM((2, 8, width), BF16),
            pltpu.VMEM((4, width), BF16),
            pltpu.VMEM((4, width), BF16),
            pltpu.VMEM((1, 4), F32),
            pltpu.VMEM((1, 4), F32),
            pltpu.VMEM((1, 128), F32),
            pltpu.VMEM((seqs, width), BF16),
            pltpu.VMEM((4 * width, 128), BF16),
            pltpu.VMEM((4 * width, 128), BF16),
            pltpu.VMEM((512, width), BF16),
            pltpu.VMEM((seqs, 128), F32),
            pltpu.VMEM((seqs, 4), F32),
            pltpu.VMEM((2, 2, 2, SIDE, SIDE, blk, 128), F32),
            pltpu.VMEM((2, 2, 2, 3, SIDE, blk, 128), F32),
            pltpu.VMEM((2, 2, 3, 2, blk, 128), F32),
            pltpu.VMEM((SIDE, 8, 128), F32),
            pltpu.VMEM((6, 8, 128), F32),
            pltpu.VMEM((3, 8, 128), F32),
            pltpu.VMEM((128, 128), F32),
            pltpu.VMEM((blk, 512), BF16),
            pltpu.VMEM((HEADS, blk, 256), F32),
            pltpu.VMEM((2, 128, 1024), BF16),
            pltpu.VMEM((SIDE * blk, 1024), F32),
            pltpu.SemaphoreType.DMA((2 * SIDE,)),
            pltpu.SemaphoreType.DMA((11,)),
            pltpu.SemaphoreType.DMA((2,)),
            pltpu.SemaphoreType.DMA((51,)),
        ],
        compiler_params=pltpu.CompilerParams(
            collective_id=0, has_side_effects=True, vmem_limit_bytes=36 * 1024 * 1024
        ),
        name="exchange",
    )(
        *(
            pltpu.with_memory_space_constraint(operand, pltpu.HBM)
            for operand in (
                jnp.transpose(w_query, (1, 2, 0)),
                jnp.transpose(w_key, (1, 2, 0)),
                jnp.transpose(w_decay, (1, 0)),
                jnp.transpose(w_beta, (1, 0)),
                decay_log.reshape(1, 4),
                dt_bias.reshape(1, 4),
                norm_gain.reshape(1, 128),
                hidden_in,
                w_value.reshape(4 * width, 128),
                w_zgate.reshape(4 * width, 128),
                w_out.reshape(512, width),
                state,
            )
        )
    )
    layer_out, new_state = pl.pallas_call(
        finish_kernel,
        out_shape=(
            jax.ShapeDtypeStruct((blk, 256), BF16),
            jax.ShapeDtypeStruct(state.shape, F32),
        ),
        in_specs=[vmem] * 4,
        out_specs=(anywhere, anywhere),
        scratch_shapes=[
            pltpu.VMEM((2 * SIDE, blk, 2, 8, 128), F32),
            pltpu.VMEM((blk, 256), BF16),
            pltpu.SemaphoreType.DMA((2,)),
        ],
        compiler_params=pltpu.CompilerParams(vmem_limit_bytes=16 * 1024 * 1024),
        name="finish",
    )(*(pltpu.with_memory_space_constraint(a, pltpu.VMEM) for a in (held, delta_all, lift, outs_land)))
    return layer_out, new_state


def solution(mesh):
    in_specs = (
        P(),
        P(None, "head", "row"),
        P(None, "head", "row"),
        P(None, "head", None),
        P(None, "head", None),
        P(None, "head"),
        P(None, "head"),
        P("head"),
        P("head"),
        P(),
        P("head", None, None),
        P(None, "head", "row", None),
    )
    out_specs = (P("row", "head"), P(None, "head", "row", None))
    return jax.shard_map(local, mesh=mesh, in_specs=in_specs, out_specs=out_specs, check_vma=False)
```

```python
import math

import jax
import jax.numpy as jnp
from jax import lax
from jax.experimental import pallas as pl
from jax.experimental.pallas import tpu as pltpu
from jax.sharding import PartitionSpec as P

F32 = jnp.float32
BF16 = jnp.bfloat16
NT = (((1,), (1,)), ((), ()))
SIDE = 4
COLS = 40
HEADS = 8
PITCH = 40


def softplus(x):
    return jnp.maximum(x, 0.0) + jnp.log1p(jnp.exp(-jnp.abs(x)))


def size(ref):
    return math.prod(ref.shape) * jnp.dtype(ref.dtype).itemsize


class Group:
    def __init__(self, copies, sem, like):
        self.copies, self.sem, self.like, self.bytes = copies, sem, like, 0

    def start(self, src, dst, peer, count=True):
        if count:
            self.bytes += size(src)
            self.copies.sent[self.like is None].bytes += size(src)
        pltpu.make_async_remote_copy(
            src_ref=src,
            dst_ref=dst,
            send_sem=self.copies.sent[self.like is None].sem,
            recv_sem=self.sem,
            device_id=peer,
            device_id_type=pl.DeviceIdType.MESH,
        ).start()

    def wait(self):
        if self.like is None:
            rows = self.bytes // size(self.copies.held.at[0, pl.ds(0, 4)])
            ref = self.copies.held.at[pl.ds(0, rows), pl.ds(0, 4)]
        else:
            ref = self.like.at[pl.ds(0, self.bytes // size(self.like.at[0]))]
        pltpu.make_async_copy(ref, ref, self.sem).wait()


class Copies:
    def __init__(self, held, little, send, recv):
        self.held, self.recv, self.used = held, recv, 0
        self.sent = {True: Group(self, send.at[0], None), False: Group(self, send.at[1], little)}

    def group(self, like=None):
        self.used += 1
        return Group(self, self.recv.at[self.used - 1], like)

    def drain(self):
        for group in self.sent.values():
            group.wait()


class Ring:
    def __init__(self, me, row_of):
        self.me = me
        self.right = lax.rem(me + 1, SIDE)
        self.far = lax.rem(me + 2, SIDE)
        self.left = lax.rem(me + 3, SIDE)
        self.to_right = {"row": row_of(self.right)}
        self.to_far = {"row": row_of(self.far)}
        self.to_left = {"row": row_of(self.left)}
        self.at = {"far": self.far, "right": self.right, "left": self.left}
        self.to = {"far": self.to_far, "right": self.to_right, "left": self.to_left}


class Scatter:
    def __init__(self, copies, ring, pieces, part, land, fine):
        self.ring, self.pieces, self.part, self.land = ring, pieces, part, land
        self.relay = [copies.group() for _ in pieces] if fine else [copies.group()] * len(pieces)
        self.joint = [copies.group() for _ in pieces]

    def send_far(self, count=True):
        r = self.ring
        for n, b in enumerate(self.pieces):
            for half, peer in ((0, r.to_left), (1, r.to_right)):
                self.relay[n].start(self.part(half, r.far).at[b], self.land.at[half, 0, b], peer, count)

    def send_right(self):
        r = self.ring
        self.joint[0].start(self.part(0, r.right), self.land.at[0, 1], r.to_right)

    def send_left(self):
        r = self.ring
        self.joint[0].start(self.part(1, r.left), self.land.at[1, 1], r.to_left)

    def forward(self):
        r = self.ring
        for n, b in enumerate(self.pieces):
            if self.relay[n] not in self.relay[:n]:
                self.relay[n].wait()
            for half, to, peer in ((0, r.left, r.to_left), (1, r.right, r.to_right)):
                piece = self.part(half, to).at[b]
                piece[...] = piece[...] + self.land[half, 0, b]
                self.joint[n].start(piece, self.land.at[half, 2, b], peer)

    def finish(self, n):
        b = self.pieces[n]
        if self.joint[n] not in self.joint[:n]:
            self.joint[n].wait()
        for half in (0, 1):
            piece = self.part(half, self.ring.me).at[b]
            piece[...] = piece[...] + self.land[half, 1, b] + self.land[half, 2, b]


WAYS = ("far", "right", "left")


def split(x):
    hi = x.astype(BF16)
    return hi, (x - hi.astype(F32)).astype(BF16)


def growth(delta_all, lift, o, first, second, r):
    hi, lo = split(jnp.concatenate([delta_all[o, c, first, second] for c in (0, 1)], axis=1))
    add = jnp.dot(lift[r, o], jnp.concatenate([hi, lo, hi], axis=0), preferred_element_type=F32)
    return [add[:, c * 128 : (c + 1) * 128].reshape(hi.shape[0], 8, 128) for c in (0, 1)]


def exchange_kernel(
    wq_hbm,
    wk_hbm,
    wd_hbm,
    wb_hbm,
    decay_log_hbm,
    dt_bias_hbm,
    gain_hbm,
    hid_hbm,
    wv_hbm,
    wz_hbm,
    w_out_hbm,
    state,
    held,
    delta_all,
    lift,
    outs_land,
    wq,
    wk,
    wd,
    wb,
    decay_log,
    dt_bias,
    gain,
    hid,
    wv,
    wz,
    w_out,
    proj,
    decay_all,
    part,
    land1,
    land2,
    small,
    small_land1,
    small_land2,
    scales,
    normed,
    outs,
    picked,
    wide,
    load_sem,
    weight_sem,
    send_sem,
    recv_sem,
):
    row = lax.axis_index("row")
    head = lax.axis_index("head")
    x, z = row // SIDE, lax.rem(row, SIDE)
    rows = SIDE * SIDE
    blk = held.shape[0] // rows

    def row_at(o, first, second):
        return first * SIDE + second if o == 0 else second * SIDE + first

    first = []
    small_weights = ((wq_hbm, wq), (wk_hbm, wk), (wd_hbm, wd), (wb_hbm, wb))
    quarter = hid.shape[0] // 4
    pieces = tuple((hid_hbm.at[pl.ds(n * quarter, quarter)], hid.at[pl.ds(n * quarter, quarter)]) for n in range(4))
    for src, dst in pieces:
        pltpu.make_async_copy(src, dst, weight_sem.at[4]).start()
    for n, (src, dst) in enumerate(small_weights):
        first.append(pltpu.make_async_copy(src, dst, weight_sem.at[n]))
        first[-1].start()
    params = []
    for n, (src, dst) in enumerate(((decay_log_hbm, decay_log), (dt_bias_hbm, dt_bias), (gain_hbm, gain))):
        params.append(pltpu.make_async_copy(src, dst, weight_sem.at[8 + n]))
        params[-1].start()
    all_hid = pltpu.make_async_copy(hid, hid, weight_sem.at[4])

    barrier = pltpu.get_barrier_semaphore()
    peers = []
    for d in (1, 2, 3):
        peers.append({"row": lax.rem(x + d, SIDE) * SIDE + z})
        peers.append({"row": x * SIDE + lax.rem(z + d, SIDE)})
    for d in range(1, HEADS):
        peers.append({"head": lax.rem(head + d, HEADS)})
    for peer in peers:
        pl.semaphore_signal(barrier, inc=1, device_id=peer, device_id_type=pl.DeviceIdType.MESH)

    rings1 = [
        Ring(x, lambda a: row_at(0, a, z)),
        Ring(z, lambda a: row_at(1, a, x)),
    ]
    rings2 = [
        Ring(z, lambda b: row_at(0, x, b)),
        Ring(x, lambda b: row_at(1, z, b)),
    ]
    order = [[r.far, r.right, r.left, r.me] for r in rings1]

    def load(j, o):
        for b in range(SIDE):
            at = row_at(o, order[o][j], b) * blk
            pltpu.make_async_copy(
                state.at[pl.ds(at, blk), pl.ds(2 * o, 2)],
                held.at[pl.ds(at, blk), pl.ds(2 * o, 2)],
                load_sem.at[j * 2 + o],
            ).start()

    def await_load(j, o):
        ref = held.at[pl.ds(0, SIDE * blk // 2), pl.ds(0, 4)]
        pltpu.make_async_copy(ref, ref, load_sem.at[j * 2 + o]).wait()

    proj[...] = jnp.zeros_like(proj)
    for o in (0, 1):
        source = lax.broadcasted_iota(jnp.int32, (128, 1024), 0) % 64
        picked[o] = (source == 8 * o + lax.broadcasted_iota(jnp.int32, (128, 1024), 1) // 128).astype(F32).astype(BF16)
    with jax.named_scope("p01"):
        for copy in first:
            copy.wait()
    load(0, 0)
    parts = [ref[n].astype(F32) for ref in (wq, wk) for n in (0, 1)] + [wd[...].astype(F32), wb[...].astype(F32)]
    w = jnp.concatenate(parts, axis=0).astype(BF16)
    swapped = jnp.concatenate(parts[2:4] + parts[:2] + parts[4:], axis=0).astype(BF16)
    with jax.named_scope("p02"):
        all_hid.wait()
    load(0, 1)
    half = hid.shape[0] // 2
    with jax.named_scope("p03"):
        upper = lax.dot_general(hid[:half, :], w, NT, preferred_element_type=F32)
    with jax.named_scope("p04"):
        lower = lax.dot_general(hid[half:, :], swapped, NT, preferred_element_type=F32)
    proj[:half, :COLS] = upper
    proj[half:, 0:16] = lower[:, 16:32]
    proj[half:, 16:32] = lower[:, 0:16]
    proj[half:, 32:COLS] = lower[:, 32:COLS]
    for j in (1, 2, 3):
        for o in (0, 1):
            load(j, o)

    with jax.named_scope("p05"):
        copies = Copies(held, small_land1, send_sem, recv_sem)
    flat = held.reshape(held.shape[0] * PITCH, 128)

    def read_blocks(o, first):
        starts = [pl.multiple_of(row_at(o, first, b) * blk, blk) for b in range(SIDE)]
        vecs = [proj[pl.ds(at, blk), :] for at in starts]
        hi, lo = split(jnp.concatenate(vecs, axis=0))
        both_terms = (hi.astype(F32) + pltpu.roll(lo.astype(F32), 64, 1)).astype(BF16)
        wide[...] = jnp.dot(both_terms, picked[o], preferred_element_type=F32)
        for b, at in enumerate(starts):
            for g in range(blk // 8):
                mine = slice(g * 8, (g + 1) * 8)
                sums = [[None, None], [None, None]]
                for i in range(8):
                    n = 16 + 8 * o + i
                    key = jnp.broadcast_to(vecs[b][mine, n : n + 1], (8, 128))
                    query = wide[b * blk + g * 8 : b * blk + (g + 1) * 8, i * 128 : (i + 1) * 128]
                    for c in (0, 1):
                        start = (at + g * 8) * PITCH + (2 * o + c) * 8 + i
                        values = flat[pl.ds(start, 8, stride=PITCH), :]
                        for t, vector in ((0, key), (1, query)):
                            term = vector * values
                            sums[t][c] = term if i == 0 else sums[t][c] + term
                for c in (0, 1):
                    for t in (0, 1):
                        part[o, c, t, first, b, mine] = sums[t][c]

    def send_sums():
        for a in range(SIDE):
            cols = proj[a * 128 : (a + 1) * 128, :].T
            terms = []
            for u, v in ((0, 0), (16, 16), (0, 16)):
                for hk in (0, 8):
                    product = cols[u + hk : u + hk + 8] * cols[v + hk : v + hk + 8]
                    terms.append(jnp.sum(product, axis=0, keepdims=True))
            terms.append(jnp.zeros((2, 128), F32))
            small[a] = jnp.concatenate(terms, axis=0)
        group = copies.group(small_land1)
        for n, name in enumerate(WAYS):
            group.start(small.at[rings1[0].at[name]], small_land1.at[n], rings1[0].to[name])
        return group

    def scatter1(o, t):
        r = rings2[o]
        pieces = (r.far, r.right, r.left, r.me)
        return Scatter(copies, rings1[o], pieces, lambda c, a: part.at[o, c, t, a], land1.at[o, t], t == 0)

    def own_piece(o, c, t):
        return part.at[o, c, t, rings1[o].me, rings2[o].me]

    def finish1(t, scatters):
        groups = [copies.group() for _ in scatters]
        for n, name in enumerate(WAYS):
            for o, s in enumerate(scatters):
                r = rings2[o]
                s.finish(n)
                groups[o].start(part.at[o, :, t, rings1[o].me, r.at[name]], land2.at[o, t, n], r.to[name])
        return groups

    def finish2(o, t, first, s):
        first.finish(3)
        s.wait()
        for c in (0, 1):
            piece = own_piece(o, c, t)
            piece[...] = piece[...] + land2[o, t, 0, c] + land2[o, t, 1, c] + land2[o, t, 2, c]

    k1 = [scatter1(o, 0) for o in (0, 1)]
    q1 = [scatter1(o, 1) for o in (0, 1)]

    for j in range(SIDE):
        for o in (0, 1):
            with jax.named_scope(f"wait{j}"):
                await_load(j, o)
            if j == 0:
                with jax.named_scope(f"read{j}{o}"):
                    read_blocks(o, order[o][j])
                    if o == 0:
                        pl.semaphore_wait(barrier, len(peers))
                k1[o].send_far()
        if j == 0:
            with jax.named_scope("sums"):
                small1 = send_sums()

            @pl.when(lax.rem(head, 2) == 0)
            def _():
                for o in (0, 1):
                    q1[o].send_far()

        else:
            for o in (0, 1):
                with jax.named_scope(f"read{j}{o}"):
                    read_blocks(o, order[o][j])
                if j == 1:
                    k1[o].send_right()
                if j == 2:
                    k1[o].send_left()
        if j == 1:
            load_weights = []
            for n, (src, dst) in enumerate(((wv_hbm, wv), (wz_hbm, wz), (w_out_hbm, w_out))):
                load_weights.append(pltpu.make_async_copy(src, dst, weight_sem.at[n + 5]))
                load_weights[-1].start()
    with jax.named_scope("p07"):
        for s in k1:
            s.forward()

    @pl.when(lax.rem(head, 2) == 1)
    def _():
        for o in (0, 1):
            q1[o].send_far(count=False)

    with jax.named_scope("p08"):
        for s in q1:
            s.send_right()
            s.send_left()
    with jax.named_scope("p09"):
        small1.wait()
    small[x] = small[x] + small_land1[0] + small_land1[1] + small_land1[2]
    small2 = copies.group(small_land2)
    for n, name in enumerate(WAYS):
        small2.start(small.at[x], small_land2.at[n], rings2[0].to[name])

    mine = pl.ds(pl.multiple_of(row * blk, blk), blk)
    own_hid = hid[mine, :]
    chunks = own_hid.shape[1] // 256
    tall = jnp.concatenate([own_hid[:, n * 256 : (n + 1) * 256] for n in range(chunks)], axis=0)
    repeat = (
        lax.broadcasted_iota(jnp.int32, (256, 1024), 1) // 4 == lax.broadcasted_iota(jnp.int32, (256, 1024), 0)
    ).astype(F32).astype(BF16)
    with jax.named_scope("p10"):
        tall = jnp.dot(tall, repeat, preferred_element_type=F32)
    at_head = lax.broadcasted_iota(jnp.int32, (blk, 1024), 1) % 4
    with jax.named_scope("p11"):
        load_weights[0].wait()
    with jax.named_scope("p12"):
        load_weights[1].wait()
    both = jnp.zeros((4 * blk, 256), F32)
    with jax.named_scope("p13"):
        for n in range(chunks):
            piece = tall[n * blk : (n + 1) * blk]
            piece = jnp.concatenate([jnp.where(at_head == h, piece, 0.0).astype(BF16) for h in range(4)], axis=0)
            at = slice(n * 1024, (n + 1) * 1024)
            weights = jnp.concatenate([wv[at, :], wz[at, :]], axis=1)
            both = both + jnp.dot(piece, weights, preferred_element_type=F32)

    with jax.named_scope("p14"):
        for s in q1:
            s.forward()
    k2 = finish1(0, k1)

    with jax.named_scope("p15"):
        for copy in params:
            copy.wait()
    decay_all[...] = jnp.exp(-jnp.exp(decay_log[...]) * softplus(proj[:, 32:36] + dt_bias[...]))
    own_t = lax.broadcasted_iota(jnp.int32, (8 * blk, 3 * blk), 0) // 8 == lax.rem(
        lax.broadcasted_iota(jnp.int32, (8 * blk, 3 * blk), 1), blk
    )
    picks = [
        (
            lax.broadcasted_iota(jnp.int32, (8 * blk, COLS), 1)
            == 16 + 8 * o + lax.broadcasted_iota(jnp.int32, (8 * blk, COLS), 0) % 8
        )
        .astype(F32)
        .astype(BF16)
        for o in (0, 1)
    ]

    def prepare(r, carry):
        at = pl.ds(pl.multiple_of(r * blk, blk), blk)
        hi, lo = split(proj[at, :COLS])
        three = jnp.concatenate([hi.astype(F32), hi.astype(F32), lo.astype(F32)], axis=0).astype(BF16)
        decay = decay_all[at, :]
        for o in (0, 1):
            wide = lax.dot_general(picks[o], three, NT, preferred_element_type=F32)
            lift[r, o] = jnp.where(own_t, wide, 0.0).astype(BF16)
            pair = held[at, pl.ds(2 * o, 2)]
            keep = [jnp.broadcast_to(decay[:, h : h + 1], (blk, 128))[:, None, :] for h in (2 * o, 2 * o + 1)]
            held[at, pl.ds(2 * o, 2)] = jnp.stack([keep[c] * pair[:, c] for c in (0, 1)], axis=1)
        return carry

    with jax.named_scope("p16"):
        lax.fori_loop(0, rows // 2, prepare, 0)

    q2 = finish1(1, q1)

    with jax.named_scope("p17"):
        small2.wait()
    total = small[x] + small_land2[0] + small_land2[1] + small_land2[2]
    scales[...] = jnp.concatenate([total, jnp.zeros((120, 128), F32)], axis=0).T
    raw = scales[pl.ds(pl.multiple_of(z * blk, blk), blk), :]
    q_scale = lax.rsqrt(1.0 + raw[:, 0:2])
    k_scale = lax.rsqrt(1.0 + raw[:, 2:4])
    with jax.named_scope("p18"):
        unit_dot = raw[:, 4:6] * q_scale * k_scale
    decay = decay_all[mine, :]
    beta = 1.0 / (1.0 + jnp.exp(-proj[mine, 36:40]))

    g2 = {(o, name): copies.group() for o in (0, 1) for name in WAYS}
    near = {(o, name): copies.group() for o in (0, 1) for name in ("me", "left", "right", "far")}
    onward = [copies.group() for _ in (0, 1)]
    straight = [copies.group() for _ in (0, 1)]

    def send_near(o, name):
        r = rings1[o]
        b = rings2[o].me if name == "me" else rings2[o].at[name]
        piece = delta_all.at[o, :, r.me, b]
        for way in ("right", "left"):
            near[o, name].start(piece, piece, r.to[way])
        if name == "far":
            straight[o].start(piece, piece, r.to_far)

    def send_on(o, name):
        r = rings1[o]
        b = rings2[o].me if name == "me" else rings2[o].at[name]
        near[o, name].wait()
        for half, at, peer in ((0, r.left, r.to_right), (1, r.right, r.to_left)):
            piece = delta_all.at[o, half, at, b]
            onward[o].start(piece, piece, peer)

    deltas = []
    with jax.named_scope("p19"):
        for o in (0, 1):
            finish2(o, 0, k1[o], k2[o])
            for c in (0, 1):
                h = 2 * o + c
                readk = own_piece(o, c, 0)[...] * k_scale[:, o : o + 1]
                value = both[h * blk : (h + 1) * blk, :128]
                delta = beta[:, h : h + 1] * (value - decay[:, h : h + 1] * readk)
                delta_all[o, c, rings1[o].me, rings2[o].me] = delta * k_scale[:, o : o + 1]
                deltas.append(delta)
            here = delta_all.at[o, :, rings1[o].me, rings2[o].me]
            for name in ("right", "left", "far"):
                g2[o, name].start(here, here, rings2[o].to[name])
    with jax.named_scope("p20"):
        for o in (0, 1):
            send_near(o, "me")

    with jax.named_scope("p21"):
        lax.fori_loop(rows // 2, rows, prepare, 0)
    with jax.named_scope("p22"):
        for o in (0, 1):
            finish2(o, 1, q1[o], q2[o])
            for c in (0, 1):
                h = 2 * o + c
                old = own_piece(o, c, 1)[...] * q_scale[:, o : o + 1]
                readq = decay[:, h : h + 1] * old + unit_dot[:, o : o + 1] * deltas[h]
                meansq = jnp.mean(readq * readq, axis=-1, keepdims=True)
                gate = both[h * blk : (h + 1) * blk, 128:]
                gate = gate / (1.0 + jnp.exp(-gate))
                normed[:, h * 128 : (h + 1) * 128] = (readq * lax.rsqrt(meansq + 0.5) * gain[...] * gate).astype(BF16)

    with jax.named_scope("p23"):
        load_weights[2].wait()
    width = outs.shape[-1]
    out_group = copies.group()
    chip, core = head // 2, lax.rem(head, 2)
    order_out = []
    for up, other in ((2, 0), (2, 1), (1, 0), (1, 1), (3, 0), (3, 1), (0, 1), (0, 0)):
        order_out.append(lax.rem(chip + up, HEADS // 2) * 2 + lax.rem(core + other, 2))
    with jax.named_scope("p24"):
        for some in ((0, 1, 2, 3), (4, 5, 6, 7)):
            pieces = []
            for n in some:
                at = pl.ds(pl.multiple_of(order_out[n] * width, width), width)
                pieces.append(jnp.dot(normed[...], w_out[:, at], preferred_element_type=F32))
            for n, piece in zip(some, pieces):
                if n == 7:
                    outs_land[head] = piece
                else:
                    outs[n] = piece
            for n in some:
                if n == 7:
                    continue
                out_group.start(outs.at[n], outs_land.at[head], {"head": order_out[n]})

    with jax.named_scope("p25"):
        for o in (0, 1):
            for sent, name in (("right", "left"), ("left", "right")):
                g2[o, sent].wait()
                send_near(o, name)
    with jax.named_scope("p26"):
        for o in (0, 1):
            send_on(o, "me")
            g2[o, "far"].wait()
            send_near(o, "far")
    with jax.named_scope("p27"):
        for o in (0, 1):
            for name in ("left", "right"):
                send_on(o, name)

    def update_rows(o, first):
        for b in range(SIDE):
            r = row_at(o, first, b)
            at = pl.ds(pl.multiple_of(r * blk, blk), blk)
            add = growth(delta_all, lift, o, first, b, r)
            pair = held[at, pl.ds(2 * o, 2)]
            held[at, pl.ds(2 * o, 2)] = jnp.stack([pair[:, c] + add[c] for c in (0, 1)], axis=1)

    with jax.named_scope("p28"):
        for o in (0, 1):
            update_rows(o, rings1[o].me)
    with jax.named_scope("p29"):
        for o in (0, 1):
            near[o, "far"].wait()
    with jax.named_scope("p30"):
        for o in (0, 1):
            update_rows(o, rings1[o].left)
            update_rows(o, rings1[o].right)
    with jax.named_scope("p31"):
        out_group.wait()
    with jax.named_scope("p32"):
        for o in (0, 1):
            onward[o].wait()
            straight[o].wait()
    copies.drain()


def finish_kernel(held, delta_all, lift, outs_land, layer_out, new_state, last, layer, sems):
    row = lax.axis_index("row")
    spots = (row // SIDE, lax.rem(row, SIDE))
    blk = held.shape[0] // (SIDE * SIDE)

    def store(src, o, r, count=1):
        dst = new_state.at[pl.ds(pl.multiple_of(r * blk, blk), count * blk), pl.ds(2 * o, 2)]
        pltpu.make_async_copy(src, dst, sems.at[0]).start()

    for d in (0, 1, 3):
        first = lax.rem(spots[0] + d, SIDE)
        at = pl.ds(pl.multiple_of(first * SIDE * blk, blk), SIDE * blk)
        store(held.at[at, pl.ds(0, 2)], 0, first * SIDE, SIDE)
        for b in range(SIDE):
            r = b * SIDE + lax.rem(spots[1] + d, SIDE)
            store(held.at[pl.ds(pl.multiple_of(r * blk, blk), blk), pl.ds(2, 2)], 1, r)
    total = outs_land[0]
    for n in range(1, HEADS):
        total = total + outs_land[n]
    layer[...] = total.astype(BF16)
    layer_copy = pltpu.make_async_copy(layer, layer_out, sems.at[1])
    layer_copy.start()
    for o in (0, 1):
        first = lax.rem(spots[o] + 2, SIDE)
        for b in range(SIDE):
            r = first * SIDE + b if o == 0 else b * SIDE + first
            at = pl.ds(pl.multiple_of(r * blk, blk), blk)
            add = growth(delta_all, lift, o, first, b, r)
            pair = held[at, pl.ds(2 * o, 2)]
            last[o * SIDE + b] = jnp.stack([pair[:, c] + add[c] for c in (0, 1)], axis=1)
            store(last.at[o * SIDE + b], o, r)
    layer_copy.wait()
    pltpu.make_async_copy(new_state, new_state, sems.at[0]).wait()


def local(
    hidden_in,
    w_query,
    w_key,
    w_value,
    w_zgate,
    w_decay,
    w_beta,
    decay_log,
    dt_bias,
    norm_gain,
    w_out,
    state,
):
    seqs, width = hidden_in.shape
    rows = SIDE * SIDE
    blk = seqs // rows
    vmem = pl.BlockSpec(memory_space=pltpu.VMEM)
    anywhere = pl.BlockSpec(memory_space=pltpu.HBM)
    held, delta_all, lift, outs_land = pl.pallas_call(
        exchange_kernel,
        out_shape=(
            pltpu.VMEM((seqs, PITCH // 8, 8, 128), F32),
            pltpu.VMEM((2, 2, SIDE, SIDE, blk, 128), F32),
            pltpu.VMEM((rows, 2, 8 * blk, 3 * blk), BF16),
            pltpu.VMEM((HEADS, blk, 256), F32),
        ),
        in_specs=[anywhere] * 12,
        out_specs=(vmem,) * 4,
        scratch_shapes=[
            pltpu.VMEM((2, 8, width), BF16),
            pltpu.VMEM((2, 8, width), BF16),
            pltpu.VMEM((4, width), BF16),
            pltpu.VMEM((4, width), BF16),
            pltpu.VMEM((1, 4), F32),
            pltpu.VMEM((1, 4), F32),
            pltpu.VMEM((1, 128), F32),
            pltpu.VMEM((seqs, width), BF16),
            pltpu.VMEM((4 * width, 128), BF16),
            pltpu.VMEM((4 * width, 128), BF16),
            pltpu.VMEM((512, width), BF16),
            pltpu.VMEM((seqs, 128), F32),
            pltpu.VMEM((seqs, 4), F32),
            pltpu.VMEM((2, 2, 2, SIDE, SIDE, blk, 128), F32),
            pltpu.VMEM((2, 2, 2, 3, SIDE, blk, 128), F32),
            pltpu.VMEM((2, 2, 3, 2, blk, 128), F32),
            pltpu.VMEM((SIDE, 8, 128), F32),
            pltpu.VMEM((6, 8, 128), F32),
            pltpu.VMEM((3, 8, 128), F32),
            pltpu.VMEM((128, 128), F32),
            pltpu.VMEM((blk, 512), BF16),
            pltpu.VMEM((HEADS, blk, 256), F32),
            pltpu.VMEM((2, 128, 1024), BF16),
            pltpu.VMEM((SIDE * blk, 1024), F32),
            pltpu.SemaphoreType.DMA((2 * SIDE,)),
            pltpu.SemaphoreType.DMA((11,)),
            pltpu.SemaphoreType.DMA((2,)),
            pltpu.SemaphoreType.DMA((51,)),
        ],
        compiler_params=pltpu.CompilerParams(
            collective_id=0, has_side_effects=True, vmem_limit_bytes=36 * 1024 * 1024
        ),
        name="exchange",
    )(
        *(
            pltpu.with_memory_space_constraint(operand, pltpu.HBM)
            for operand in (
                jnp.transpose(w_query, (1, 2, 0)),
                jnp.transpose(w_key, (1, 2, 0)),
                jnp.transpose(w_decay, (1, 0)),
                jnp.transpose(w_beta, (1, 0)),
                decay_log.reshape(1, 4),
                dt_bias.reshape(1, 4),
                norm_gain.reshape(1, 128),
                hidden_in,
                w_value.reshape(4 * width, 128),
                w_zgate.reshape(4 * width, 128),
                w_out.reshape(512, width),
                state,
            )
        )
    )
    layer_out, new_state = pl.pallas_call(
        finish_kernel,
        out_shape=(
            jax.ShapeDtypeStruct((blk, 256), BF16),
            jax.ShapeDtypeStruct(state.shape, F32),
        ),
        in_specs=[vmem] * 4,
        out_specs=(anywhere, anywhere),
        scratch_shapes=[
            pltpu.VMEM((2 * SIDE, blk, 2, 8, 128), F32),
            pltpu.VMEM((blk, 256), BF16),
            pltpu.SemaphoreType.DMA((2,)),
        ],
        compiler_params=pltpu.CompilerParams(vmem_limit_bytes=16 * 1024 * 1024),
        name="finish",
    )(*(pltpu.with_memory_space_constraint(a, pltpu.VMEM) for a in (held, delta_all, lift, outs_land)))
    return layer_out, new_state


def solution(mesh):
    in_specs = (
        P(),
        P(None, "head", "row"),
        P(None, "head", "row"),
        P(None, "head", None),
        P(None, "head", None),
        P(None, "head"),
        P(None, "head"),
        P("head"),
        P("head"),
        P(),
        P("head", None, None),
        P(None, "head", "row", None),
    )
    out_specs = (P("row", "head"), P(None, "head", "row", None))
    return jax.shard_map(local, mesh=mesh, in_specs=in_specs, out_specs=out_specs, check_vma=False)
```
